32 devices in a mesh: gx: 4 (over y, core), gy: 4 (over z), gz: 2 (over x).
Axes of the slice: x: 2, y: 2, z: 4, core: 2. Of those that a mesh axis runs over, the one named last changes fastest.
Arguments:
- fractions: float32 [3, 4, 8, 4, 128], P(None, 'gx', 'gy', 'gz'), may hold values from 0 to 1
- polarizability: float32 [4, 8, 4, 128], P('gx', 'gy', 'gz'), may hold values from 0.5 to 2
- occupancy: int32 [4, 8, 4, 128], P('gx', 'gy', 'gz'), may hold values 0 or 1
- pair_mask: int32 [4, 8, 4, 27], P('gx', 'gy', 'gz'), may hold values from 0 to 1, as said below
- perm_field: float32 [6, 4, 8, 4, 128], P(None, 'gx', 'gy', 'gz'), may hold values from -6 to 6
- history: float32 [6, 6, 4, 8, 4, 128], P(None, None, 'gx', 'gy', 'gz'), may hold values from -12 to 12
Outputs:
- induced: float32 [6, 4, 8, 4, 128], P(None, 'gx', 'gy', 'gz')
- change: float32 [], replicated
The draws below stay inside these ranges and needn't reach their ends.
Inputs may be any that keep to these rules, and one draw needn't show every extreme that they name: pair_mask[t, k] equals pair_mask at tile t + offset(k) for the opposite offset 26 - k (periodic); pair_mask[t, 13] (the tile itself) is 1.
All inputs are finite; a program needn't handle non-finite values. No bound on the sum of `occupancy` on one device may be relied on, other than what follows from the above.
Results may differ from the reference program's by a relative error of at most 0.0003.
Values sent between devices are 32-bit elements; how exact they have to be, the bound alone decides.
A program may use at most 64 MiB of HBM per device.

```python
import math
import jax
import jax.numpy as jnp
from jax import lax

TILE = 128
HIST = 6
TILES_X = 1
TILES_Y = 2
TILES_Z = 2
BOX_X = 4
BOX_Y = 8
BOX_Z = 4


def draw_history(key, part):
    subkeys = jax.random.split(key, 6)
    full_shape = (6, BOX_X, BOX_Y, BOX_Z, TILE)
    block_counts = (BOX_X // TILES_X, BOX_Y // TILES_Y, BOX_Z // TILES_Z)
    frequency_table = jax.random.uniform(subkeys[4], block_counts, jnp.float32, 0.25, 2.2)
    index_x = jnp.arange(BOX_X) // TILES_X
    index_y = jnp.arange(BOX_Y) // TILES_Y
    index_z = jnp.arange(BOX_Z) // TILES_Z
    frequency = frequency_table[index_x[:, None, None], index_y[None, :, None], index_z[None, None, :]]
    step_index = jnp.arange(HIST, dtype=jnp.float32).reshape(HIST, 1, 1, 1, 1, 1)
    phase_angle = step_index * frequency[None, None, :, :, :, None]
    baseline = jax.random.normal(subkeys[0], full_shape, jnp.float32)
    cosine_part = jax.random.normal(subkeys[1], full_shape, jnp.float32)
    sine_part = jax.random.normal(subkeys[2], full_shape, jnp.float32)
    jitter = 0.2 * jax.random.normal(subkeys[3], (HIST,) + full_shape, jnp.float32)
    amplitude = jnp.exp(jax.random.uniform(subkeys[5], (1, 1, BOX_X, BOX_Y, BOX_Z, 1), jnp.float32, -0.7, 0.7))
    values = amplitude * (baseline[None] + jnp.cos(phase_angle) * cosine_part[None] + jnp.sin(phase_angle) * sine_part[None] + jitter)
    return jnp.clip(values, -12.0, 12.0).astype(jnp.float32)


def draw_pair_mask(key, part):
    coin_flips = jax.random.randint(key, (BOX_X, BOX_Y, BOX_Z, 27), 0, 4)
    one_side = (coin_flips > 0).astype(jnp.int32)
    columns = []
    for offset in range(27):
        along_x = offset // 9 - 1
        along_y = offset // 3 % 3 - 1
        along_z = offset % 3 - 1
        if offset == 13:
            columns.append(jnp.ones_like(one_side[..., offset]))
        else:
            mirror = jnp.roll(one_side[..., 26 - offset], shift=(-along_x, -along_y, -along_z), axis=(0, 1, 2))
            columns.append(one_side[..., offset] * mirror)
    return jnp.stack(columns, -1).astype(jnp.int32)


def with_ends(drawn, own_key, low, top_value):
    extent = drawn.shape
    index_at = [jax.random.randint(jax.random.fold_in(own_key, axis), (), 0, extent[axis]) for axis in range(len(extent))]
    drawn = drawn.at[tuple(index_at)].set(low)
    longest = extent.index(max(extent))
    index_at[longest] = (index_at[longest] + 1) % extent[longest]
    return drawn.at[tuple(index_at)].set(top_value)


def shard_levels(key, extent, cuts, least, high):
    loudness = 1.0
    for axis_at, blocks in cuts:
        draws = jax.random.uniform(jax.random.fold_in(jax.random.fold_in(key, 6), axis_at), (blocks,), jnp.float32, least / len(cuts), high / len(cuts))
        loudness = loudness * jnp.repeat(jnp.exp(draws), extent[axis_at] // blocks).reshape((-1,) + (1,) * (len(extent) - 1 - axis_at))
    return loudness


def scatter_about(key, dims, width, limit, pieces=(), held_as=jnp.bfloat16):
    result = jax.random.normal(key, dims, jnp.float32) * width
    if len(pieces) > 0:
        result = shard_levels(key, dims, pieces, -0.22, 0.18) * result
    return jnp.clip(result, min=-limit, max=limit).astype(held_as)


def setup_inputs(seed: int = 0) -> dict:
    key_of = jax.random.split(jax.random.key(seed), 7)
    fractions = jnp.clip(1.0 * jax.random.uniform(key_of[0], (3, BOX_X, BOX_Y, BOX_Z, TILE), jnp.float32) ** shard_levels(key_of[0], (3, BOX_X, BOX_Y, BOX_Z, TILE), ((1, 4), (2, 4), (3, 2)), -0.2, 0.2), 0.0, 1.0)
    polarizability = jnp.clip(jnp.exp(math.log(2.0) - 1.3862944 * jax.random.uniform(key_of[1], (BOX_X, BOX_Y, BOX_Z, TILE), jnp.float32) ** shard_levels(key_of[1], (BOX_X, BOX_Y, BOX_Z, TILE), ((0, 4), (1, 4), (2, 2)), -0.2, 0.2)), 0.5, 2.0)
    occupancy = with_ends((jax.random.randint(key_of[2], (BOX_X, BOX_Y, BOX_Z, TILE), 0, 8) < 7).astype(jnp.int32), jax.random.fold_in(key_of[2], 1), 0, 1)
    pair_mask = draw_pair_mask(jax.random.fold_in(key_of[6], 71), 0)
    perm_field = scatter_about(key_of[4], (6, BOX_X, BOX_Y, BOX_Z, TILE), 1.0, 6.0, ((1, 4), (2, 4), (3, 2)), jnp.float32)
    history = draw_history(jax.random.fold_in(key_of[6], 71), 0)
    return {"fractions": fractions, "polarizability": polarizability, "occupancy": occupancy, "pair_mask": pair_mask, "perm_field": perm_field, "history": history}


CELL_EDGE = 10.0
SOFTENING = 0.3
THOLE_DAMP = 0.39
RELAXATION = 0.7

def pair_field(target, source, moment, offset_vec, itself, allowed):
    displace = [(offset_vec[axis_num] + source[axis_num][:, None, :] - target[axis_num][:, :, None]) * CELL_EDGE for axis_num in range(3)]
    dist_sq = displace[0] * displace[0] + displace[1] * displace[1] + displace[2] * displace[2] + SOFTENING
    inv_cube = lax.rsqrt(dist_sq) / dist_sq
    thole_arg = dist_sq * jnp.sqrt(dist_sq) * lax.rsqrt(target[3][:, :, None] * source[3][:, None, :])
    damping = jnp.exp(-THOLE_DAMP * thole_arg)
    lambda_three = 1.0 - damping
    lambda_five = 1.0 - (1.0 + THOLE_DAMP * thole_arg) * damping
    slots = target.shape[-1]
    self_pair = jnp.logical_and(itself, jnp.eye(slots, dtype=bool))
    weight = jnp.where(self_pair, 0.0, allowed[:, None, None])
    radial = 3.0 * lambda_five * inv_cube / dist_sq * weight
    direct = lambda_three * inv_cube * weight
    fields = []
    for which_set in range(moment.shape[0] // 3):
        parts = [moment[3 * which_set + axis_num][:, None, :] for axis_num in range(3)]
        project = displace[0] * parts[0] + displace[1] * parts[1] + displace[2] * parts[2]
        for axis_num in range(3):
            fields.append(lax.optimization_barrier(jnp.sum(radial * project * displace[axis_num] - direct * parts[axis_num], axis=-1)))
    return jnp.stack(fields)

def slab_field(geometry_pad, moment_pad, allowed_slab, slab_index):
    width_y = geometry_pad.shape[2] - 2
    width_z = geometry_pad.shape[3] - 2
    slots = geometry_pad.shape[4]
    rows = moment_pad.shape[0]
    zero = jnp.zeros((), jnp.int32)
    one = jnp.ones((), jnp.int32)
    first_x = (jnp.asarray(slab_index) + 1).astype(jnp.int32)
    target = lax.dynamic_slice(geometry_pad, (zero, first_x, one, one, zero), (4, 1, width_y, width_z, slots)).reshape(4, width_y * width_z, slots)

    def offset_step(offset, summed):
        offset = jnp.asarray(offset).astype(jnp.int32)
        along_x = offset // 9 - 1
        along_y = offset // 3 % 3 - 1
        along_z = offset % 3 - 1
        starts = (zero, first_x + along_x, one + along_y, one + along_z, zero)
        source = lax.dynamic_slice(geometry_pad, starts, (4, 1, width_y, width_z, slots)).reshape(4, width_y * width_z, slots)
        moment = lax.dynamic_slice(moment_pad, starts, (rows, 1, width_y, width_z, slots)).reshape(rows, width_y * width_z, slots)
        allowed = lax.dynamic_index_in_dim(allowed_slab, offset, 2, keepdims=False).reshape(-1).astype(jnp.float32)
        offset_vec = jnp.stack([along_x, along_y, along_z]).astype(jnp.float32)
        return summed + pair_field(target, source, moment, offset_vec, offset == 13, allowed)
    summed = lax.fori_loop(0, 27, offset_step, jnp.zeros((rows, width_y * width_z, slots), jnp.float32))
    return summed.reshape(rows, width_y, width_z, slots)

def wrap_pad(values):
    return jnp.pad(values, ((0, 0), (1, 1), (1, 1), (1, 1), (0, 0)), mode='wrap')

def box_field(geometry_pad, moment, pair_mask):
    moment_pad = wrap_pad(moment)

    def one_slab(slab_index):
        allowed_slab = lax.dynamic_index_in_dim(pair_mask, slab_index, 0, keepdims=False)
        return slab_field(geometry_pad, moment_pad, allowed_slab, slab_index)
    slabs = lax.map(one_slab, jnp.arange(pair_mask.shape[0], dtype=jnp.int32))
    return jnp.moveaxis(slabs, 0, 1)

def fit_coefficients(gram_matrix):
    past_count = gram_matrix.shape[0] - 1
    gram_past = gram_matrix[:past_count, :past_count]
    gram_next = gram_matrix[:past_count, past_count]
    ridge_term = 0.001 * jnp.trace(gram_past) / past_count + 1.0
    factor = jnp.linalg.cholesky(gram_past + ridge_term * jnp.eye(past_count, dtype=jnp.float32))
    return jax.scipy.linalg.cho_solve((factor, True), gram_next)

def reference(fractions, polarizability, occupancy, pair_mask, perm_field, history):
    filled = occupancy.astype(jnp.float32)
    geometry = jnp.concatenate([fractions, polarizability[None]], 0)
    masked = history * filled
    flat_hist = masked.reshape(masked.shape[0], -1)
    gram_matrix = jnp.dot(flat_hist, flat_hist.T, precision=lax.Precision.HIGHEST)
    coeffs = fit_coefficients(gram_matrix)
    predicted = jnp.tensordot(coeffs, masked[1:], axes=1, precision=lax.Precision.HIGHEST)
    geometry_pad = wrap_pad(geometry)
    scaled = RELAXATION * filled * polarizability
    field_one = box_field(geometry_pad, predicted, pair_mask)
    dipole_one = (1.0 - RELAXATION) * predicted + scaled * (perm_field + field_one)
    field_two = box_field(geometry_pad, dipole_one, pair_mask)
    induced = (1.0 - RELAXATION) * dipole_one + scaled * (perm_field + field_two)
    update = induced - dipole_one
    change = jnp.sqrt(jnp.sum(update * update) / (jnp.sum(induced * induced) + 1.0))
    return (induced, change)
```

```python
import functools

import jax
import jax.numpy as jnp
from jax import lax
from jax.experimental import pallas as pl
from jax.experimental.pallas import tpu as pltpu
from jax.sharding import PartitionSpec as P

CELL_EDGE = 10.0
SOFTENING = 0.3
THOLE_DAMP = 0.39
RELAXATION = 0.7
MESH = pl.DeviceIdType.MESH
AXES = ("gx", "gy", "gz")
ROWS = 8
BLOCK = 32
STREAMS = 4


def halo_moves(devices, tiles):
    options = []
    for count, n in zip(devices, tiles):
        if count == 2 and n == 2:
            around = [(1, 0, 2, 2)]
        else:
            around = [(1, n - 1, 1, n + 1), (-1, 0, 1, n)]
        options.append([(0, 0, n, 0)] + around)
    return [
        (a, b, c) for a in options[0] for b in options[1] for c in options[2] if (a[0], b[0], c[0]) != (0, 0, 0)
    ]


def solve_fit(total, past, lane, pair_lane):
    def pick(a, b):
        index = pair_lane[(min(a, b), max(a, b))]
        return jnp.sum(jnp.where(lane == index, total, 0.0), axis=1, keepdims=True)

    diagonal = [pick(a, a) for a in range(past)]
    trace = diagonal[0]
    for value in diagonal[1:]:
        trace = trace + value
    ridge = 0.001 * trace / past + 1.0
    lower, inverse = {}, []
    for j in range(past):
        pivot = diagonal[j] + ridge
        for m in range(j):
            pivot = pivot - lower[j, m] * lower[j, m]
        inverse.append(1.0 / jnp.sqrt(pivot))
        for i in range(j + 1, past):
            value = pick(i, j)
            for m in range(j):
                value = value - lower[i, m] * lower[j, m]
            lower[i, j] = value * inverse[j]
    forward = []
    for i in range(past):
        value = pick(i, past)
        for m in range(i):
            value = value - lower[i, m] * forward[m]
        forward.append(value * inverse[i])
    coeffs = [None] * past
    for i in reversed(range(past)):
        value = forward[i]
        for m in range(i + 1, past):
            value = value - lower[m, i] * coeffs[m]
        coeffs[i] = value * inverse[i]
    return coeffs


def kernel(
    devices,
    frac_in, pol_in, occ_in, mask_in, perm_in, hist_in,
    out_ref, change_ref,
    frac_ref, pol_ref, occ_ref, mask_ref, perm_ref, hist_ref,
    geom, held_one, held_two, past_sets, own, spots, turns, links, weights, scaled, fixed, slots_a, slots_b,
    load_sem, send_all, recv_all, send_geom, recv_geom, send_one, recv_one, send_two, recv_two,
):
    tiles = tuple(frac_ref.shape[1:4])
    slots = frac_ref.shape[4]
    steps = hist_ref.shape[0]
    rows = hist_ref.shape[1]
    past = steps - 1
    total_devices = devices[0] * devices[1] * devices[2]
    at = [lax.axis_index(axis) for axis in AXES]
    me = (at[0] * devices[1] + at[1]) * devices[2] + at[2]
    moves = halo_moves(devices, tiles)
    lane = lax.broadcasted_iota(jnp.int32, (1, slots), 1)
    loads = [
        pltpu.make_async_copy(source, target, load_sem.at[number])
        for number, (source, target) in enumerate(
            (
                (hist_in, hist_ref), (occ_in, occ_ref), (frac_in, frac_ref),
                (pol_in, pol_ref), (perm_in, perm_ref), (mask_in, mask_ref),
            )
        )
    ]
    for load in loads:
        load.start()

    def each_other(act):
        def pair(step, carry):
            ahead = (step // devices[1], step % devices[1])
            first = []
            for axis in range(2):
                place = at[axis] + ahead[axis]
                first.append(jnp.where(place >= devices[axis], place - devices[axis], place))
            for shift in range(devices[2] - 1, -1, -1):
                last = at[2] + shift
                last = jnp.where(last >= devices[2], last - devices[2], last)
                if shift == 0:
                    @pl.when(step > 0)
                    def _():
                        act((first[0], first[1], last))
                else:
                    act((first[0], first[1], last))
            return carry

        lax.fori_loop(0, devices[0] * devices[1], pair, 0)

    barrier = pltpu.get_barrier_semaphore()

    each_other(
        lambda device: pl.semaphore_signal(barrier, inc=1, device_id=device, device_id_type=MESH)
    )
    for load in loads:
        load.wait()

    def everyone(index, held):
        def start(device):
            pltpu.make_async_remote_copy(
                src_ref=held.at[pl.ds(me, 1)],
                dst_ref=held.at[pl.ds(me, 1)],
                send_sem=send_all.at[index],
                recv_sem=recv_all.at[index],
                device_id=device,
                device_id_type=MESH,
            ).start()

        each_other(start)

    def everyone_wait(index, held):
        whole = pltpu.make_async_remote_copy(
            src_ref=held.at[pl.ds(0, total_devices - 1)],
            dst_ref=held.at[pl.ds(0, total_devices - 1)],
            send_sem=send_all.at[index],
            recv_sem=recv_all.at[index],
            device_id=(at[0], at[1], (at[2] + 1) % devices[2]),
            device_id_type=MESH,
        )
        whole.wait_send()
        whole.wait_recv()

    def halo(held, send, recv, moves=moves):
        copies = []
        for number, move in enumerate(moves):
            source = tuple(pl.ds(part[1], part[2]) for part in move)
            place = tuple(pl.ds(part[3], part[2]) for part in move)
            target = tuple((at[axis] + move[axis][0] + devices[axis]) % devices[axis] for axis in range(3))
            copies.append(
                pltpu.make_async_remote_copy(
                    src_ref=held.at[source],
                    dst_ref=held.at[place],
                    send_sem=send.at[number],
                    recv_sem=recv.at[number],
                    device_id=target,
                    device_id_type=MESH,
                )
            )
        return copies

    places = [(x, y, z) for x in range(tiles[0]) for y in range(tiles[1]) for z in range(tiles[2])]
    zero_row = jnp.zeros((1, slots), jnp.float32)
    spare = jnp.zeros((ROWS - rows, slots), jnp.float32)
    for t, (x, y, z) in enumerate(places):
        full = occ_ref[x, y, z, :].reshape(1, slots).astype(jnp.float32)
        pol = pol_ref[x, y, z, :].reshape(1, slots)
        scaled[t] = jnp.broadcast_to(RELAXATION * full * pol, (ROWS, slots))
        tile = jnp.concatenate(
            [frac_ref[c, x, y, z, :].reshape(1, slots) * CELL_EDGE for c in range(3)]
            + [lax.rsqrt(pol)] + [zero_row] * (ROWS - 4),
            axis=0,
        )
        geom[x, y, z] = tile
        for h in range(steps):
            moment = jnp.concatenate(
                [hist_ref[h, c, x, y, z, :].reshape(1, slots) for c in range(rows)], axis=0
            )
            past_sets[h, t] = jnp.concatenate([moment * full, spare], axis=0)
        fixed[t] = jnp.concatenate(
            [perm_ref[c, x, y, z, :].reshape(1, slots) for c in range(rows)] + [spare], axis=0
        )
    pair_lane = {}
    gram = zero_row
    for a in range(steps):
        for b in range(a, steps):
            product = past_sets[a, 0] * past_sets[b, 0]
            for t in range(1, len(places)):
                product = product + past_sets[a, t] * past_sets[b, t]
            value = jnp.sum(jnp.sum(product, axis=0, keepdims=True), axis=1, keepdims=True)
            pair_lane[(a, b)] = len(pair_lane)
            gram = jnp.where(lane == pair_lane[(a, b)], value, gram)
    slots_a[pl.ds(me, 1)] = gram.reshape(1, 1, slots)

    pl.semaphore_wait(barrier, total_devices - 1)
    geom_copies = halo(geom, send_geom, recv_geom)
    everyone(0, slots_a)
    for copy in geom_copies:
        copy.start()

    for move, copy in zip(moves, geom_copies):
        if move[0][0] == 0:
            copy.wait()

    wraps = tuple(n + 2 for n in tiles)
    row_of = lax.broadcasted_iota(jnp.int32, (ROWS, slots), 0)
    count = len(places)
    offsets = 27
    kinds = 5

    def wrap(value, size):
        return jnp.where(value < 0, value + size, value)

    def spot(t):
        x = t // (tiles[1] * tiles[2])
        y = t // tiles[2] % tiles[1]
        z = t % tiles[2]
        return (x, y, z)

    def settle(place, slot):
        tile = geom[slot[0], slot[1], slot[2]]
        shift = jnp.zeros((ROWS, slots), jnp.float32)
        for axis in range(3):
            corner = CELL_EDGE * (place[axis].astype(jnp.float32) - 0.5 * tiles[axis])
            shift = jnp.where(row_of == axis, corner, shift)
        tile = tile + shift
        spots[slot[0], slot[1], slot[2]] = tile
        one = jnp.ones((2, slots), jnp.float32)
        turns[0, slot[0], slot[1], slot[2]] = jnp.concatenate(
            [tile[0:3], tile[0:3], jnp.zeros((2, slots), jnp.float32)], axis=0
        )
        turns[1, slot[0], slot[1], slot[2]] = jnp.concatenate([one, tile[0:3], tile[0:3]], axis=0)

    def settle_plane(along_x):
        def one(step, carry):
            y, z = step // wraps[2] - 1, step % wraps[2] - 1
            place = (along_x, y, z)
            settle(place, tuple(wrap(place[i], wraps[i]) for i in range(3)))
            return carry

        lax.fori_loop(0, wraps[1] * wraps[2], one, 0)

    for x in range(tiles[0]):
        settle_plane(jnp.int32(x))
    for t, (x, y, z) in enumerate(places):
        for c in range(4):
            row = spots[x, y, z, c, :].reshape(1, slots)
            own[t, c] = jnp.broadcast_to(row, (slots, slots)).T

    def geometry(t, nine):
        along_x, along_y = nine // 3 - 1, nine % 3 - 1
        base = spot(t)
        for along_z in (-1, 0, 1):
            along = (along_x, along_y, along_z)
            k = nine * 3 + along_z + 1
            place = tuple(wrap(base[i] + along[i], wraps[i]) for i in range(3))
            source = [spots[place[0], place[1], place[2], pl.ds(c, 1), :] for c in range(4)]
            damp = source[3] * -THOLE_DAMP
            allowed = mask_ref[base[0], base[1], base[2], k].astype(jnp.float32)
            for first in range(0, slots, BLOCK):
                part = pl.ds(first, BLOCK)
                dx = source[0] - own[t, 0, part, :]
                dy = source[1] - own[t, 1, part, :]
                dz = source[2] - own[t, 2, part, :]
                square = dx * dx + dy * dy + dz * dz + SOFTENING
                root = lax.rsqrt(square)
                root_two = root * root
                cube = root_two * root * allowed
                arg = (square * square) * root * (damp * own[t, 3, part, :])
                fade = jnp.exp(arg)
                three = 1.0 - fade
                five = three + arg * fade
                direct = three * cube
                radial = five * cube * (3.0 * root_two)
                for number, value in ((0, radial), (2, direct)):
                    high = value.astype(jnp.bfloat16)
                    low = (value - high.astype(jnp.float32)).astype(jnp.bfloat16)
                    links[t, number, k, part, :] = high
                    links[t, number + 1, k, part, :] = low

    def same_x(step, carry):
        geometry(step // 3, 3 + step % 3)
        return carry

    def other_x(step, carry):
        part = step % 6
        geometry(step // 6, jnp.where(part < 3, part, part + 3))
        return carry

    lax.fori_loop(0, count * 3, same_x, 0)

    everyone_wait(0, slots_a)
    total = jnp.sum(slots_a[...], axis=0)
    coeffs = solve_fit(total, past, lane, pair_lane)
    for t, (x, y, z) in enumerate(places):
        value = coeffs[0] * past_sets[1, t]
        for h in range(1, past):
            value = value + coeffs[h] * past_sets[h + 1, t]
        held_one[x, y, z] = value
    one_copies = halo(held_one, send_one, recv_one)
    for copy in one_copies:
        copy.start()
    for move, copy in zip(moves, geom_copies):
        if move[0][0] != 0:
            copy.wait()
    settle_plane(jnp.int32(-1))
    settle_plane(jnp.int32(tiles[0]))
    lax.fori_loop(0, count * 6, other_x, 0)
    off_diagonal = lax.broadcasted_iota(jnp.int32, (slots, slots), 0) != lax.broadcasted_iota(
        jnp.int32, (slots, slots), 1
    )
    empty = jnp.zeros((slots, slots), jnp.bfloat16)
    for t in range(count):
        for number in range(STREAMS):
            own_link = links[t, number, 13].astype(jnp.float32)
            links[t, number, 13] = jnp.where(off_diagonal, own_link, 0.0).astype(jnp.bfloat16)
            links[t, number, offsets] = empty
    spread = wraps[0] * wraps[1] * wraps[2]
    weights[spread] = empty

    def weigh(held):
        def one(step, carry):
            slot = (step // (wraps[1] * wraps[2]), step // wraps[2] % wraps[1], step % wraps[2])
            moment = held[slot[0], slot[1], slot[2]]
            along = moment * turns[0, slot[0], slot[1], slot[2]]
            first = jnp.sum(jnp.where(row_of < 3, along, 0.0), axis=0, keepdims=True)
            second = jnp.sum(jnp.where(row_of < 3, 0.0, along), axis=0, keepdims=True)
            which = jnp.logical_or(row_of == 0, jnp.logical_and(row_of >= 2, row_of < 5))
            both = jnp.where(which, first, second) * turns[1, slot[0], slot[1], slot[2]]
            parts = [spots[slot[0], slot[1], slot[2], pl.ds(c, 1), :] * moment for c in range(3)]
            value = jnp.concatenate(parts + [moment, both], axis=0)
            high = value.astype(jnp.bfloat16).astype(jnp.float32)
            rest = value - high
            middle = rest.astype(jnp.bfloat16).astype(jnp.float32)
            pad = jnp.zeros((slots - 3 * kinds * ROWS, slots), jnp.float32)
            weights[step] = jnp.concatenate([high, middle, rest - middle, pad], axis=0).astype(jnp.bfloat16)
            return carry

        lax.fori_loop(0, spread, one, 0)

    def field_of(t, sums):
        x, y, z = spot(t)
        radial = (sums[0:slots] + sums[slots : 2 * slots]).T
        direct = (sums[2 * slots : 3 * slots] + sums[3 * slots : 4 * slots]).T

        def tile(value, kind):
            total = value[kind * ROWS : (kind + 1) * ROWS]
            for level in (1, 2):
                first = (level * kinds + kind) * ROWS
                total = total + value[first : first + ROWS]
            return total

        turn = turns[0, x, y, z]
        plain = tile(radial, 3)
        both = tile(radial, 4)
        inner = []
        for c in range(3):
            along = (tile(radial, c) - spots[x, y, z, pl.ds(c, 1), :] * plain) * turn
            first = jnp.sum(jnp.where(row_of < 3, along, 0.0), axis=0, keepdims=True)
            second = jnp.sum(jnp.where(row_of < 3, 0.0, along), axis=0, keepdims=True)
            inner.append((first, second))
        inner = jnp.concatenate(
            [inner[c][0] for c in range(3)] + [inner[c][1] for c in range(3)] + [zero_row, zero_row], axis=0
        )
        lifted = jnp.concatenate([both[2:8], zero_row, zero_row], axis=0)
        dots = jnp.where(row_of < 3, both[0:1], both[1:2])
        return lifted - dots * turn - inner - tile(direct, 3)

    def slot_at(base, k):
        along = (k // 9 - 1, k // 3 % 3 - 1, k % 3 - 1)
        slot = [wrap(base[i] + along[i], wraps[i]) for i in range(3)]
        return (slot[0] * wraps[1] + slot[1]) * wraps[2] + slot[2]

    def field(t):
        base = spot(t)
        sums = jnp.zeros((STREAMS * slots, slots), jnp.float32)
        for pair in range(0, offsets, 2):
            left = jnp.concatenate(
                [
                    jnp.concatenate([links[t, number, pair], links[t, number, pair + 1]], axis=1)
                    for number in range(STREAMS)
                ],
                axis=0,
            )
            behind = spread if pair + 1 == offsets else slot_at(base, pair + 1)
            right = jnp.concatenate([weights[slot_at(base, pair)], weights[behind]], axis=1)
            sums = sums + lax.dot_general(
                left, right, (((1,), (1,)), ((), ())), preferred_element_type=jnp.float32
            )
        return field_of(t, sums)

    for copy in one_copies:
        copy.wait()
    weigh(held_one)

    def first_pass(t, carry):
        x, y, z = spot(t)
        held_two[x, y, z] = (1.0 - RELAXATION) * held_one[x, y, z] + scaled[t] * (fixed[t] + field(t))
        return carry

    lax.fori_loop(0, count, first_pass, 0)
    two_copies = halo(held_two, send_two, recv_two)
    for copy in two_copies:
        copy.start()
    for copy in two_copies:
        copy.wait()
    weigh(held_two)

    def second_pass(t, carry):
        changed, size = carry
        x, y, z = spot(t)
        before = held_two[x, y, z]
        after = (1.0 - RELAXATION) * before + scaled[t] * (fixed[t] + field(t))
        for c in range(rows):
            out_ref[c, x, y, z, :] = after[c]
        changed = changed + (after - before) * (after - before)
        return changed, size + after * after

    nothing = jnp.zeros((ROWS, slots), jnp.float32)
    changed, size = lax.fori_loop(0, count, second_pass, (nothing, nothing))

    def all_of(value):
        return jnp.sum(jnp.sum(value, axis=0, keepdims=True), axis=1, keepdims=True)

    pair = jnp.where(lane == 0, all_of(changed), jnp.where(lane == 1, all_of(size), 0.0))
    slots_b[pl.ds(me, 1)] = pair.reshape(1, 1, slots)
    everyone(1, slots_b)
    everyone_wait(1, slots_b)
    pair = jnp.sum(slots_b[...], axis=0)
    above = jnp.sum(jnp.where(lane == 0, pair, 0.0), axis=1, keepdims=True)
    below = jnp.sum(jnp.where(lane == 1, pair, 0.0), axis=1, keepdims=True)
    change_ref[...] = jnp.broadcast_to(jnp.sqrt(above / (below + 1.0)), (1, slots))


def solution(mesh):
    devices = tuple(mesh.shape[axis] for axis in AXES)
    total_devices = devices[0] * devices[1] * devices[2]

    def on_device(fractions, polarizability, occupancy, pair_mask, perm_field, history):
        tiles = fractions.shape[1:4]
        slots = fractions.shape[4]
        count = tiles[0] * tiles[1] * tiles[2]
        wraps = tuple(n + 2 for n in tiles)
        moves = len(halo_moves(devices, tiles))
        rows = history.shape[1]
        vmem = pl.BlockSpec(memory_space=pltpu.VMEM)
        f32 = jnp.float32
        induced, change = pl.pallas_call(
            functools.partial(kernel, devices),
            out_shape=(
                jax.ShapeDtypeStruct(perm_field.shape, f32),
                jax.ShapeDtypeStruct((1, slots), f32),
            ),
            in_specs=[pl.BlockSpec(memory_space=pltpu.HBM)] * 6,
            out_specs=(vmem, vmem),
            scratch_shapes=[
                pltpu.VMEM(fractions.shape, f32),
                pltpu.VMEM(polarizability.shape, f32),
                pltpu.VMEM(occupancy.shape, jnp.int32),
                pltpu.SMEM(pair_mask.shape, jnp.int32),
                pltpu.VMEM(perm_field.shape, f32),
                pltpu.VMEM(history.shape, f32),
                pltpu.VMEM(wraps + (ROWS, slots), f32),
                pltpu.VMEM(wraps + (ROWS, slots), f32),
                pltpu.VMEM(wraps + (ROWS, slots), f32),
                pltpu.VMEM((history.shape[0], count, ROWS, slots), f32),
                pltpu.VMEM((count, 4, slots, slots), f32),
                pltpu.VMEM(wraps + (ROWS, slots), f32),
                pltpu.VMEM((2,) + wraps + (ROWS, slots), f32),
                pltpu.VMEM((count, STREAMS, 28, slots, slots), jnp.bfloat16),
                pltpu.VMEM((wraps[0] * wraps[1] * wraps[2] + 1, slots, slots), jnp.bfloat16),
                pltpu.VMEM((count, ROWS, slots), f32),
                pltpu.VMEM((count, ROWS, slots), f32),
                pltpu.VMEM((total_devices, 1, slots), f32),
                pltpu.VMEM((total_devices, 1, slots), f32),
                pltpu.SemaphoreType.DMA((6,)),
                pltpu.SemaphoreType.DMA((2,)),
                pltpu.SemaphoreType.DMA((2,)),
            ]
            + [pltpu.SemaphoreType.DMA((moves,))] * 6,
            compiler_params=pltpu.CompilerParams(
                collective_id=0, has_side_effects=True, vmem_limit_bytes=67043328
            ),
        )(fractions, polarizability, occupancy, pair_mask, perm_field, history)
        return induced, change[0, 0]

    in_specs = (
        P(None, "gx", "gy", "gz", None),
        P("gx", "gy", "gz", None),
        P("gx", "gy", "gz", None),
        P("gx", "gy", "gz", None),
        P(None, "gx", "gy", "gz", None),
        P(None, None, "gx", "gy", "gz", None),
    )
    out_specs = (P(None, "gx", "gy", "gz", None), P())
    return jax.shard_map(
        on_device, mesh=mesh, in_specs=in_specs, out_specs=out_specs, check_vma=False
    )
```

```python
import functools

import jax
import jax.numpy as jnp
from jax import lax
from jax.experimental import pallas as pl
from jax.experimental.pallas import tpu as pltpu
from jax.sharding import PartitionSpec as P

CELL_EDGE = 10.0
SOFTENING = 0.3
THOLE_DAMP = 0.39
RELAXATION = 0.7
MESH = pl.DeviceIdType.MESH
AXES = ("gx", "gy", "gz")
ROWS = 8
BLOCK = 32
STREAMS = 4
SPREAD = 128
SPREAD_LOW = 96
SPREAD_PLAIN = 32


def halo_moves(devices, tiles):
    options = []
    for count, n in zip(devices, tiles):
        if count == 2 and n == 2:
            around = [(1, 0, 2, 2)]
        else:
            around = [(1, n - 1, 1, n + 1), (-1, 0, 1, n)]
        options.append([(0, 0, n, 0)] + around)
    return [
        (a, b, c) for a in options[0] for b in options[1] for c in options[2] if (a[0], b[0], c[0]) != (0, 0, 0)
    ]


def solve_fit(total, past, lane, pair_lane):
    def pick(a, b):
        index = pair_lane[(min(a, b), max(a, b))]
        return jnp.sum(jnp.where(lane == index, total, 0.0), axis=1, keepdims=True)

    diagonal = [pick(a, a) for a in range(past)]
    trace = diagonal[0]
    for value in diagonal[1:]:
        trace = trace + value
    ridge = 0.001 * trace / past + 1.0
    lower, inverse = {}, []
    for j in range(past):
        pivot = diagonal[j] + ridge
        for m in range(j):
            pivot = pivot - lower[j, m] * lower[j, m]
        inverse.append(1.0 / jnp.sqrt(pivot))
        for i in range(j + 1, past):
            value = pick(i, j)
            for m in range(j):
                value = value - lower[i, m] * lower[j, m]
            lower[i, j] = value * inverse[j]
    forward = []
    for i in range(past):
        value = pick(i, past)
        for m in range(i):
            value = value - lower[i, m] * forward[m]
        forward.append(value * inverse[i])
    coeffs = [None] * past
    for i in reversed(range(past)):
        value = forward[i]
        for m in range(i + 1, past):
            value = value - lower[m, i] * coeffs[m]
        coeffs[i] = value * inverse[i]
    return coeffs


def kernel(
    devices,
    frac_in, pol_in, occ_in, mask_in, perm_in, hist_in,
    out_ref, change_ref,
    frac_ref, pol_ref, occ_ref, mask_ref, perm_ref, hist_ref,
    geom, held_one, held_two, past_sets, spots, columns, turns, links, weights,
    partial_main, partial_rest, partial_plain, scaled, fixed, slots_a, slots_b,
    load_sem, send_all, recv_all, send_geom, recv_geom, send_one, recv_one, send_two, recv_two,
):
    tiles = tuple(frac_ref.shape[1:4])
    slots = frac_ref.shape[4]
    steps = hist_ref.shape[0]
    rows = hist_ref.shape[1]
    past = steps - 1
    total_devices = devices[0] * devices[1] * devices[2]
    at = [lax.axis_index(axis) for axis in AXES]
    me = (at[0] * devices[1] + at[1]) * devices[2] + at[2]
    moves = halo_moves(devices, tiles)
    lane = lax.broadcasted_iota(jnp.int32, (1, slots), 1)
    loads = [
        pltpu.make_async_copy(source, target, load_sem.at[number])
        for number, (source, target) in enumerate(
            (
                (hist_in, hist_ref), (occ_in, occ_ref), (frac_in, frac_ref),
                (pol_in, pol_ref), (perm_in, perm_ref), (mask_in, mask_ref),
            )
        )
    ]
    for load in loads:
        load.start()

    def each_other(act):
        def pair(step, carry):
            ahead = (step // devices[1], step % devices[1])
            first = []
            for axis in range(2):
                place = at[axis] + ahead[axis]
                first.append(jnp.where(place >= devices[axis], place - devices[axis], place))
            for shift in range(devices[2] - 1, -1, -1):
                last = at[2] + shift
                last = jnp.where(last >= devices[2], last - devices[2], last)
                if shift == 0:
                    @pl.when(step > 0)
                    def _():
                        act((first[0], first[1], last))
                else:
                    act((first[0], first[1], last))
            return carry

        lax.fori_loop(0, devices[0] * devices[1], pair, 0)

    barrier = pltpu.get_barrier_semaphore()

    each_other(
        lambda device: pl.semaphore_signal(barrier, inc=1, device_id=device, device_id_type=MESH)
    )
    for load in loads:
        load.wait()

    def everyone(index, held):
        def start(device):
            pltpu.make_async_remote_copy(
                src_ref=held.at[pl.ds(me, 1)],
                dst_ref=held.at[pl.ds(me, 1)],
                send_sem=send_all.at[index],
                recv_sem=recv_all.at[index],
                device_id=device,
                device_id_type=MESH,
            ).start()

        each_other(start)

    def everyone_wait(index, held):
        whole = pltpu.make_async_remote_copy(
            src_ref=held.at[pl.ds(0, total_devices - 1)],
            dst_ref=held.at[pl.ds(0, total_devices - 1)],
            send_sem=send_all.at[index],
            recv_sem=recv_all.at[index],
            device_id=(at[0], at[1], (at[2] + 1) % devices[2]),
            device_id_type=MESH,
        )
        whole.wait_send()
        whole.wait_recv()

    def halo(held, send, recv, depth):
        copies = []
        for number, move in enumerate(moves):
            source = tuple(pl.ds(part[1], part[2]) for part in move)
            place = tuple(pl.ds(part[3], part[2]) for part in move)
            target = tuple((at[axis] + move[axis][0] + devices[axis]) % devices[axis] for axis in range(3))
            copies.append(
                pltpu.make_async_remote_copy(
                    src_ref=held.at[source + (pl.ds(0, depth),)],
                    dst_ref=held.at[place + (pl.ds(0, depth),)],
                    send_sem=send.at[number],
                    recv_sem=recv.at[number],
                    device_id=target,
                    device_id_type=MESH,
                )
            )
        return copies

    places = [(x, y, z) for x in range(tiles[0]) for y in range(tiles[1]) for z in range(tiles[2])]
    zero_row = jnp.zeros((1, slots), jnp.float32)
    spare = jnp.zeros((ROWS - rows, slots), jnp.float32)
    for t, (x, y, z) in enumerate(places):
        full = occ_ref[x, y, z, :].reshape(1, slots).astype(jnp.float32)
        pol = pol_ref[x, y, z, :].reshape(1, slots)
        scaled[t] = jnp.broadcast_to(RELAXATION * full * pol, (ROWS, slots))
        tile = jnp.concatenate(
            [frac_ref[c, x, y, z, :].reshape(1, slots) * CELL_EDGE for c in range(3)]
            + [lax.rsqrt(pol)] + [zero_row] * (ROWS - 4),
            axis=0,
        )
        geom[x, y, z] = tile
        for h in range(steps):
            moment = jnp.concatenate(
                [hist_ref[h, c, x, y, z, :].reshape(1, slots) for c in range(rows)], axis=0
            )
            past_sets[h, t] = jnp.concatenate([moment * full, spare], axis=0)
        fixed[t] = jnp.concatenate(
            [perm_ref[c, x, y, z, :].reshape(1, slots) for c in range(rows)] + [spare], axis=0
        )
    pair_lane = {}
    gram = zero_row
    for a in range(steps):
        for b in range(a, steps):
            product = past_sets[a, 0] * past_sets[b, 0]
            for t in range(1, len(places)):
                product = product + past_sets[a, t] * past_sets[b, t]
            value = jnp.sum(jnp.sum(product, axis=0, keepdims=True), axis=1, keepdims=True)
            pair_lane[(a, b)] = len(pair_lane)
            gram = jnp.where(lane == pair_lane[(a, b)], value, gram)
    slots_a[pl.ds(me, 1)] = gram.reshape(1, 1, slots)

    pl.semaphore_wait(barrier, total_devices - 1)
    geom_copies = halo(geom, send_geom, recv_geom, 4)
    everyone(0, slots_a)
    for copy in geom_copies:
        copy.start()

    wraps = tuple(n + 2 for n in tiles)
    row_of = lax.broadcasted_iota(jnp.int32, (ROWS, slots), 0)
    count = len(places)
    wide = tiles[2] * slots
    levels = list(range(tiles[2])) + [-1, tiles[2]]

    def wrap(value, size):
        return jnp.where(value < 0, value + size, value)

    def settle(place, slot):
        tile = geom[slot[0], slot[1], slot[2]]
        shift = jnp.zeros((ROWS, slots), jnp.float32)
        for axis in range(3):
            corner = CELL_EDGE * (jnp.asarray(place[axis], jnp.float32) - 0.5 * tiles[axis])
            shift = jnp.where(row_of == axis, corner, shift)
        tile = tile + shift
        spots[slot[0], slot[1], slot[2]] = tile
        columns[slot[0], slot[1], slot[2]] = tile.T
        one = jnp.ones((2, slots), jnp.float32)
        turns[0, slot[0], slot[1], slot[2]] = jnp.concatenate(
            [tile[0:3], tile[0:3], jnp.zeros((2, slots), jnp.float32)], axis=0
        )
        turns[1, slot[0], slot[1], slot[2]] = jnp.concatenate([one, tile[0:3], tile[0:3]], axis=0)

    def settle_all(xs, ys, zs):
        def one(step, carry):
            x = step + xs[0]
            for y in ys:
                for z in zs:
                    settle((x, y, z), (wrap(x, wraps[0]), y % wraps[1], z % wraps[2]))
            return carry

        lax.fori_loop(0, len(xs), one, 0)

    near_y, far_y = list(range(tiles[1])), [-1, tiles[1]]
    every_x = list(range(-1, tiles[0] + 1))
    own_z, side_z = list(range(tiles[2])), [-1, tiles[2]]

    def geometry(x, y, along_x, along_y, zs):
        nine = (along_x + 1) * 3 + along_y + 1
        line = x * tiles[1] + y
        slot_x, slot_y = wrap(x + along_x, wraps[0]), wrap(y + along_y, wraps[1])
        for level in zs:
            spot_at = levels.index(level)
            slot_z = level % wraps[2]
            takers = [z for z in range(tiles[2]) if abs(level - z) <= 1]
            fixed_rows = [[spots[x, y, z, pl.ds(c, 1), :] for c in range(4)] for z in takers]
            allowed = [mask_ref[x, y, z, nine * 3 + level - z + 1].astype(jnp.float32) for z in takers]
            damps = [own_row[3] * -THOLE_DAMP for own_row in fixed_rows]
            for first in range(0, slots, BLOCK):
                part = pl.ds(first, BLOCK)
                moving = [
                    jnp.broadcast_to(columns[slot_x, slot_y, slot_z, part, c : c + 1], (BLOCK, slots))
                    for c in range(4)
                ]
                for z, own_row, damp, allow in zip(takers, fixed_rows, damps, allowed):
                    dx = moving[0] - own_row[0]
                    dy = moving[1] - own_row[1]
                    dz = moving[2] - own_row[2]
                    square = dx * dx + dy * dy + dz * dz + SOFTENING
                    root = lax.rsqrt(square)
                    root_two = root * root
                    cube = root_two * root * allow
                    arg = (square * square) * root * (damp * moving[3])
                    fade = jnp.exp(arg)
                    three = 1.0 - fade
                    five = three + arg * fade
                    direct = three * cube
                    radial = five * cube * (3.0 * root_two)
                    for number, value in ((0, radial), (2, direct)):
                        high = value.astype(jnp.bfloat16)
                        low = (value - high.astype(jnp.float32)).astype(jnp.bfloat16)
                        links[line, nine, number, spot_at, part, z * slots : (z + 1) * slots] = high
                        links[line, nine, number + 1, spot_at, part, z * slots : (z + 1) * slots] = low

    def geometry_near(along_xs, zs):
        def one(step, carry):
            x = step % tiles[0]
            y = step // tiles[0] % tiles[1]
            to_y = step // (tiles[0] * tiles[1]) % tiles[1]
            along_x = step // (tiles[0] * tiles[1] * tiles[1]) + along_xs[0]
            geometry(x, y, along_x, to_y - y, zs)
            return carry

        lax.fori_loop(0, tiles[0] * tiles[1] * tiles[1] * len(along_xs), one, 0)

    def geometry_far():
        def one(step, carry):
            x = step % tiles[0]
            side = step // tiles[0] % 2
            along_x = step // (2 * tiles[0]) - 1
            geometry(x, side * (tiles[1] - 1), along_x, 2 * side - 1, levels)
            return carry

        lax.fori_loop(0, 6 * tiles[0], one, 0)

    settle_all([x for x in every_x if 0 <= x < tiles[0]], near_y, own_z)
    geometry_near([0], own_z)
    off_diagonal = lax.broadcasted_iota(jnp.int32, (slots, slots), 0) != lax.broadcasted_iota(
        jnp.int32, (slots, slots), 1
    )
    for x, y, z in places:
        lanes = slice(z * slots, (z + 1) * slots)
        for number in range(STREAMS):
            link = links[x * tiles[1] + y, 4, number, levels.index(z), :, lanes].astype(jnp.float32)
            links[x * tiles[1] + y, 4, number, levels.index(z), :, lanes] = jnp.where(
                off_diagonal, link, 0.0
            ).astype(jnp.bfloat16)

    for move, copy in zip(moves, geom_copies):
        if move[1][0] == 0:
            copy.wait()
    settle_all([x for x in every_x if 0 <= x < tiles[0]], near_y, side_z)
    settle_all([-1], near_y, levels)
    settle_all([tiles[0]], near_y, levels)
    geometry_near([0], side_z)
    geometry_near([-1], levels)

    everyone_wait(0, slots_a)
    total = jnp.sum(slots_a[...], axis=0)
    coeffs = solve_fit(total, past, lane, pair_lane)
    for t, (x, y, z) in enumerate(places):
        value = coeffs[0] * past_sets[1, t]
        for h in range(1, past):
            value = value + coeffs[h] * past_sets[h + 1, t]
        held_one[x, y, z] = value
    one_copies = halo(held_one, send_one, recv_one, rows)
    for copy in one_copies:
        copy.start()
    geometry_near([1], levels)
    for move, copy in zip(moves, geom_copies):
        if move[1][0] != 0:
            copy.wait()
    settle_all(every_x, far_y, levels)
    geometry_far()

    kinds = 5

    def weigh(held, ys):
        def one(step, carry):
            x = wrap(step - 1, wraps[0])
            for y in ys:
                for z in range(wraps[2]):
                    slot = (x, y % wraps[1], z)
                    moment = jnp.where(row_of < rows, held[slot], 0.0)
                    along = moment * turns[(0,) + slot]
                    first = jnp.sum(jnp.where(row_of < 3, along, 0.0), axis=0, keepdims=True)
                    second = jnp.sum(jnp.where(row_of < 3, 0.0, along), axis=0, keepdims=True)
                    which = jnp.logical_or(row_of == 0, jnp.logical_and(row_of >= 2, row_of < 5))
                    both = jnp.where(which, first, second) * turns[(1,) + slot]
                    tiles_of = [moment, both] + [
                        spots[slot + (pl.ds(c, 1), slice(None))] * moment for c in range(3)
                    ]
                    parts = [[], [], []]
                    for value in tiles_of:
                        for level in range(3):
                            piece = value.astype(jnp.bfloat16).astype(jnp.float32)
                            parts[level].append(piece)
                            value = value - piece
                    order = [parts[0][0], parts[1][0], parts[2][0]]
                    for level in range(3):
                        order = order + parts[level][1:]
                    order.append(jnp.zeros((ROWS, slots), jnp.float32))
                    weights[slot] = jnp.concatenate(order, axis=0).astype(jnp.bfloat16)
            return carry

        lax.fori_loop(0, wraps[0], one, 0)

    def products(line, visits):
        width = 2 * slots if len(levels) % 2 == 0 else slots
        main = jnp.zeros((SPREAD, wide), jnp.float32)
        rest = jnp.zeros((SPREAD_LOW, wide), jnp.float32)
        plain = jnp.zeros((SPREAD_PLAIN, wide), jnp.float32)
        per = width // slots
        blank = jnp.zeros((slots, slots), jnp.bfloat16)
        for nine, slot_x, slot_y in visits:
            for start in range(0, len(levels), per):
                chunk = range(start, start + per)
                left = jnp.concatenate(
                    [weights[slot_x, slot_y, levels[i] % wraps[2]] for i in chunk], axis=1
                )

                def matrix(number):
                    lines = []
                    for i in chunk:
                        lines.append(
                            jnp.concatenate(
                                [
                                    links[line, nine, number, i, :, z * slots : (z + 1) * slots]
                                    if abs(levels[i] - z) <= 1
                                    else blank
                                    for z in range(tiles[2])
                                ],
                                axis=1,
                            )
                        )
                    return jnp.concatenate(lines, axis=0)

                def times(values, number):
                    return jnp.dot(values, matrix(number), preferred_element_type=jnp.float32)

                main = main + times(left, 0)
                rest = rest + times(left[0:SPREAD_LOW], 1)
                plain = plain + times(left[0:SPREAD_PLAIN], 2)
                plain = plain + times(left[0:SPREAD_PLAIN], 3)
        return main, rest, plain

    def near_products(x, y):
        visits = [
            ((along + 1) * 3 + to_y - y + 1, wrap(x + along, wraps[0]), to_y)
            for along in (-1, 0, 1)
            for to_y in range(tiles[1])
        ]
        return products(x * tiles[1] + y, visits)

    def far_products(x, y, side):
        visits = [
            ((along + 1) * 3 + 2 * side, wrap(x + along, wraps[0]), wrap((tiles[1] + 1) * side - 1, wraps[1]))
            for along in (-1, 0, 1)
        ]
        return products(x * tiles[1] + y, visits)

    def keep_near(step, carry):
        x, y = step // tiles[1], step % tiles[1]
        main, rest, plain = near_products(x, y)
        partial_main[step] = main
        partial_rest[step] = rest
        partial_plain[step] = plain
        return carry

    def field_of(x, y, main, rest, plain):
        def tile(value, index):
            return value[index * ROWS : (index + 1) * ROWS]

        def both_sum(first):
            total = tile(main, first[0]) + tile(rest, first[0])
            for index in first[1:]:
                total = total + tile(main, index)
                if (index + 1) * ROWS <= SPREAD_LOW:
                    total = total + tile(rest, index)
            return total

        moment = both_sum((0, 1, 2))
        both = both_sum((3, 7, 11))
        lifts = [both_sum((4 + c, 8 + c, 12 + c)) for c in range(3)]
        straight = tile(plain, 0) + tile(plain, 1) + tile(plain, 2)
        result = []
        for z in range(tiles[2]):
            lanes = slice(z * slots, (z + 1) * slots)
            turn = turns[0, x, y, z]
            inner = []
            for c in range(3):
                along = (lifts[c][:, lanes] - spots[x, y, z, pl.ds(c, 1), :] * moment[:, lanes]) * turn
                first = jnp.sum(jnp.where(row_of < 3, along, 0.0), axis=0, keepdims=True)
                second = jnp.sum(jnp.where(row_of < 3, 0.0, along), axis=0, keepdims=True)
                inner.append((first, second))
            inner = jnp.concatenate(
                [inner[c][0] for c in range(3)] + [inner[c][1] for c in range(3)] + [zero_row, zero_row], axis=0
            )
            lifted = jnp.concatenate([both[2:8, lanes], zero_row, zero_row], axis=0)
            dots = jnp.where(row_of < 3, both[0:1, lanes], both[1:2, lanes])
            result.append(lifted - dots * turn - inner - straight[:, lanes])
        return result

    lines = tiles[0] * tiles[1]

    def field(step, held, act):
        x, y = step // tiles[1], step % tiles[1]
        main, rest, plain = partial_main[step], partial_rest[step], partial_plain[step]
        for side in range(2):
            if tiles[1] == 1:
                more = far_products(x, y, side)
                main, rest, plain = main + more[0], rest + more[1], plain + more[2]
        if tiles[1] > 1:
            side = y // (tiles[1] - 1)
            more = far_products(x, y, side)
            keep = jnp.logical_or(y == 0, y == tiles[1] - 1).astype(jnp.float32)
            if tiles[1] > 2:
                more = tuple(jnp.where(keep > 0.5, value, 0.0) for value in more)
            main, rest, plain = main + more[0], rest + more[1], plain + more[2]
        fields = field_of(x, y, main, rest, plain)
        for z in range(tiles[2]):
            t = step * tiles[2] + z
            act(x, y, z, t, (1.0 - RELAXATION) * held[x, y, z] + scaled[t] * (fixed[t] + fields[z]))

    def sweep(held, copies, act):
        for move, copy in zip(moves, copies):
            if move[1][0] == 0:
                copy.wait()
        weigh(held, near_y)
        lax.fori_loop(0, lines, keep_near, 0)
        for move, copy in zip(moves, copies):
            if move[1][0] != 0:
                copy.wait()
        weigh(held, far_y)

        def one(step, carry):
            field(step, held, act)
            return carry

        lax.fori_loop(0, lines, one, 0)

    def first_act(x, y, z, t, value):
        held_two[x, y, z] = value

    sweep(held_one, one_copies, first_act)
    two_copies = halo(held_two, send_two, recv_two, rows)
    for copy in two_copies:
        copy.start()

    def second_act(x, y, z, t, value):
        held_one[x, y, z] = value

    sweep(held_two, two_copies, second_act)
    changed = jnp.zeros((ROWS, slots), jnp.float32)
    size = jnp.zeros((ROWS, slots), jnp.float32)
    for t, (x, y, z) in enumerate(places):
        before, after = held_two[x, y, z], held_one[x, y, z]
        for c in range(rows):
            out_ref[c, x, y, z, :] = after[c]
        changed = changed + (after - before) * (after - before)
        size = size + after * after

    def all_of(value):
        return jnp.sum(jnp.sum(value, axis=0, keepdims=True), axis=1, keepdims=True)

    pair = jnp.where(lane == 0, all_of(changed), jnp.where(lane == 1, all_of(size), 0.0))
    slots_b[pl.ds(me, 1)] = pair.reshape(1, 1, slots)
    everyone(1, slots_b)
    everyone_wait(1, slots_b)
    pair = jnp.sum(slots_b[...], axis=0)
    above = jnp.sum(jnp.where(lane == 0, pair, 0.0), axis=1, keepdims=True)
    below = jnp.sum(jnp.where(lane == 1, pair, 0.0), axis=1, keepdims=True)
    change_ref[...] = jnp.broadcast_to(jnp.sqrt(above / (below + 1.0)), (1, slots))


def solution(mesh):
    devices = tuple(mesh.shape[axis] for axis in AXES)
    total_devices = devices[0] * devices[1] * devices[2]

    def on_device(fractions, polarizability, occupancy, pair_mask, perm_field, history):
        tiles = fractions.shape[1:4]
        slots = fractions.shape[4]
        count = tiles[0] * tiles[1] * tiles[2]
        lines = tiles[0] * tiles[1]
        wraps = tuple(n + 2 for n in tiles)
        moves = len(halo_moves(devices, tiles))
        rows = history.shape[1]
        vmem = pl.BlockSpec(memory_space=pltpu.VMEM)
        f32 = jnp.float32
        induced, change = pl.pallas_call(
            functools.partial(kernel, devices),
            out_shape=(
                jax.ShapeDtypeStruct(perm_field.shape, f32),
                jax.ShapeDtypeStruct((1, slots), f32),
            ),
            in_specs=[pl.BlockSpec(memory_space=pltpu.HBM)] * 6,
            out_specs=(vmem, vmem),
            scratch_shapes=[
                pltpu.VMEM(fractions.shape, f32),
                pltpu.VMEM(polarizability.shape, f32),
                pltpu.VMEM(occupancy.shape, jnp.int32),
                pltpu.SMEM(pair_mask.shape, jnp.int32),
                pltpu.VMEM(perm_field.shape, f32),
                pltpu.VMEM(history.shape, f32),
                pltpu.VMEM(wraps + (ROWS, slots), f32),
                pltpu.VMEM(wraps + (ROWS, slots), f32),
                pltpu.VMEM(wraps + (ROWS, slots), f32),
                pltpu.VMEM((history.shape[0], count, ROWS, slots), f32),
                pltpu.VMEM(wraps + (ROWS, slots), f32),
                pltpu.VMEM(wraps + (slots, ROWS), f32),
                pltpu.VMEM((2,) + wraps + (ROWS, slots), f32),
                pltpu.VMEM((lines, 9, STREAMS, wraps[2], slots, tiles[2] * slots), jnp.bfloat16),
                pltpu.VMEM(wraps + (SPREAD, slots), jnp.bfloat16),
                pltpu.VMEM((lines, SPREAD, tiles[2] * slots), f32),
                pltpu.VMEM((lines, SPREAD_LOW, tiles[2] * slots), f32),
                pltpu.VMEM((lines, SPREAD_PLAIN, tiles[2] * slots), f32),
                pltpu.VMEM((count, ROWS, slots), f32),
                pltpu.VMEM((count, ROWS, slots), f32),
                pltpu.VMEM((total_devices, 1, slots), f32),
                pltpu.VMEM((total_devices, 1, slots), f32),
                pltpu.SemaphoreType.DMA((6,)),
                pltpu.SemaphoreType.DMA((2,)),
                pltpu.SemaphoreType.DMA((2,)),
            ]
            + [pltpu.SemaphoreType.DMA((moves,))] * 6,
            compiler_params=pltpu.CompilerParams(
                collective_id=0, has_side_effects=True, vmem_limit_bytes=67043328
            ),
        )(fractions, polarizability, occupancy, pair_mask, perm_field, history)
        return induced, change[0, 0]

    in_specs = (
        P(None, "gx", "gy", "gz", None),
        P("gx", "gy", "gz", None),
        P("gx", "gy", "gz", None),
        P("gx", "gy", "gz", None),
        P(None, "gx", "gy", "gz", None),
        P(None, None, "gx", "gy", "gz", None),
    )
    out_specs = (P(None, "gx", "gy", "gz", None), P())
    return jax.shard_map(
        on_device, mesh=mesh, in_specs=in_specs, out_specs=out_specs, check_vma=False
    )
```

```python
import functools

import jax
import jax.numpy as jnp
from jax import lax
from jax.experimental import pallas as pl
from jax.experimental.pallas import tpu as pltpu
from jax.sharding import PartitionSpec as P

CELL_EDGE = 10.0
SOFTENING = 0.3
THOLE_DAMP = 0.39
RELAXATION = 0.7
MESH = pl.DeviceIdType.MESH
AXES = ("gx", "gy", "gz")
ROWS = 8
BLOCK = 16
APART = 2.5e25
STREAMS = 4
SPREAD = 128
SPREAD_LOW = 96
SPREAD_PLAIN = 32


def halo_moves(devices, tiles):
    options = []
    for count, n in zip(devices, tiles):
        if count == 2 and n == 2:
            around = [(1, 0, 2, 2)]
        else:
            around = [(1, n - 1, 1, n + 1), (-1, 0, 1, n)]
        options.append([(0, 0, n, 0)] + around)
    return [
        (a, b, c) for a in options[0] for b in options[1] for c in options[2] if (a[0], b[0], c[0]) != (0, 0, 0)
    ]


def solve_fit(total, past, lane, pair_lane):
    def pick(a, b):
        index = pair_lane[(min(a, b), max(a, b))]
        return jnp.sum(jnp.where(lane == index, total, 0.0), axis=1, keepdims=True)

    diagonal = [pick(a, a) for a in range(past)]
    trace = diagonal[0]
    for value in diagonal[1:]:
        trace = trace + value
    ridge = 0.001 * trace / past + 1.0
    lower, inverse = {}, []
    for j in range(past):
        pivot = diagonal[j] + ridge
        for m in range(j):
            pivot = pivot - lower[j, m] * lower[j, m]
        inverse.append(1.0 / jnp.sqrt(pivot))
        for i in range(j + 1, past):
            value = pick(i, j)
            for m in range(j):
                value = value - lower[i, m] * lower[j, m]
            lower[i, j] = value * inverse[j]
    forward = []
    for i in range(past):
        value = pick(i, past)
        for m in range(i):
            value = value - lower[i, m] * forward[m]
        forward.append(value * inverse[i])
    coeffs = [None] * past
    for i in reversed(range(past)):
        value = forward[i]
        for m in range(i + 1, past):
            value = value - lower[m, i] * coeffs[m]
        coeffs[i] = value * inverse[i]
    return coeffs


def kernel(
    devices,
    frac_in, pol_in, occ_in, mask_in, perm_in, hist_in,
    out_hbm, change_ref,
    out_ref,
    frac_ref, pol_ref, occ_ref, mask_ref, perm_ref, hist_ref,
    geom, held_one, held_two, past_sets, spots, columns, turns, links, weights,
    partial_main, partial_rest, partial_plain, scaled, fixed, slots_a, slots_b,
    load_sem, send_all, recv_all, send_geom, recv_geom, send_one, recv_one, send_two, recv_two,
):
    tiles = tuple(frac_ref.shape[1:4])
    slots = frac_ref.shape[4]
    steps = hist_ref.shape[0]
    rows = hist_ref.shape[1]
    past = steps - 1
    total_devices = devices[0] * devices[1] * devices[2]
    at = [lax.axis_index(axis) for axis in AXES]
    me = (at[0] * devices[1] + at[1]) * devices[2] + at[2]
    moves = halo_moves(devices, tiles)
    lane = lax.broadcasted_iota(jnp.int32, (1, slots), 1)
    loads = [
        pltpu.make_async_copy(source, target, load_sem.at[number])
        for number, (source, target) in enumerate(
            (
                (hist_in, hist_ref), (occ_in, occ_ref), (frac_in, frac_ref),
                (pol_in, pol_ref), (perm_in, perm_ref), (mask_in, mask_ref),
            )
        )
    ]
    for load in loads:
        load.start()

    def each_other(act):
        def pair(step, carry):
            ahead = (step // devices[1], step % devices[1])
            first = []
            for axis in range(2):
                place = at[axis] + ahead[axis]
                first.append(jnp.where(place >= devices[axis], place - devices[axis], place))
            for shift in range(devices[2] - 1, -1, -1):
                last = at[2] + shift
                last = jnp.where(last >= devices[2], last - devices[2], last)
                if shift == 0:
                    @pl.when(step > 0)
                    def _():
                        act((first[0], first[1], last))
                else:
                    act((first[0], first[1], last))
            return carry

        lax.fori_loop(0, devices[0] * devices[1], pair, 0)

    barrier = pltpu.get_barrier_semaphore()

    each_other(
        lambda device: pl.semaphore_signal(barrier, inc=1, device_id=device, device_id_type=MESH)
    )
    for load in loads:
        load.wait()

    def everyone(index, held):
        def start(device):
            pltpu.make_async_remote_copy(
                src_ref=held.at[pl.ds(me, 1)],
                dst_ref=held.at[pl.ds(me, 1)],
                send_sem=send_all.at[index],
                recv_sem=recv_all.at[index],
                device_id=device,
                device_id_type=MESH,
            ).start()

        each_other(start)

    def everyone_wait(index, held):
        whole = pltpu.make_async_remote_copy(
            src_ref=held.at[pl.ds(0, total_devices - 1)],
            dst_ref=held.at[pl.ds(0, total_devices - 1)],
            send_sem=send_all.at[index],
            recv_sem=recv_all.at[index],
            device_id=(at[0], at[1], (at[2] + 1) % devices[2]),
            device_id_type=MESH,
        )
        whole.wait_send()
        whole.wait_recv()

    def halo(held, send, recv, depth):
        copies = []
        for number, move in enumerate(moves):
            source = tuple(pl.ds(part[1], part[2]) for part in move)
            place = tuple(pl.ds(part[3], part[2]) for part in move)
            target = tuple((at[axis] + move[axis][0] + devices[axis]) % devices[axis] for axis in range(3))
            copies.append(
                pltpu.make_async_remote_copy(
                    src_ref=held.at[source + (pl.ds(0, depth),)],
                    dst_ref=held.at[place + (pl.ds(0, depth),)],
                    send_sem=send.at[number],
                    recv_sem=recv.at[number],
                    device_id=target,
                    device_id_type=MESH,
                )
            )
        return copies

    places = [(x, y, z) for x in range(tiles[0]) for y in range(tiles[1]) for z in range(tiles[2])]
    zero_row = jnp.zeros((1, slots), jnp.float32)
    spare = jnp.zeros((ROWS - rows, slots), jnp.float32)
    for t, (x, y, z) in enumerate(places):
        full = occ_ref[x, y, z, :].reshape(1, slots).astype(jnp.float32)
        pol = pol_ref[x, y, z, :].reshape(1, slots)
        scaled[t] = jnp.broadcast_to(RELAXATION * full * pol, (ROWS, slots))
        tile = jnp.concatenate(
            [frac_ref[c, x, y, z, :].reshape(1, slots) * CELL_EDGE for c in range(3)]
            + [lax.rsqrt(pol)] + [zero_row] * (ROWS - 4),
            axis=0,
        )
        geom[x, y, z] = tile
        for h in range(steps):
            moment = jnp.concatenate(
                [hist_ref[h, c, x, y, z, :].reshape(1, slots) for c in range(rows)], axis=0
            )
            past_sets[h, t] = jnp.concatenate([moment * full, spare], axis=0)
        fixed[t] = jnp.concatenate(
            [perm_ref[c, x, y, z, :].reshape(1, slots) for c in range(rows)] + [spare], axis=0
        )
    pair_lane = {}
    gram = zero_row
    for a in range(steps):
        for b in range(a, steps):
            product = past_sets[a, 0] * past_sets[b, 0]
            for t in range(1, len(places)):
                product = product + past_sets[a, t] * past_sets[b, t]
            value = jnp.sum(jnp.sum(product, axis=0, keepdims=True), axis=1, keepdims=True)
            pair_lane[(a, b)] = len(pair_lane)
            gram = jnp.where(lane == pair_lane[(a, b)], value, gram)
    slots_a[pl.ds(me, 1)] = gram.reshape(1, 1, slots)

    pl.semaphore_wait(barrier, total_devices - 1)
    geom_copies = halo(geom, send_geom, recv_geom, 4)
    everyone(0, slots_a)
    for copy in geom_copies:
        copy.start()

    wraps = tuple(n + 2 for n in tiles)
    row_of = lax.broadcasted_iota(jnp.int32, (ROWS, slots), 0)
    count = len(places)
    wide = tiles[2] * slots
    levels = list(range(tiles[2])) + [-1, tiles[2]]

    def wrap(value, size):
        return jnp.where(value < 0, value + size, value)

    def settle(place, slot):
        tile = geom[slot[0], slot[1], slot[2]]
        shift = jnp.zeros((ROWS, slots), jnp.float32)
        for axis in range(3):
            corner = CELL_EDGE * (jnp.asarray(place[axis], jnp.float32) - 0.5 * tiles[axis])
            shift = jnp.where(row_of == axis, corner, shift)
        tile = tile + shift
        spots[slot[0], slot[1], slot[2]] = tile
        columns[slot[0], slot[1], slot[2]] = tile.T
        one = jnp.ones((2, slots), jnp.float32)
        turns[0, slot[0], slot[1], slot[2]] = jnp.concatenate(
            [tile[0:3], tile[0:3], jnp.zeros((2, slots), jnp.float32)], axis=0
        )
        turns[1, slot[0], slot[1], slot[2]] = jnp.concatenate([one, tile[0:3], tile[0:3]], axis=0)

    def settle_all(xs, ys, zs):
        def one(step, carry):
            x = step + xs[0]
            for y in ys:
                for z in zs:
                    settle((x, y, z), (wrap(x, wraps[0]), y % wraps[1], z % wraps[2]))
            return carry

        lax.fori_loop(0, len(xs), one, 0)

    near_y, far_y = list(range(tiles[1])), [-1, tiles[1]]
    every_x = list(range(-1, tiles[0] + 1))
    own_z, side_z = list(range(tiles[2])), [-1, tiles[2]]

    def geometry(x, y, along_x, along_y, zs):
        nine = (along_x + 1) * 3 + along_y + 1
        line = x * tiles[1] + y
        slot_x, slot_y = wrap(x + along_x, wraps[0]), wrap(y + along_y, wraps[1])
        for level in zs:
            spot_at = levels.index(level)
            slot_z = level % wraps[2]
            takers = [z for z in range(tiles[2]) if abs(level - z) <= 1]
            fixed_rows = [[spots[x, y, z, pl.ds(c, 1), :] for c in range(4)] for z in takers]
            softs = [
                SOFTENING + (1 - mask_ref[x, y, z, nine * 3 + level - z + 1]).astype(jnp.float32) * APART
                for z in takers
            ]
            damps = [own_row[3] * -THOLE_DAMP for own_row in fixed_rows]
            for first in range(0, slots, BLOCK):
                part = pl.ds(first, BLOCK)
                moving = [
                    jnp.broadcast_to(columns[slot_x, slot_y, slot_z, part, c : c + 1], (BLOCK, slots))
                    for c in range(4)
                ]
                for z, own_row, damp, soft in zip(takers, fixed_rows, damps, softs):
                    dx = moving[0] - own_row[0]
                    dy = moving[1] - own_row[1]
                    dz = moving[2] - own_row[2]
                    square = dx * dx + dy * dy + dz * dz + soft
                    root = lax.rsqrt(square)
                    root_two = root * root
                    cube = root_two * root
                    arg = (square * root) * square * (damp * moving[3])
                    faded = jnp.exp(arg) * cube
                    direct = cube - faded
                    radial = (direct + arg * faded) * root_two
                    for number, value in ((0, radial), (2, direct)):
                        high = value.astype(jnp.bfloat16)
                        low = (value - high.astype(jnp.float32)).astype(jnp.bfloat16)
                        links[line, nine, number, spot_at, part, z * slots : (z + 1) * slots] = high
                        links[line, nine, number + 1, spot_at, part, z * slots : (z + 1) * slots] = low

    def geometry_near(along_xs, zs):
        def one(step, carry):
            x = step % tiles[0]
            y = step // tiles[0] % tiles[1]
            to_y = step // (tiles[0] * tiles[1]) % tiles[1]
            along_x = step // (tiles[0] * tiles[1] * tiles[1]) + along_xs[0]
            geometry(x, y, along_x, to_y - y, zs)
            return carry

        lax.fori_loop(0, tiles[0] * tiles[1] * tiles[1] * len(along_xs), one, 0)

    def geometry_far():
        def one(step, carry):
            x = step % tiles[0]
            side = step // tiles[0] % 2
            along_x = step // (2 * tiles[0]) - 1
            geometry(x, side * (tiles[1] - 1), along_x, 2 * side - 1, levels)
            return carry

        lax.fori_loop(0, 6 * tiles[0], one, 0)

    settle_all([x for x in every_x if 0 <= x < tiles[0]], near_y, own_z)
    geometry_near([0], own_z)
    off_diagonal = lax.broadcasted_iota(jnp.int32, (slots, slots), 0) != lax.broadcasted_iota(
        jnp.int32, (slots, slots), 1
    )
    for x, y, z in places:
        lanes = slice(z * slots, (z + 1) * slots)
        for number in range(STREAMS):
            link = links[x * tiles[1] + y, 4, number, levels.index(z), :, lanes].astype(jnp.float32)
            links[x * tiles[1] + y, 4, number, levels.index(z), :, lanes] = jnp.where(
                off_diagonal, link, 0.0
            ).astype(jnp.bfloat16)

    for move, copy in zip(moves, geom_copies):
        if move[1][0] == 0:
            copy.wait()
    settle_all([x for x in every_x if 0 <= x < tiles[0]], near_y, side_z)
    settle_all([-1], near_y, levels)
    settle_all([tiles[0]], near_y, levels)
    geometry_near([0], side_z)
    geometry_near([-1], levels)

    everyone_wait(0, slots_a)
    total = jnp.sum(slots_a[...], axis=0)
    coeffs = solve_fit(total, past, lane, pair_lane)
    for t, (x, y, z) in enumerate(places):
        value = coeffs[0] * past_sets[1, t]
        for h in range(1, past):
            value = value + coeffs[h] * past_sets[h + 1, t]
        held_one[x, y, z] = value
    one_copies = halo(held_one, send_one, recv_one, rows)
    for copy in one_copies:
        copy.start()
    geometry_near([1], levels)
    for move, copy in zip(moves, geom_copies):
        if move[1][0] != 0:
            copy.wait()
    settle_all(every_x, far_y, levels)
    geometry_far()

    kinds = 5

    def weigh(held, ys):
        def one(step, carry):
            x = wrap(step - 1, wraps[0])
            for y in ys:
                for z in range(wraps[2]):
                    slot = (x, y % wraps[1], z)
                    moment = jnp.where(row_of < rows, held[slot], 0.0)
                    along = moment * turns[(0,) + slot]
                    first = jnp.sum(jnp.where(row_of < 3, along, 0.0), axis=0, keepdims=True)
                    second = jnp.sum(jnp.where(row_of < 3, 0.0, along), axis=0, keepdims=True)
                    which = jnp.logical_or(row_of == 0, jnp.logical_and(row_of >= 2, row_of < 5))
                    both = jnp.where(which, first, second) * turns[(1,) + slot]
                    tiles_of = [moment, both] + [
                        spots[slot + (pl.ds(c, 1), slice(None))] * moment for c in range(3)
                    ]
                    parts = [[], [], []]
                    for value in tiles_of:
                        for level in range(3):
                            piece = value.astype(jnp.bfloat16).astype(jnp.float32)
                            parts[level].append(piece)
                            value = value - piece
                    order = [parts[0][0], parts[1][0], parts[2][0]]
                    for level in range(3):
                        order = order + parts[level][1:]
                    order.append(jnp.zeros((ROWS, slots), jnp.float32))
                    weights[slot] = jnp.concatenate(order, axis=0).astype(jnp.bfloat16)
            return carry

        lax.fori_loop(0, wraps[0], one, 0)

    def products(line, visits):
        width = 2 * slots if len(levels) % 2 == 0 else slots
        main = jnp.zeros((SPREAD, wide), jnp.float32)
        rest = jnp.zeros((SPREAD_LOW, wide), jnp.float32)
        plain = jnp.zeros((SPREAD_PLAIN, wide), jnp.float32)
        per = width // slots
        blank = jnp.zeros((slots, slots), jnp.bfloat16)
        for nine, slot_x, slot_y in visits:
            for start in range(0, len(levels), per):
                chunk = range(start, start + per)
                left = jnp.concatenate(
                    [weights[slot_x, slot_y, levels[i] % wraps[2]] for i in chunk], axis=1
                )

                def matrix(number):
                    lines = []
                    for i in chunk:
                        lines.append(
                            jnp.concatenate(
                                [
                                    links[line, nine, number, i, :, z * slots : (z + 1) * slots]
                                    if abs(levels[i] - z) <= 1
                                    else blank
                                    for z in range(tiles[2])
                                ],
                                axis=1,
                            )
                        )
                    return jnp.concatenate(lines, axis=0)

                def times(values, number):
                    return jnp.dot(values, matrix(number), preferred_element_type=jnp.float32)

                main = main + times(left, 0)
                rest = rest + times(left[0:SPREAD_LOW], 1)
                plain = plain + times(left[0:SPREAD_PLAIN], 2)
                plain = plain + times(left[0:SPREAD_PLAIN], 3)
        return main, rest, plain

    def near_products(x, y):
        visits = [
            ((along + 1) * 3 + to_y - y + 1, wrap(x + along, wraps[0]), to_y)
            for along in (-1, 0, 1)
            for to_y in range(tiles[1])
        ]
        return products(x * tiles[1] + y, visits)

    def far_products(x, y, side):
        visits = [
            ((along + 1) * 3 + 2 * side, wrap(x + along, wraps[0]), wrap((tiles[1] + 1) * side - 1, wraps[1]))
            for along in (-1, 0, 1)
        ]
        return products(x * tiles[1] + y, visits)

    def keep_near(step, carry):
        x, y = step // tiles[1], step % tiles[1]
        main, rest, plain = near_products(x, y)
        partial_main[step] = main
        partial_rest[step] = rest
        partial_plain[step] = plain
        return carry

    def field_of(x, y, main, rest, plain):
        def tile(value, index):
            return value[index * ROWS : (index + 1) * ROWS]

        def both_sum(first):
            total = tile(main, first[0]) + tile(rest, first[0])
            for index in first[1:]:
                total = total + tile(main, index)
                if (index + 1) * ROWS <= SPREAD_LOW:
                    total = total + tile(rest, index)
            return total

        moment = both_sum((0, 1, 2))
        both = both_sum((3, 7, 11))
        lifts = [both_sum((4 + c, 8 + c, 12 + c)) for c in range(3)]
        straight = tile(plain, 0) + tile(plain, 1) + tile(plain, 2)
        result = []
        for z in range(tiles[2]):
            lanes = slice(z * slots, (z + 1) * slots)
            turn = turns[0, x, y, z]
            inner = []
            for c in range(3):
                along = (lifts[c][:, lanes] - spots[x, y, z, pl.ds(c, 1), :] * moment[:, lanes]) * turn
                first = jnp.sum(jnp.where(row_of < 3, along, 0.0), axis=0, keepdims=True)
                second = jnp.sum(jnp.where(row_of < 3, 0.0, along), axis=0, keepdims=True)
                inner.append((first, second))
            inner = jnp.concatenate(
                [inner[c][0] for c in range(3)] + [inner[c][1] for c in range(3)] + [zero_row, zero_row], axis=0
            )
            lifted = jnp.concatenate([both[2:8, lanes], zero_row, zero_row], axis=0)
            dots = jnp.where(row_of < 3, both[0:1, lanes], both[1:2, lanes])
            result.append(3.0 * (lifted - dots * turn - inner) - straight[:, lanes])
        return result

    lines = tiles[0] * tiles[1]

    def field(step, held, act):
        x, y = step // tiles[1], step % tiles[1]
        main, rest, plain = partial_main[step], partial_rest[step], partial_plain[step]
        for side in range(2):
            if tiles[1] == 1:
                more = far_products(x, y, side)
                main, rest, plain = main + more[0], rest + more[1], plain + more[2]
        if tiles[1] > 1:
            side = y // (tiles[1] - 1)
            more = far_products(x, y, side)
            keep = jnp.logical_or(y == 0, y == tiles[1] - 1).astype(jnp.float32)
            if tiles[1] > 2:
                more = tuple(jnp.where(keep > 0.5, value, 0.0) for value in more)
            main, rest, plain = main + more[0], rest + more[1], plain + more[2]
        fields = field_of(x, y, main, rest, plain)
        for z in range(tiles[2]):
            t = step * tiles[2] + z
            act(x, y, z, t, (1.0 - RELAXATION) * held[x, y, z] + scaled[t] * (fixed[t] + fields[z]))

    def sweep(held, copies, act):
        for move, copy in zip(moves, copies):
            if move[1][0] == 0:
                copy.wait()
        weigh(held, near_y)
        lax.fori_loop(0, lines, keep_near, 0, unroll=True)
        for move, copy in zip(moves, copies):
            if move[1][0] != 0:
                copy.wait()
        weigh(held, far_y)

        def one(step, carry):
            field(step, held, act)
            return carry

        lax.fori_loop(0, lines, one, 0, unroll=True)

    def first_act(x, y, z, t, value):
        held_two[x, y, z] = value

    sweep(held_one, one_copies, first_act)
    two_copies = halo(held_two, send_two, recv_two, rows)
    for copy in two_copies:
        copy.start()

    def second_act(x, y, z, t, value):
        held_one[x, y, z] = value

    sweep(held_two, two_copies, second_act)
    changed = jnp.zeros((ROWS, slots), jnp.float32)
    size = jnp.zeros((ROWS, slots), jnp.float32)
    for t, (x, y, z) in enumerate(places):
        before, after = held_two[x, y, z], held_one[x, y, z]
        for c in range(rows):
            out_ref[c, x, y, z, :] = after[c]
        changed = changed + (after - before) * (after - before)
        size = size + after * after
    put = pltpu.make_async_copy(out_ref, out_hbm, load_sem.at[len(loads)])
    put.start()

    def all_of(value):
        return jnp.sum(jnp.sum(value, axis=0, keepdims=True), axis=1, keepdims=True)

    pair = jnp.where(lane == 0, all_of(changed), jnp.where(lane == 1, all_of(size), 0.0))
    slots_b[pl.ds(me, 1)] = pair.reshape(1, 1, slots)
    everyone(1, slots_b)
    everyone_wait(1, slots_b)
    pair = jnp.sum(slots_b[...], axis=0)
    above = jnp.sum(jnp.where(lane == 0, pair, 0.0), axis=1, keepdims=True)
    below = jnp.sum(jnp.where(lane == 1, pair, 0.0), axis=1, keepdims=True)
    change_ref[...] = jnp.broadcast_to(jnp.sqrt(above / (below + 1.0)), (1, slots))
    put.wait()


def solution(mesh):
    devices = tuple(mesh.shape[axis] for axis in AXES)
    total_devices = devices[0] * devices[1] * devices[2]

    def on_device(fractions, polarizability, occupancy, pair_mask, perm_field, history):
        tiles = fractions.shape[1:4]
        slots = fractions.shape[4]
        count = tiles[0] * tiles[1] * tiles[2]
        lines = tiles[0] * tiles[1]
        wraps = tuple(n + 2 for n in tiles)
        moves = len(halo_moves(devices, tiles))
        rows = history.shape[1]
        vmem = pl.BlockSpec(memory_space=pltpu.VMEM)
        f32 = jnp.float32
        induced, change = pl.pallas_call(
            functools.partial(kernel, devices),
            out_shape=(
                jax.ShapeDtypeStruct(perm_field.shape, f32),
                jax.ShapeDtypeStruct((1, slots), f32),
            ),
            in_specs=[pl.BlockSpec(memory_space=pltpu.HBM)] * 6,
            out_specs=(pl.BlockSpec(memory_space=pltpu.HBM), vmem),
            scratch_shapes=[
                pltpu.VMEM(perm_field.shape, f32),
                pltpu.VMEM(fractions.shape, f32),
                pltpu.VMEM(polarizability.shape, f32),
                pltpu.VMEM(occupancy.shape, jnp.int32),
                pltpu.SMEM(pair_mask.shape, jnp.int32),
                pltpu.VMEM(perm_field.shape, f32),
                pltpu.VMEM(history.shape, f32),
                pltpu.VMEM(wraps + (ROWS, slots), f32),
                pltpu.VMEM(wraps + (ROWS, slots), f32),
                pltpu.VMEM(wraps + (ROWS, slots), f32),
                pltpu.VMEM((history.shape[0], count, ROWS, slots), f32),
                pltpu.VMEM(wraps + (ROWS, slots), f32),
                pltpu.VMEM(wraps + (slots, ROWS), f32),
                pltpu.VMEM((2,) + wraps + (ROWS, slots), f32),
                pltpu.VMEM((lines, 9, STREAMS, wraps[2], slots, tiles[2] * slots), jnp.bfloat16),
                pltpu.VMEM(wraps + (SPREAD, slots), jnp.bfloat16),
                pltpu.VMEM((lines, SPREAD, tiles[2] * slots), f32),
                pltpu.VMEM((lines, SPREAD_LOW, tiles[2] * slots), f32),
                pltpu.VMEM((lines, SPREAD_PLAIN, tiles[2] * slots), f32),
                pltpu.VMEM((count, ROWS, slots), f32),
                pltpu.VMEM((count, ROWS, slots), f32),
                pltpu.VMEM((total_devices, 1, slots), f32),
                pltpu.VMEM((total_devices, 1, slots), f32),
                pltpu.SemaphoreType.DMA((7,)),
                pltpu.SemaphoreType.DMA((2,)),
                pltpu.SemaphoreType.DMA((2,)),
            ]
            + [pltpu.SemaphoreType.DMA((moves,))] * 6,
            compiler_params=pltpu.CompilerParams(
                collective_id=0, has_side_effects=True, vmem_limit_bytes=67043328
            ),
        )(fractions, polarizability, occupancy, pair_mask, perm_field, history)
        return induced, change[0, 0]

    in_specs = (
        P(None, "gx", "gy", "gz", None),
        P("gx", "gy", "gz", None),
        P("gx", "gy", "gz", None),
        P("gx", "gy", "gz", None),
        P(None, "gx", "gy", "gz", None),
        P(None, None, "gx", "gy", "gz", None),
    )
    out_specs = (P(None, "gx", "gy", "gz", None), P())
    return jax.shard_map(
        on_device, mesh=mesh, in_specs=in_specs, out_specs=out_specs, check_vma=False
    )
```

```python
import functools

import jax
import jax.numpy as jnp
from jax import lax
from jax.experimental import pallas as pl
from jax.experimental.pallas import tpu as pltpu
from jax.sharding import PartitionSpec as P

CELL_EDGE = 10.0
SOFTENING = 0.3
THOLE_DAMP = 0.39
RELAXATION = 0.7
MESH = pl.DeviceIdType.MESH
AXES = ("gx", "gy", "gz")
ROWS = 8
BLOCK = 16
APART = 2.5e25
STREAMS = 4
SPREAD = 128
SPREAD_LOW = 96
SPREAD_PLAIN = 32


def halo_moves(devices, tiles):
    options = []
    for count, n in zip(devices, tiles):
        if count == 2 and n == 2:
            around = [(1, 0, 2, 2)]
        else:
            around = [(1, n - 1, 1, n + 1), (-1, 0, 1, n)]
        options.append([(0, 0, n, 0)] + around)
    return [
        (a, b, c) for a in options[0] for b in options[1] for c in options[2] if (a[0], b[0], c[0]) != (0, 0, 0)
    ]


def solve_fit(total, past, lane, pair_lane):
    def pick(a, b):
        index = pair_lane[(min(a, b), max(a, b))]
        return jnp.sum(jnp.where(lane == index, total, 0.0), axis=1, keepdims=True)

    diagonal = [pick(a, a) for a in range(past)]
    trace = diagonal[0]
    for value in diagonal[1:]:
        trace = trace + value
    ridge = 0.001 * trace / past + 1.0
    lower, inverse = {}, []
    for j in range(past):
        pivot = diagonal[j] + ridge
        for m in range(j):
            pivot = pivot - lower[j, m] * lower[j, m]
        inverse.append(1.0 / jnp.sqrt(pivot))
        for i in range(j + 1, past):
            value = pick(i, j)
            for m in range(j):
                value = value - lower[i, m] * lower[j, m]
            lower[i, j] = value * inverse[j]
    forward = []
    for i in range(past):
        value = pick(i, past)
        for m in range(i):
            value = value - lower[i, m] * forward[m]
        forward.append(value * inverse[i])
    coeffs = [None] * past
    for i in reversed(range(past)):
        value = forward[i]
        for m in range(i + 1, past):
            value = value - lower[m, i] * coeffs[m]
        coeffs[i] = value * inverse[i]
    return coeffs


def kernel(
    devices,
    frac_in, pol_in, occ_in, mask_in, perm_in, hist_in,
    out_hbm, change_ref,
    out_ref,
    frac_ref, pol_ref, occ_ref, mask_ref, perm_ref, hist_ref,
    geom, held_one, held_two, past_sets, spots, features, distance, damping, turns, links, weights,
    partial_main, partial_rest, partial_plain, scaled, fixed, slots_a, slots_b,
    load_sem, send_all, recv_all, send_geom, recv_geom, send_one, recv_one, send_two, recv_two,
):
    tiles = tuple(frac_ref.shape[1:4])
    slots = frac_ref.shape[4]
    steps = hist_ref.shape[0]
    rows = hist_ref.shape[1]
    past = steps - 1
    total_devices = devices[0] * devices[1] * devices[2]
    at = [lax.axis_index(axis) for axis in AXES]
    me = (at[0] * devices[1] + at[1]) * devices[2] + at[2]
    moves = sorted(halo_moves(devices, tiles), key=lambda move: (move[1][0] != 0, sum(abs(part[0]) for part in move)))
    lane = lax.broadcasted_iota(jnp.int32, (1, slots), 1)
    loads = [
        pltpu.make_async_copy(source, target, load_sem.at[number])
        for number, (source, target) in enumerate(
            (
                (hist_in, hist_ref), (occ_in, occ_ref), (frac_in, frac_ref),
                (pol_in, pol_ref), (perm_in, perm_ref), (mask_in, mask_ref),
            )
        )
    ]
    for load in loads:
        load.start()

    def each_other(act):
        def pair(step, carry):
            down, across = step // devices[0], step % devices[0]
            x = at[0] + across
            x = jnp.where(x >= devices[0], x - devices[0], x)
            y = jnp.where(2 * at[1] < devices[1], devices[1] - 1 - down, down)
            for shift in range(devices[2] - 1, -1, -1):
                last = at[2] + shift
                last = jnp.where(last >= devices[2], last - devices[2], last)
                if shift == 0:
                    @pl.when(jnp.logical_or(across > 0, y != at[1]))
                    def _():
                        act((x, y, last))
                else:
                    act((x, y, last))
            return carry

        lax.fori_loop(0, devices[0] * devices[1], pair, 0)

    barrier = pltpu.get_barrier_semaphore()

    each_other(
        lambda device: pl.semaphore_signal(barrier, inc=1, device_id=device, device_id_type=MESH)
    )
    for load in loads:
        load.wait()

    def everyone(index, held):
        def start(device):
            pltpu.make_async_remote_copy(
                src_ref=held.at[pl.ds(me, 1)],
                dst_ref=held.at[pl.ds(me, 1)],
                send_sem=send_all.at[index],
                recv_sem=recv_all.at[index],
                device_id=device,
                device_id_type=MESH,
            ).start()

        each_other(start)

    def everyone_wait(index, held):
        whole = pltpu.make_async_remote_copy(
            src_ref=held.at[pl.ds(0, total_devices - 1)],
            dst_ref=held.at[pl.ds(0, total_devices - 1)],
            send_sem=send_all.at[index],
            recv_sem=recv_all.at[index],
            device_id=(at[0], at[1], (at[2] + 1) % devices[2]),
            device_id_type=MESH,
        )
        whole.wait_send()
        whole.wait_recv()

    def halo(held, send, recv, depth):
        copies = []
        for number, move in enumerate(moves):
            source = tuple(pl.ds(part[1], part[2]) for part in move)
            place = tuple(pl.ds(part[3], part[2]) for part in move)
            target = tuple((at[axis] + move[axis][0] + devices[axis]) % devices[axis] for axis in range(3))
            copies.append(
                pltpu.make_async_remote_copy(
                    src_ref=held.at[source + (pl.ds(0, depth),)],
                    dst_ref=held.at[place + (pl.ds(0, depth),)],
                    send_sem=send.at[number],
                    recv_sem=recv.at[number],
                    device_id=target,
                    device_id_type=MESH,
                )
            )
        return copies

    places = [(x, y, z) for x in range(tiles[0]) for y in range(tiles[1]) for z in range(tiles[2])]
    zero_row = jnp.zeros((1, slots), jnp.float32)
    spare = jnp.zeros((ROWS - rows, slots), jnp.float32)
    for t, (x, y, z) in enumerate(places):
        full = occ_ref[x, y, z, :].reshape(1, slots).astype(jnp.float32)
        pol = pol_ref[x, y, z, :].reshape(1, slots)
        scaled[t] = jnp.broadcast_to(RELAXATION * full * pol, (ROWS, slots))
        tile = jnp.concatenate(
            [frac_ref[c, x, y, z, :].reshape(1, slots) * CELL_EDGE for c in range(3)]
            + [lax.rsqrt(pol)] + [zero_row] * (ROWS - 4),
            axis=0,
        )
        geom[x, y, z] = tile
        for h in range(steps):
            moment = jnp.concatenate(
                [hist_ref[h, c, x, y, z, :].reshape(1, slots) for c in range(rows)], axis=0
            )
            past_sets[h, t] = jnp.concatenate([moment * full, spare], axis=0)
        fixed[t] = jnp.concatenate(
            [perm_ref[c, x, y, z, :].reshape(1, slots) for c in range(rows)] + [spare], axis=0
        )
    pair_lane = {}
    gram = zero_row
    for a in range(steps):
        for b in range(a, steps):
            product = past_sets[a, 0] * past_sets[b, 0]
            for t in range(1, len(places)):
                product = product + past_sets[a, t] * past_sets[b, t]
            value = jnp.sum(jnp.sum(product, axis=0, keepdims=True), axis=1, keepdims=True)
            pair_lane[(a, b)] = len(pair_lane)
            gram = jnp.where(lane == pair_lane[(a, b)], value, gram)
    slots_a[pl.ds(me, 1)] = gram.reshape(1, 1, slots)

    pl.semaphore_wait(barrier, total_devices - 1)
    geom_copies = halo(geom, send_geom, recv_geom, 4)
    everyone(0, slots_a)
    for copy in geom_copies:
        copy.start()

    wraps = tuple(n + 2 for n in tiles)
    row_of = lax.broadcasted_iota(jnp.int32, (ROWS, slots), 0)
    count = len(places)
    wide = tiles[2] * slots
    levels = list(range(tiles[2])) + [-1, tiles[2]]

    def wrap(value, size):
        return jnp.where(value < 0, value + size, value)

    def pieces(value):
        high = value.astype(jnp.bfloat16).astype(jnp.float32)
        value = value - high
        middle = value.astype(jnp.bfloat16).astype(jnp.float32)
        return high, middle, value - middle

    def choose(values):
        result = values[0]
        for row, value in enumerate(values[1:], 1):
            result = jnp.where(row_of == row, value, result)
        return result

    one_tile = jnp.ones((ROWS, slots), jnp.float32)
    zero_tile = jnp.zeros((ROWS, slots), jnp.float32)

    def broad(slot, c):
        return jnp.broadcast_to(spots[slot[0], slot[1], slot[2], pl.ds(c, 1), :], (ROWS, slots))

    def padded(parts):
        return parts + [zero_tile] * (slots // ROWS - len(parts))

    def source_features(slot):
        parts = []
        for c in range(3):
            value = broad(slot, c)
            high, middle, low = pieces(value)
            square, square_middle, square_low = pieces(value * value)
            parts.append(
                choose([square, one_tile, high, square_middle, high, middle, one_tile, square_low])
            )
            parts.append(choose([middle, high, low, one_tile, middle, low, zero_tile, zero_tile]))
        high, middle, low = pieces(broad(slot, 3))
        parts.append(choose([high, high, middle, high, low, middle, middle, low]))
        return jnp.concatenate(padded(parts), axis=0).astype(jnp.bfloat16)

    def taker_features(slot):
        parts = []
        for c in range(3):
            value = broad(slot, c)
            high, middle, low = pieces(value)
            square, square_middle, square_low = pieces(value * value)
            high, middle, low = -2.0 * high, -2.0 * middle, -2.0 * low
            parts.append(
                choose([one_tile, square, high, one_tile, middle, high, square_middle, one_tile])
            )
            parts.append(choose([middle, low, high, square_low, low, middle, zero_tile, zero_tile]))
        high, middle, low = pieces(broad(slot, 3) * -THOLE_DAMP)
        damp = choose([high, middle, high, low, high, middle, low, middle])
        far = jnp.concatenate(padded(parts), axis=0).astype(jnp.bfloat16)
        fade = jnp.concatenate(padded([zero_tile] * len(parts) + [damp]), axis=0).astype(jnp.bfloat16)
        return far, fade

    def settle(place, slot):
        tile = geom[slot[0], slot[1], slot[2]]
        shift = jnp.zeros((ROWS, slots), jnp.float32)
        for axis in range(3):
            corner = CELL_EDGE * (jnp.asarray(place[axis], jnp.float32) - 0.5 * tiles[axis])
            shift = jnp.where(row_of == axis, corner, shift)
        tile = tile + shift
        spots[slot[0], slot[1], slot[2]] = tile
        features[slot[0], slot[1], slot[2]] = source_features(slot).T
        one = jnp.ones((2, slots), jnp.float32)
        turns[0, slot[0], slot[1], slot[2]] = jnp.concatenate(
            [tile[0:3], tile[0:3], jnp.zeros((2, slots), jnp.float32)], axis=0
        )
        turns[1, slot[0], slot[1], slot[2]] = jnp.concatenate([one, tile[0:3], tile[0:3]], axis=0)

    def settle_all(xs, ys, zs):
        def one(step, carry):
            x = step + xs[0]
            for y in ys:
                for z in zs:
                    settle((x, y, z), (wrap(x, wraps[0]), y % wraps[1], z % wraps[2]))
            return carry

        lax.fori_loop(0, len(xs), one, 0)

    near_y, far_y = list(range(tiles[1])), [-1, tiles[1]]
    every_x = list(range(-1, tiles[0] + 1))
    own_z, side_z = list(range(tiles[2])), [-1, tiles[2]]

    def geometry(x, y, along_x, along_y, zs):
        nine = (along_x + 1) * 3 + along_y + 1
        line = x * tiles[1] + y
        slot_x, slot_y = wrap(x + along_x, wraps[0]), wrap(y + along_y, wraps[1])
        for level in zs:
            spot_at = levels.index(level)
            slot_z = level % wraps[2]
            takers = [z for z in range(tiles[2]) if abs(level - z) <= 1]
            softs = [
                SOFTENING + (1 - mask_ref[x, y, z, nine * 3 + level - z + 1]).astype(jnp.float32) * APART
                for z in takers
            ]
            lanes = slice(takers[0] * slots, (takers[-1] + 1) * slots)
            left = features[slot_x, slot_y, slot_z]
            squares = jnp.dot(left, distance[line, :, lanes], preferred_element_type=jnp.float32)
            damps = jnp.dot(left, damping[line, :, lanes], preferred_element_type=jnp.float32)
            for first in range(0, slots, BLOCK):
                part = pl.ds(first, BLOCK)
                for z, soft in zip(takers, softs):
                    at_lane = (z - takers[0]) * slots
                    square = squares[first : first + BLOCK, at_lane : at_lane + slots] + soft
                    damp = damps[first : first + BLOCK, at_lane : at_lane + slots]
                    root = lax.rsqrt(square)
                    root_two = root * root
                    cube = root_two * root
                    arg = (square * root) * square * damp
                    faded = jnp.exp(arg) * cube
                    direct = cube - faded
                    radial = (direct + arg * faded) * root_two
                    for number, value in ((0, radial), (2, direct)):
                        high = value.astype(jnp.bfloat16)
                        low = (value - high.astype(jnp.float32)).astype(jnp.bfloat16)
                        links[line, nine, number, spot_at, part, z * slots : (z + 1) * slots] = high
                        links[line, nine, number + 1, spot_at, part, z * slots : (z + 1) * slots] = low

    def geometry_near(along_x, zs):
        def one(step, carry):
            x = step % tiles[0]
            y = step // tiles[0] % tiles[1]
            to_y = step // (tiles[0] * tiles[1])
            geometry(x, y, along_x, to_y - y, zs)
            return carry

        lax.fori_loop(0, tiles[0] * tiles[1] * tiles[1], one, 0, unroll=True)

    def arrive(copies, kinds_of):
        for move, copy in zip(moves, copies):
            if move[1][0] != 0:
                kind = "far"
            else:
                kind = ("x" if move[0][0] != 0 else "") + ("z" if move[2][0] != 0 else "")
            if kind in kinds_of:
                copy.wait()

    def geometry_far():
        def one(step, carry):
            x = step % tiles[0]
            side = step // tiles[0] % 2
            along_x = step // (2 * tiles[0]) - 1
            geometry(x, side * (tiles[1] - 1), along_x, 2 * side - 1, levels)
            return carry

        lax.fori_loop(0, 6 * tiles[0], one, 0, unroll=True)

    own_x = list(range(tiles[0]))
    settle_all(own_x, near_y, own_z)
    for x, y, z in places:
        lanes = slice(z * slots, (z + 1) * slots)
        far, fade = taker_features((x, y, z))
        distance[x * tiles[1] + y, :, lanes] = far
        damping[x * tiles[1] + y, :, lanes] = fade
    geometry_near(0, own_z)
    off_diagonal = lax.broadcasted_iota(jnp.int32, (slots, slots), 0) != lax.broadcasted_iota(
        jnp.int32, (slots, slots), 1
    )
    for x, y, z in places:
        lanes = slice(z * slots, (z + 1) * slots)
        for number in range(STREAMS):
            link = links[x * tiles[1] + y, 4, number, levels.index(z), :, lanes].astype(jnp.float32)
            links[x * tiles[1] + y, 4, number, levels.index(z), :, lanes] = jnp.where(
                off_diagonal, link, 0.0
            ).astype(jnp.bfloat16)

    arrive(geom_copies, ("z",))
    settle_all(own_x, near_y, side_z)
    geometry_near(0, side_z)
    arrive(geom_copies, ("x", "xz"))
    settle_all([-1], near_y, levels)
    settle_all([tiles[0]], near_y, levels)
    geometry_near(-1, levels)

    everyone_wait(0, slots_a)
    total = jnp.sum(slots_a[...], axis=0)
    coeffs = solve_fit(total, past, lane, pair_lane)
    for t, (x, y, z) in enumerate(places):
        value = coeffs[0] * past_sets[1, t]
        for h in range(1, past):
            value = value + coeffs[h] * past_sets[h + 1, t]
        held_one[x, y, z] = value
    one_copies = halo(held_one, send_one, recv_one, rows)
    for copy in one_copies:
        copy.start()
    geometry_near(1, levels)
    arrive(geom_copies, ("far",))
    settle_all(every_x, far_y, levels)

    kinds = 5

    def weigh(held, xs, ys, zs):
        def one(step, carry):
            x = step * (xs[1] - xs[0] if len(xs) > 1 else 1) + xs[0]
            x = wrap(x, wraps[0])
            for y in ys:
                for z in zs:
                    slot = (x, y % wraps[1], z % wraps[2])
                    moment = jnp.where(row_of < rows, held[slot], 0.0)
                    along = moment * turns[(0,) + slot]
                    first = jnp.sum(jnp.where(row_of < 3, along, 0.0), axis=0, keepdims=True)
                    second = jnp.sum(jnp.where(row_of < 3, 0.0, along), axis=0, keepdims=True)
                    which = jnp.logical_or(row_of == 0, jnp.logical_and(row_of >= 2, row_of < 5))
                    both = jnp.where(which, first, second) * turns[(1,) + slot]
                    tiles_of = [moment, both] + [
                        spots[slot + (pl.ds(c, 1), slice(None))] * moment for c in range(3)
                    ]
                    parts = [[], [], []]
                    for value in tiles_of:
                        for level in range(3):
                            piece = value.astype(jnp.bfloat16).astype(jnp.float32)
                            parts[level].append(piece)
                            value = value - piece
                    order = [parts[0][0], parts[1][0], parts[2][0]]
                    for level in range(3):
                        order = order + parts[level][1:]
                    order.append(jnp.zeros((ROWS, slots), jnp.float32))
                    weights[slot] = jnp.concatenate(order, axis=0).astype(jnp.bfloat16)
            return carry

        lax.fori_loop(0, len(xs), one, 0)

    def products(line, visits):
        main = jnp.zeros((SPREAD, wide), jnp.float32)
        rest = jnp.zeros((SPREAD_LOW, wide), jnp.float32)
        plain = jnp.zeros((SPREAD_PLAIN, wide), jnp.float32)
        blank = jnp.zeros((slots, slots), jnp.bfloat16)
        for nine, slot_x, slot_y, zs in visits:
            for start in range(0, len(zs), 2):
                chunk = [levels.index(z) for z in zs[start : start + 2]]
                left = jnp.concatenate(
                    [weights[slot_x, slot_y, levels[i] % wraps[2]] for i in chunk], axis=1
                )

                def matrix(number):
                    lines = []
                    for i in chunk:
                        lines.append(
                            jnp.concatenate(
                                [
                                    links[line, nine, number, i, :, z * slots : (z + 1) * slots]
                                    if abs(levels[i] - z) <= 1
                                    else blank
                                    for z in range(tiles[2])
                                ],
                                axis=1,
                            )
                        )
                    return jnp.concatenate(lines, axis=0)

                def times(values, number):
                    return jnp.dot(values, matrix(number), preferred_element_type=jnp.float32)

                main = main + times(left, 0)
                rest = rest + times(left[0:SPREAD_LOW], 1)
                plain = plain + times(left[0:SPREAD_PLAIN], 2)
                plain = plain + times(left[0:SPREAD_PLAIN], 3)
        return main, rest, plain

    def near_products(x, y, parts):
        visits = [
            ((along + 1) * 3 + to_y - y + 1, wrap(x + along, wraps[0]), to_y, zs)
            for along, zs in parts
            for to_y in range(tiles[1])
        ]
        return products(x * tiles[1] + y, visits)

    def far_products(x, y, side):
        visits = [
            ((along + 1) * 3 + 2 * side, wrap(x + along, wraps[0]), wrap((tiles[1] + 1) * side - 1, wraps[1]), levels)
            for along in (-1, 0, 1)
        ]
        return products(x * tiles[1] + y, visits)

    partials = (partial_main, partial_rest, partial_plain)

    def gather(parts, start):
        def one(step, carry):
            sums = near_products(step // tiles[1], step % tiles[1], parts)
            for partial, value in zip(partials, sums):
                partial[step] = value if start else partial[step] + value
            return carry

        lax.fori_loop(0, tiles[0] * tiles[1], one, 0, unroll=True)

    def field_of(x, y, main, rest, plain):
        def tile(value, index):
            return value[index * ROWS : (index + 1) * ROWS]

        def both_sum(first):
            total = tile(main, first[0]) + tile(rest, first[0])
            for index in first[1:]:
                total = total + tile(main, index)
                if (index + 1) * ROWS <= SPREAD_LOW:
                    total = total + tile(rest, index)
            return total

        moment = both_sum((0, 1, 2))
        both = both_sum((3, 7, 11))
        lifts = [both_sum((4 + c, 8 + c, 12 + c)) for c in range(3)]
        straight = tile(plain, 0) + tile(plain, 1) + tile(plain, 2)
        result = []
        for z in range(tiles[2]):
            lanes = slice(z * slots, (z + 1) * slots)
            turn = turns[0, x, y, z]
            inner = []
            for c in range(3):
                along = (lifts[c][:, lanes] - spots[x, y, z, pl.ds(c, 1), :] * moment[:, lanes]) * turn
                first = jnp.sum(jnp.where(row_of < 3, along, 0.0), axis=0, keepdims=True)
                second = jnp.sum(jnp.where(row_of < 3, 0.0, along), axis=0, keepdims=True)
                inner.append((first, second))
            inner = jnp.concatenate(
                [inner[c][0] for c in range(3)] + [inner[c][1] for c in range(3)] + [zero_row, zero_row], axis=0
            )
            lifted = jnp.concatenate([both[2:8, lanes], zero_row, zero_row], axis=0)
            dots = jnp.where(row_of < 3, both[0:1, lanes], both[1:2, lanes])
            result.append(3.0 * (lifted - dots * turn - inner) - straight[:, lanes])
        return result

    lines = tiles[0] * tiles[1]

    def field(step, held, act):
        x, y = step // tiles[1], step % tiles[1]
        main, rest, plain = partial_main[step], partial_rest[step], partial_plain[step]
        for side in range(2):
            if tiles[1] == 1:
                more = far_products(x, y, side)
                main, rest, plain = main + more[0], rest + more[1], plain + more[2]
        if tiles[1] > 1:
            side = y // (tiles[1] - 1)
            more = far_products(x, y, side)
            keep = jnp.logical_or(y == 0, y == tiles[1] - 1).astype(jnp.float32)
            if tiles[1] > 2:
                more = tuple(jnp.where(keep > 0.5, value, 0.0) for value in more)
            main, rest, plain = main + more[0], rest + more[1], plain + more[2]
        fields = field_of(x, y, main, rest, plain)
        for z in range(tiles[2]):
            t = step * tiles[2] + z
            act(x, y, z, t, (1.0 - RELAXATION) * held[x, y, z] + scaled[t] * (fixed[t] + fields[z]))

    edge_x = [-1, tiles[0]]

    def first_near(held, copies):
        weigh(held, own_x, near_y, own_z)
        gather([(0, own_z)], True)
        geometry_far()
        arrive(copies, ("x", "z", "xz"))
        weigh(held, own_x, near_y, side_z)
        weigh(held, edge_x, near_y, levels)
        gather([(0, side_z), (-1, levels), (1, levels)], False)

    def second_near(held, copies):
        weigh(held, own_x, near_y, own_z)
        gather([(0, own_z)], True)
        arrive(copies, ("x", "z"))
        weigh(held, own_x, near_y, side_z)
        weigh(held, edge_x, near_y, own_z)
        gather([(0, side_z), (-1, own_z), (1, own_z)], False)
        arrive(copies, ("xz",))
        weigh(held, edge_x, near_y, side_z)
        gather([(-1, side_z), (1, side_z)], False)

    def sweep(held, copies, act):
        arrive(copies, ("far",))
        weigh(held, every_x, far_y, levels)

        def one(step, carry):
            field(step, held, act)
            return carry

        lax.fori_loop(0, lines, one, 0, unroll=True)

    def first_act(x, y, z, t, value):
        held_two[x, y, z] = value

    first_near(held_one, one_copies)
    sweep(held_one, one_copies, first_act)
    two_copies = halo(held_two, send_two, recv_two, rows)
    for copy in two_copies:
        copy.start()

    def second_act(x, y, z, t, value):
        held_one[x, y, z] = value

    second_near(held_two, two_copies)
    sweep(held_two, two_copies, second_act)
    changed = jnp.zeros((ROWS, slots), jnp.float32)
    size = jnp.zeros((ROWS, slots), jnp.float32)
    for t, (x, y, z) in enumerate(places):
        before, after = held_two[x, y, z], held_one[x, y, z]
        for c in range(rows):
            out_ref[c, x, y, z, :] = after[c]
        changed = changed + (after - before) * (after - before)
        size = size + after * after
    put = pltpu.make_async_copy(out_ref, out_hbm, load_sem.at[len(loads)])
    put.start()

    pair = jnp.concatenate(
        [jnp.sum(value, axis=0, keepdims=True) for value in (changed, size)], axis=1
    )
    slots_b[pl.ds(me, 1)] = pair.reshape(1, 1, 2 * slots)
    everyone(1, slots_b)
    everyone_wait(1, slots_b)
    pair = jnp.sum(slots_b[...], axis=0)
    above = jnp.sum(pair[:, 0:slots], axis=1, keepdims=True)
    below = jnp.sum(pair[:, slots : 2 * slots], axis=1, keepdims=True)
    change_ref[...] = jnp.broadcast_to(jnp.sqrt(above / (below + 1.0)), (1, slots))
    put.wait()


def solution(mesh):
    devices = tuple(mesh.shape[axis] for axis in AXES)
    total_devices = devices[0] * devices[1] * devices[2]

    def on_device(fractions, polarizability, occupancy, pair_mask, perm_field, history):
        tiles = fractions.shape[1:4]
        slots = fractions.shape[4]
        count = tiles[0] * tiles[1] * tiles[2]
        lines = tiles[0] * tiles[1]
        wraps = tuple(n + 2 for n in tiles)
        moves = len(halo_moves(devices, tiles))
        rows = history.shape[1]
        vmem = pl.BlockSpec(memory_space=pltpu.VMEM)
        f32 = jnp.float32
        induced, change = pl.pallas_call(
            functools.partial(kernel, devices),
            out_shape=(
                jax.ShapeDtypeStruct(perm_field.shape, f32),
                jax.ShapeDtypeStruct((1, slots), f32),
            ),
            in_specs=[pl.BlockSpec(memory_space=pltpu.HBM)] * 6,
            out_specs=(pl.BlockSpec(memory_space=pltpu.HBM), vmem),
            scratch_shapes=[
                pltpu.VMEM(perm_field.shape, f32),
                pltpu.VMEM(fractions.shape, f32),
                pltpu.VMEM(polarizability.shape, f32),
                pltpu.VMEM(occupancy.shape, jnp.int32),
                pltpu.SMEM(pair_mask.shape, jnp.int32),
                pltpu.VMEM(perm_field.shape, f32),
                pltpu.VMEM(history.shape, f32),
                pltpu.VMEM(wraps + (ROWS, slots), f32),
                pltpu.VMEM(wraps + (ROWS, slots), f32),
                pltpu.VMEM(wraps + (ROWS, slots), f32),
                pltpu.VMEM((history.shape[0], count, ROWS, slots), f32),
                pltpu.VMEM(wraps + (ROWS, slots), f32),
                pltpu.VMEM(wraps + (slots, slots), jnp.bfloat16),
                pltpu.VMEM((lines, slots, tiles[2] * slots), jnp.bfloat16),
                pltpu.VMEM((lines, slots, tiles[2] * slots), jnp.bfloat16),
                pltpu.VMEM((2,) + wraps + (ROWS, slots), f32),
                pltpu.VMEM((lines, 9, STREAMS, wraps[2], slots, tiles[2] * slots), jnp.bfloat16),
                pltpu.VMEM(wraps + (SPREAD, slots), jnp.bfloat16),
                pltpu.VMEM((lines, SPREAD, tiles[2] * slots), f32),
                pltpu.VMEM((lines, SPREAD_LOW, tiles[2] * slots), f32),
                pltpu.VMEM((lines, SPREAD_PLAIN, tiles[2] * slots), f32),
                pltpu.VMEM((count, ROWS, slots), f32),
                pltpu.VMEM((count, ROWS, slots), f32),
                pltpu.VMEM((total_devices, 1, slots), f32),
                pltpu.VMEM((total_devices, 1, 2 * slots), f32),
                pltpu.SemaphoreType.DMA((7,)),
                pltpu.SemaphoreType.DMA((2,)),
                pltpu.SemaphoreType.DMA((2,)),
            ]
            + [pltpu.SemaphoreType.DMA((moves,))] * 6,
            compiler_params=pltpu.CompilerParams(
                collective_id=0, has_side_effects=True, vmem_limit_bytes=67043328
            ),
        )(fractions, polarizability, occupancy, pair_mask, perm_field, history)
        return induced, change[0, 0]

    in_specs = (
        P(None, "gx", "gy", "gz", None),
        P("gx", "gy", "gz", None),
        P("gx", "gy", "gz", None),
        P("gx", "gy", "gz", None),
        P(None, "gx", "gy", "gz", None),
        P(None, None, "gx", "gy", "gz", None),
    )
    out_specs = (P(None, "gx", "gy", "gz", None), P())
    return jax.shard_map(
        on_device, mesh=mesh, in_specs=in_specs, out_specs=out_specs, check_vma=False
    )
```

```python
import functools

import jax
import jax.numpy as jnp
from jax import lax
from jax.experimental import pallas as pl
from jax.experimental.pallas import tpu as pltpu
from jax.sharding import PartitionSpec as P

CELL_EDGE = 10.0
SOFTENING = 0.3
THOLE_DAMP = 0.39
RELAXATION = 0.7
MESH = pl.DeviceIdType.MESH
AXES = ("gx", "gy", "gz")
ROWS = 8
BLOCK = 16
APART = 2.5e25
STREAMS = 4
SPREAD = 128
SPREAD_LOW = 96
SPREAD_PLAIN = 32


def halo_moves(devices, tiles):
    options = []
    for count, n in zip(devices, tiles):
        if count == 2 and n == 2:
            around = [(1, 0, 2, 2)]
        else:
            around = [(1, n - 1, 1, n + 1), (-1, 0, 1, n)]
        options.append([(0, 0, n, 0)] + around)
    return [
        (a, b, c) for a in options[0] for b in options[1] for c in options[2] if (a[0], b[0], c[0]) != (0, 0, 0)
    ]


def solve_fit(total, past, lane, pair_lane):
    def pick(a, b):
        index = pair_lane[(min(a, b), max(a, b))]
        return jnp.sum(jnp.where(lane == index, total, 0.0), axis=1, keepdims=True)

    diagonal = [pick(a, a) for a in range(past)]
    trace = diagonal[0]
    for value in diagonal[1:]:
        trace = trace + value
    ridge = 0.001 * trace / past + 1.0
    lower, inverse = {}, []
    for j in range(past):
        pivot = diagonal[j] + ridge
        for m in range(j):
            pivot = pivot - lower[j, m] * lower[j, m]
        inverse.append(1.0 / jnp.sqrt(pivot))
        for i in range(j + 1, past):
            value = pick(i, j)
            for m in range(j):
                value = value - lower[i, m] * lower[j, m]
            lower[i, j] = value * inverse[j]
    forward = []
    for i in range(past):
        value = pick(i, past)
        for m in range(i):
            value = value - lower[i, m] * forward[m]
        forward.append(value * inverse[i])
    coeffs = [None] * past
    for i in reversed(range(past)):
        value = forward[i]
        for m in range(i + 1, past):
            value = value - lower[m, i] * coeffs[m]
        coeffs[i] = value * inverse[i]
    return coeffs


def kernel(
    devices,
    frac_in, pol_in, occ_in, mask_in, perm_in, hist_in,
    out_hbm, change_ref,
    out_ref,
    frac_ref, pol_ref, occ_ref, mask_ref, perm_ref, hist_ref,
    geom, held_one, held_two, past_sets, spots, split_ref, features, distance, damping, turns, links, weights,
    partial_main, partial_rest, partial_plain, scaled, fixed, slots_a, slots_b,
    load_sem, send_all, recv_all, send_geom, recv_geom, send_one, recv_one, send_two, recv_two,
):
    tiles = tuple(frac_ref.shape[1:4])
    slots = frac_ref.shape[4]
    steps = hist_ref.shape[0]
    rows = hist_ref.shape[1]
    past = steps - 1
    total_devices = devices[0] * devices[1] * devices[2]
    at = [lax.axis_index(axis) for axis in AXES]
    me = (at[0] * devices[1] + at[1]) * devices[2] + at[2]
    moves = sorted(halo_moves(devices, tiles), key=lambda move: (move[1][0] != 0, sum(abs(part[0]) for part in move)))
    lane = lax.broadcasted_iota(jnp.int32, (1, slots), 1)
    loads = [
        pltpu.make_async_copy(source, target, load_sem.at[number])
        for number, (source, target) in enumerate(
            (
                (hist_in, hist_ref), (occ_in, occ_ref), (frac_in, frac_ref),
                (pol_in, pol_ref), (perm_in, perm_ref), (mask_in, mask_ref),
            )
        )
    ]
    for load in loads:
        load.start()

    def each_other(act):
        def pair(step, carry):
            down, across = step // devices[0], step % devices[0]
            x = at[0] + across
            x = jnp.where(x >= devices[0], x - devices[0], x)
            y = jnp.where(2 * at[1] < devices[1], devices[1] - 1 - down, down)
            for shift in range(devices[2] - 1, -1, -1):
                last = at[2] + shift
                last = jnp.where(last >= devices[2], last - devices[2], last)
                if shift == 0:
                    @pl.when(jnp.logical_or(across > 0, y != at[1]))
                    def _():
                        act((x, y, last))
                else:
                    act((x, y, last))
            return carry

        lax.fori_loop(0, devices[0] * devices[1], pair, 0, unroll=4)

    barrier = pltpu.get_barrier_semaphore()

    each_other(
        lambda device: pl.semaphore_signal(barrier, inc=1, device_id=device, device_id_type=MESH)
    )
    for load in loads:
        load.wait()

    def everyone(index, held):
        def start(device):
            pltpu.make_async_remote_copy(
                src_ref=held.at[pl.ds(me, 1)],
                dst_ref=held.at[pl.ds(me, 1)],
                send_sem=send_all.at[index],
                recv_sem=recv_all.at[index],
                device_id=device,
                device_id_type=MESH,
            ).start()

        each_other(start)

    def everyone_wait(index, held):
        whole = pltpu.make_async_remote_copy(
            src_ref=held.at[pl.ds(0, total_devices - 1)],
            dst_ref=held.at[pl.ds(0, total_devices - 1)],
            send_sem=send_all.at[index],
            recv_sem=recv_all.at[index],
            device_id=(at[0], at[1], (at[2] + 1) % devices[2]),
            device_id_type=MESH,
        )
        whole.wait_send()
        whole.wait_recv()

    def halo(held, send, recv, depth):
        copies = []
        for number, move in enumerate(moves):
            source = tuple(pl.ds(part[1], part[2]) for part in move)
            place = tuple(pl.ds(part[3], part[2]) for part in move)
            target = tuple((at[axis] + move[axis][0] + devices[axis]) % devices[axis] for axis in range(3))
            copies.append(
                pltpu.make_async_remote_copy(
                    src_ref=held.at[source + (pl.ds(0, depth),)],
                    dst_ref=held.at[place + (pl.ds(0, depth),)],
                    send_sem=send.at[number],
                    recv_sem=recv.at[number],
                    device_id=target,
                    device_id_type=MESH,
                )
            )
        return copies

    x_moves = {
        move[0][0]: number
        for number, move in enumerate(moves)
        if move[0][0] != 0 and move[1][0] == 0 and move[2][0] == 0
    }
    if len(x_moves) == 2:
        first_x = jnp.where(at[0] % 2 == 0, 1, -1)
        second_x = -first_x
        first_move = jnp.where(at[0] % 2 == 0, x_moves[-1], x_moves[1])
        second_move = x_moves[-1] + x_moves[1] - first_move
    else:
        first_x, second_x = 1, -1
        first_move, second_move = x_moves[1], None

    def arrive_x(held, send, recv, depth, number):
        if number is None:
            return
        move = moves[x_moves[1]]
        pltpu.make_async_remote_copy(
            src_ref=held.at[tuple(pl.ds(part[1], part[2]) for part in move) + (pl.ds(0, depth),)],
            dst_ref=held.at[tuple(pl.ds(part[3], part[2]) for part in move) + (pl.ds(0, depth),)],
            send_sem=send.at[number],
            recv_sem=recv.at[number],
            device_id=tuple((at[axis] + move[axis][0] + devices[axis]) % devices[axis] for axis in range(3)),
            device_id_type=MESH,
        ).wait()

    places = [(x, y, z) for x in range(tiles[0]) for y in range(tiles[1]) for z in range(tiles[2])]
    zero_row = jnp.zeros((1, slots), jnp.float32)
    spare = jnp.zeros((ROWS - rows, slots), jnp.float32)
    for t, (x, y, z) in enumerate(places):
        full = occ_ref[x, y, z, :].reshape(1, slots).astype(jnp.float32)
        pol = pol_ref[x, y, z, :].reshape(1, slots)
        scaled[t] = jnp.broadcast_to(RELAXATION * full * pol, (ROWS, slots))
        tile = jnp.concatenate(
            [frac_ref[c, x, y, z, :].reshape(1, slots) * CELL_EDGE for c in range(3)]
            + [lax.rsqrt(pol)] + [zero_row] * (ROWS - 4),
            axis=0,
        )
        geom[x, y, z] = tile
        for h in range(steps):
            moment = jnp.concatenate(
                [hist_ref[h, c, x, y, z, :].reshape(1, slots) for c in range(rows)], axis=0
            )
            past_sets[h, t] = jnp.concatenate([moment * full, spare], axis=0)
        fixed[t] = jnp.concatenate(
            [perm_ref[c, x, y, z, :].reshape(1, slots) for c in range(rows)] + [spare], axis=0
        )
    pair_lane = {}
    gram = zero_row
    for a in range(steps):
        for b in range(a, steps):
            product = past_sets[a, 0] * past_sets[b, 0]
            for t in range(1, len(places)):
                product = product + past_sets[a, t] * past_sets[b, t]
            value = jnp.sum(jnp.sum(product, axis=0, keepdims=True), axis=1, keepdims=True)
            pair_lane[(a, b)] = len(pair_lane)
            gram = jnp.where(lane == pair_lane[(a, b)], value, gram)
    slots_a[pl.ds(me, 1)] = gram.reshape(1, 1, slots)


    wraps = tuple(n + 2 for n in tiles)
    row_of = lax.broadcasted_iota(jnp.int32, (ROWS, slots), 0)
    count = len(places)
    wide = tiles[2] * slots
    levels = list(range(tiles[2])) + [-1, tiles[2]]

    def wrap(value, size):
        return jnp.where(value < 0, value + size, value)

    def pieces(value):
        high = value.astype(jnp.bfloat16).astype(jnp.float32)
        value = value - high
        middle = value.astype(jnp.bfloat16).astype(jnp.float32)
        return high, middle, value - middle

    def rows_in(*which):
        result = row_of == which[0]
        for row in which[1:]:
            result = jnp.logical_or(result, row_of == row)
        return result

    def mix(base, *choices):
        for where, value in choices:
            base = jnp.where(where, value, base)
        return base

    one_tile = jnp.ones((ROWS, slots), jnp.float32)
    zero_tile = jnp.zeros((ROWS, slots), jnp.float32)

    pair_a, pair_b, pair_c, pair_d = rows_in(1, 6), rows_in(2, 4), rows_in(0, 4), rows_in(2, 5)
    row = [row_of == number for number in range(ROWS)]
    damp_m, damp_l = rows_in(2, 5, 6), rows_in(4, 7)
    damp_m_i, damp_l_i = rows_in(1, 5, 7), rows_in(3, 6)

    def split_rows(slot):
        tile = spots[slot[0], slot[1], slot[2]]
        for number, value in enumerate(pieces(tile) + pieces(tile * tile)):
            split_ref[slot[0], slot[1], slot[2], number] = value

        def take(c, *numbers):
            return [
                jnp.broadcast_to(split_ref[slot[0], slot[1], slot[2], number, pl.ds(c, 1), :], (ROWS, slots))
                for number in numbers
            ]

        return take

    def padded(parts):
        return parts + [zero_tile] * (slots // ROWS - len(parts))

    def source_features(slot):
        take = split_rows(slot)
        parts = []
        for c in range(3):
            high, middle, low, square, square_middle, square_low = take(c, 0, 1, 2, 3, 4, 5)
            parts.append(
                mix(
                    square, (pair_a, one_tile), (pair_b, high), (row[3], square_middle),
                    (row[5], middle), (row[7], square_low),
                )
            )
            parts.append(mix(zero_tile, (pair_c, middle), (row[1], high), (pair_d, low), (row[3], one_tile)))
        high, middle, low = take(3, 0, 1, 2)
        parts.append(mix(high, (damp_m, middle), (damp_l, low)))
        return jnp.concatenate(padded(parts), axis=0).astype(jnp.bfloat16)

    def taker_features(slot):
        take = split_rows(slot)
        parts = []
        for c in range(3):
            high, middle, low, square, square_middle, square_low = take(c, 0, 1, 2, 3, 4, 5)
            high, middle, low = -2.0 * high, -2.0 * middle, -2.0 * low
            parts.append(
                mix(
                    one_tile, (row[1], square), (rows_in(2, 5), high), (row[4], middle),
                    (row[6], square_middle),
                )
            )
            parts.append(
                mix(
                    zero_tile, (rows_in(0, 5), middle), (rows_in(1, 4), low), (row[2], high),
                    (row[3], square_low),
                )
            )
        value = jnp.broadcast_to(spots[slot[0], slot[1], slot[2], pl.ds(3, 1), :], (ROWS, slots))
        high, middle, low = pieces(value * -THOLE_DAMP)
        damp = mix(high, (damp_m_i, middle), (damp_l_i, low))
        far = jnp.concatenate(padded(parts), axis=0).astype(jnp.bfloat16)
        fade = jnp.concatenate(padded([zero_tile] * len(parts) + [damp]), axis=0).astype(jnp.bfloat16)
        return far, fade

    def settle(place, slot):
        tile = geom[slot[0], slot[1], slot[2]]
        shift = jnp.zeros((ROWS, slots), jnp.float32)
        for axis in range(3):
            corner = CELL_EDGE * (jnp.asarray(place[axis], jnp.float32) - 0.5 * tiles[axis])
            shift = jnp.where(row_of == axis, corner, shift)
        tile = tile + shift
        spots[slot[0], slot[1], slot[2]] = tile
        features[slot[0], slot[1], slot[2]] = source_features(slot).T
        one = jnp.ones((2, slots), jnp.float32)
        turns[0, slot[0], slot[1], slot[2]] = jnp.concatenate(
            [tile[0:3], tile[0:3], jnp.zeros((2, slots), jnp.float32)], axis=0
        )
        turns[1, slot[0], slot[1], slot[2]] = jnp.concatenate([one, tile[0:3], tile[0:3]], axis=0)

    def settle_all(xs, ys, zs):
        def one(step, carry):
            x = step + xs[0]
            for y in ys:
                for z in zs:
                    settle((x, y, z), (wrap(x, wraps[0]), y % wraps[1], z % wraps[2]))
            return carry

        lax.fori_loop(0, len(xs), one, 0)

    near_y, far_y = list(range(tiles[1])), [-1, tiles[1]]
    every_x = list(range(-1, tiles[0] + 1))
    own_z, side_z = list(range(tiles[2])), [-1, tiles[2]]

    def geometry(x, y, along_x, along_y, zs):
        nine = (along_x + 1) * 3 + (along_y + 1)
        line = x * tiles[1] + y
        slot_x, slot_y = wrap(x + along_x, wraps[0]), wrap(y + along_y, wraps[1])
        for level in zs:
            spot_at = levels.index(level)
            slot_z = level % wraps[2]
            takers = [z for z in range(tiles[2]) if abs(level - z) <= 1]
            softs = [
                SOFTENING + (1 - mask_ref[x, y, z, nine * 3 + level - z + 1]).astype(jnp.float32) * APART
                for z in takers
            ]
            lanes = slice(takers[0] * slots, (takers[-1] + 1) * slots)
            left = features[slot_x, slot_y, slot_z]
            squares = jnp.dot(left, distance[line, :, lanes], preferred_element_type=jnp.float32)
            damps = jnp.dot(left, damping[line, :, lanes], preferred_element_type=jnp.float32)
            for first in range(0, slots, BLOCK):
                part = pl.ds(first, BLOCK)
                for z, soft in zip(takers, softs):
                    at_lane = (z - takers[0]) * slots
                    square = squares[first : first + BLOCK, at_lane : at_lane + slots] + soft
                    damp = damps[first : first + BLOCK, at_lane : at_lane + slots]
                    root = lax.rsqrt(square)
                    root_two = root * root
                    cube = root_two * root
                    arg = (square * root) * square * damp
                    faded = jnp.exp(arg) * cube
                    direct = cube - faded
                    radial = (direct + arg * faded) * root_two
                    for number, value in ((0, radial), (2, direct)):
                        high = value.astype(jnp.bfloat16)
                        low = (value - high.astype(jnp.float32)).astype(jnp.bfloat16)
                        links[line, nine, number, spot_at, part, z * slots : (z + 1) * slots] = high
                        links[line, nine, number + 1, spot_at, part, z * slots : (z + 1) * slots] = low

    def geometry_near(along_x, zs):
        for to_y in range(tiles[1]):
            for x in range(tiles[0]):
                for y in range(tiles[1]):
                    if abs(to_y - y) <= 1:
                        geometry(x, y, along_x, to_y - y, zs)

    def plane_of(along_x):
        return jnp.where(along_x > 0, tiles[0], -1)

    def settle_plane(along_x, ys, zs):
        plane = plane_of(along_x)
        for y in ys:
            for z in zs:
                settle((plane, y, z), (wrap(plane, wraps[0]), y % wraps[1], z % wraps[2]))

    def arrive(copies, kinds_of):
        for move, copy in zip(moves, copies):
            if move[1][0] != 0:
                kind = "far"
            else:
                kind = ("x" if move[0][0] != 0 else "") + ("z" if move[2][0] != 0 else "")
            if kind in kinds_of:
                copy.wait()

    def geometry_far(first, last):
        def one(step, carry):
            x = step % tiles[0]
            side = step // tiles[0] % 2
            along_x = step // (2 * tiles[0]) - 1
            geometry(x, side * (tiles[1] - 1), along_x, 2 * side - 1, levels)
            return carry

        lax.fori_loop(first * tiles[0], last * tiles[0], one, 0, unroll=True)

    own_x = list(range(tiles[0]))
    settle_all(own_x, near_y, own_z)
    for x, y, z in places:
        lanes = slice(z * slots, (z + 1) * slots)
        far, fade = taker_features((x, y, z))
        distance[x * tiles[1] + y, :, lanes] = far
        damping[x * tiles[1] + y, :, lanes] = fade
    geometry_near(0, own_z)
    off_diagonal = lax.broadcasted_iota(jnp.int32, (slots, slots), 0) != lax.broadcasted_iota(
        jnp.int32, (slots, slots), 1
    )
    for x, y, z in places:
        lanes = slice(z * slots, (z + 1) * slots)
        for number in range(STREAMS):
            link = links[x * tiles[1] + y, 4, number, levels.index(z), :, lanes].astype(jnp.float32)
            links[x * tiles[1] + y, 4, number, levels.index(z), :, lanes] = jnp.where(
                off_diagonal, link, 0.0
            ).astype(jnp.bfloat16)

    pl.semaphore_wait(barrier, total_devices - 1)
    geom_copies = halo(geom, send_geom, recv_geom, 4)
    near_count = sum(1 for move in moves if move[1][0] == 0)
    for copy in geom_copies[:near_count]:
        copy.start()
    everyone(0, slots_a)
    for copy in geom_copies[near_count:]:
        copy.start()
    geom_parts = (geom, send_geom, recv_geom, 4)
    arrive_x(*geom_parts, first_move)
    settle_plane(first_x, near_y, own_z)
    geometry_near(first_x, own_z)
    arrive(geom_copies, ("z",))
    settle_all(own_x, near_y, side_z)
    geometry_near(0, side_z)
    arrive_x(*geom_parts, second_move)
    arrive(geom_copies, ("xz",))
    settle_plane(first_x, near_y, side_z)
    settle_plane(second_x, near_y, levels)
    geometry_near(first_x, side_z)

    everyone_wait(0, slots_a)
    total = jnp.sum(slots_a[...], axis=0)
    coeffs = solve_fit(total, past, lane, pair_lane)
    for t, (x, y, z) in enumerate(places):
        value = coeffs[0] * past_sets[1, t]
        for h in range(1, past):
            value = value + coeffs[h] * past_sets[h + 1, t]
        held_one[x, y, z] = value
    one_copies = halo(held_one, send_one, recv_one, rows)
    for copy in one_copies:
        copy.start()
    geometry_near(second_x, levels)
    arrive(geom_copies, ("far",))
    settle_all(every_x, far_y, levels)

    kinds = 5

    def weigh(held, xs, ys, zs):
        for x in xs:
            for y in ys:
                for z in zs:
                    slot = (wrap(x, wraps[0]), y % wraps[1], z % wraps[2])
                    moment = jnp.where(row_of < rows, held[slot], 0.0)
                    along = moment * turns[(0,) + slot]
                    first = jnp.sum(jnp.where(row_of < 3, along, 0.0), axis=0, keepdims=True)
                    second = jnp.sum(jnp.where(row_of < 3, 0.0, along), axis=0, keepdims=True)
                    which = jnp.logical_or(row_of == 0, jnp.logical_and(row_of >= 2, row_of < 5))
                    both = jnp.where(which, first, second) * turns[(1,) + slot]
                    tiles_of = [moment, both] + [
                        spots[slot + (pl.ds(c, 1), slice(None))] * moment for c in range(3)
                    ]
                    parts = [[], [], []]
                    for value in tiles_of:
                        for level in range(3):
                            piece = value.astype(jnp.bfloat16).astype(jnp.float32)
                            parts[level].append(piece)
                            value = value - piece
                    order = [parts[0][0], parts[1][0], parts[2][0]]
                    for level in range(3):
                        order = order + parts[level][1:]
                    order.append(jnp.zeros((ROWS, slots), jnp.float32))
                    weights[slot] = jnp.concatenate(order, axis=0).astype(jnp.bfloat16)

    def products(line, visits):
        main = jnp.zeros((SPREAD, wide), jnp.float32)
        rest = jnp.zeros((SPREAD_LOW, wide), jnp.float32)
        plain = jnp.zeros((SPREAD_PLAIN, wide), jnp.float32)
        blank = jnp.zeros((slots, slots), jnp.bfloat16)
        for nine, slot_x, slot_y, zs in visits:
            for start in range(0, len(zs), 2):
                chunk = [levels.index(z) for z in zs[start : start + 2]]
                left = jnp.concatenate(
                    [weights[slot_x, slot_y, levels[i] % wraps[2]] for i in chunk], axis=1
                )

                def matrix(number):
                    lines = []
                    for i in chunk:
                        lines.append(
                            jnp.concatenate(
                                [
                                    links[line, nine, number, i, :, z * slots : (z + 1) * slots]
                                    if abs(levels[i] - z) <= 1
                                    else blank
                                    for z in range(tiles[2])
                                ],
                                axis=1,
                            )
                        )
                    return jnp.concatenate(lines, axis=0)

                def times(values, number):
                    return jnp.dot(values, matrix(number), preferred_element_type=jnp.float32)

                main = main + times(left, 0)
                rest = rest + times(left[0:SPREAD_LOW], 1)
                plain = plain + times(left[0:SPREAD_PLAIN], 2)
                plain = plain + times(left[0:SPREAD_PLAIN], 3)
        return main, rest, plain

    def near_products(x, y, parts):
        visits = [
            ((along + 1) * 3 + to_y - y + 1, wrap(x + along, wraps[0]), to_y, zs)
            for along, zs in parts
            for to_y in range(tiles[1])
        ]
        return products(x * tiles[1] + y, visits)

    def far_products(x, y, side):
        visits = [
            ((along + 1) * 3 + 2 * side, wrap(x + along, wraps[0]), wrap((tiles[1] + 1) * side - 1, wraps[1]), levels)
            for along in (-1, 0, 1)
        ]
        return products(x * tiles[1] + y, visits)

    partials = (partial_main, partial_rest, partial_plain)

    def gather(parts, start):
        def one(step, carry):
            sums = near_products(step // tiles[1], step % tiles[1], parts)
            for partial, value in zip(partials, sums):
                partial[step] = value if start else partial[step] + value
            return carry

        lax.fori_loop(0, tiles[0] * tiles[1], one, 0, unroll=True)

    def field_of(x, y, main, rest, plain):
        def tile(value, index):
            return value[index * ROWS : (index + 1) * ROWS]

        def both_sum(first):
            total = tile(main, first[0]) + tile(rest, first[0])
            for index in first[1:]:
                total = total + tile(main, index)
                if (index + 1) * ROWS <= SPREAD_LOW:
                    total = total + tile(rest, index)
            return total

        moment = both_sum((0, 1, 2))
        both = both_sum((3, 7, 11))
        lifts = [both_sum((4 + c, 8 + c, 12 + c)) for c in range(3)]
        straight = tile(plain, 0) + tile(plain, 1) + tile(plain, 2)
        result = []
        for z in range(tiles[2]):
            lanes = slice(z * slots, (z + 1) * slots)
            turn = turns[0, x, y, z]
            inner = []
            for c in range(3):
                along = (lifts[c][:, lanes] - spots[x, y, z, pl.ds(c, 1), :] * moment[:, lanes]) * turn
                first = jnp.sum(jnp.where(row_of < 3, along, 0.0), axis=0, keepdims=True)
                second = jnp.sum(jnp.where(row_of < 3, 0.0, along), axis=0, keepdims=True)
                inner.append((first, second))
            inner = jnp.concatenate(
                [inner[c][0] for c in range(3)] + [inner[c][1] for c in range(3)] + [zero_row, zero_row], axis=0
            )
            lifted = jnp.concatenate([both[2:8, lanes], zero_row, zero_row], axis=0)
            dots = jnp.where(row_of < 3, both[0:1, lanes], both[1:2, lanes])
            result.append(3.0 * (lifted - dots * turn - inner) - straight[:, lanes])
        return result

    lines = tiles[0] * tiles[1]

    def field(step, held, act):
        x, y = step // tiles[1], step % tiles[1]
        main, rest, plain = partial_main[step], partial_rest[step], partial_plain[step]
        for side in range(2):
            if tiles[1] == 1:
                more = far_products(x, y, side)
                main, rest, plain = main + more[0], rest + more[1], plain + more[2]
        if tiles[1] > 1:
            side = y // (tiles[1] - 1)
            more = far_products(x, y, side)
            keep = jnp.logical_or(y == 0, y == tiles[1] - 1).astype(jnp.float32)
            if tiles[1] > 2:
                more = tuple(jnp.where(keep > 0.5, value, 0.0) for value in more)
            main, rest, plain = main + more[0], rest + more[1], plain + more[2]
        fields = field_of(x, y, main, rest, plain)
        for z in range(tiles[2]):
            t = step * tiles[2] + z
            act(x, y, z, t, (1.0 - RELAXATION) * held[x, y, z] + scaled[t] * (fixed[t] + fields[z]))

    def arrive_near(parts, copies):
        arrive_x(*parts, first_move)
        arrive_x(*parts, second_move)
        arrive(copies, ("z", "xz"))

    def first_near(held, parts, copies):
        weigh(held, own_x, near_y, own_z)
        gather([(0, own_z)], True)
        geometry_far(0, 4)
        arrive_near(parts, copies)
        weigh(held, own_x, near_y, side_z)
        weigh(held, [-1, tiles[0]], near_y, levels)
        geometry_far(4, 6)
        gather([(0, side_z), (-1, levels), (1, levels)], False)

    def second_near(held, parts, copies):
        weigh(held, own_x, near_y, own_z)
        gather([(0, own_z)], True)
        arrive_x(*parts, first_move)
        weigh(held, [plane_of(first_x)], near_y, own_z)
        gather([(first_x, own_z)], False)
        arrive(copies, ("z",))
        weigh(held, own_x, near_y, side_z)
        gather([(0, side_z)], False)
        arrive_x(*parts, second_move)
        arrive(copies, ("xz",))
        weigh(held, [plane_of(first_x)], near_y, side_z)
        weigh(held, [plane_of(second_x)], near_y, levels)
        gather([(first_x, side_z), (second_x, levels)], False)

    def sweep(held, copies, act):
        arrive(copies, ("far",))
        weigh(held, every_x, far_y, levels)

        def one(step, carry):
            field(step, held, act)
            return carry

        lax.fori_loop(0, lines, one, 0, unroll=True)

    def first_act(x, y, z, t, value):
        held_two[x, y, z] = value

    first_near(held_one, (held_one, send_one, recv_one, rows), one_copies)
    sweep(held_one, one_copies, first_act)
    two_copies = halo(held_two, send_two, recv_two, rows)
    for copy in two_copies:
        copy.start()

    def second_act(x, y, z, t, value):
        held_one[x, y, z] = value

    second_near(held_two, (held_two, send_two, recv_two, rows), two_copies)
    sweep(held_two, two_copies, second_act)
    changed = jnp.zeros((ROWS, slots), jnp.float32)
    size = jnp.zeros((ROWS, slots), jnp.float32)
    for t, (x, y, z) in enumerate(places):
        before, after = held_two[x, y, z], held_one[x, y, z]
        for c in range(rows):
            out_ref[c, x, y, z, :] = after[c]
        changed = changed + (after - before) * (after - before)
        size = size + after * after
    put = pltpu.make_async_copy(out_ref, out_hbm, load_sem.at[len(loads)])
    put.start()

    pair = jnp.concatenate(
        [jnp.sum(value, axis=0, keepdims=True) for value in (changed, size)], axis=1
    )
    slots_b[pl.ds(me, 1)] = pair.reshape(1, 1, 2 * slots)
    everyone(1, slots_b)
    everyone_wait(1, slots_b)
    pair = jnp.sum(slots_b[...], axis=0)
    above = jnp.sum(pair[:, 0:slots], axis=1, keepdims=True)
    below = jnp.sum(pair[:, slots : 2 * slots], axis=1, keepdims=True)
    change_ref[...] = jnp.broadcast_to(jnp.sqrt(above / (below + 1.0)), (1, slots))
    put.wait()


def solution(mesh):
    devices = tuple(mesh.shape[axis] for axis in AXES)
    total_devices = devices[0] * devices[1] * devices[2]

    def on_device(fractions, polarizability, occupancy, pair_mask, perm_field, history):
        tiles = fractions.shape[1:4]
        slots = fractions.shape[4]
        count = tiles[0] * tiles[1] * tiles[2]
        lines = tiles[0] * tiles[1]
        wraps = tuple(n + 2 for n in tiles)
        moves = len(halo_moves(devices, tiles))
        rows = history.shape[1]
        vmem = pl.BlockSpec(memory_space=pltpu.VMEM)
        f32 = jnp.float32
        induced, change = pl.pallas_call(
            functools.partial(kernel, devices),
            out_shape=(
                jax.ShapeDtypeStruct(perm_field.shape, f32),
                jax.ShapeDtypeStruct((1, slots), f32),
            ),
            in_specs=[pl.BlockSpec(memory_space=pltpu.HBM)] * 6,
            out_specs=(pl.BlockSpec(memory_space=pltpu.HBM), vmem),
            scratch_shapes=[
                pltpu.VMEM(perm_field.shape, f32),
                pltpu.VMEM(fractions.shape, f32),
                pltpu.VMEM(polarizability.shape, f32),
                pltpu.VMEM(occupancy.shape, jnp.int32),
                pltpu.SMEM(pair_mask.shape, jnp.int32),
                pltpu.VMEM(perm_field.shape, f32),
                pltpu.VMEM(history.shape, f32),
                pltpu.VMEM(wraps + (ROWS, slots), f32),
                pltpu.VMEM(wraps + (ROWS, slots), f32),
                pltpu.VMEM(wraps + (ROWS, slots), f32),
                pltpu.VMEM((history.shape[0], count, ROWS, slots), f32),
                pltpu.VMEM(wraps + (ROWS, slots), f32),
                pltpu.VMEM(wraps + (6, ROWS, slots), f32),
                pltpu.VMEM(wraps + (slots, slots), jnp.bfloat16),
                pltpu.VMEM((lines, slots, tiles[2] * slots), jnp.bfloat16),
                pltpu.VMEM((lines, slots, tiles[2] * slots), jnp.bfloat16),
                pltpu.VMEM((2,) + wraps + (ROWS, slots), f32),
                pltpu.VMEM((lines, 9, STREAMS, wraps[2], slots, tiles[2] * slots), jnp.bfloat16),
                pltpu.VMEM(wraps + (SPREAD, slots), jnp.bfloat16),
                pltpu.VMEM((lines, SPREAD, tiles[2] * slots), f32),
                pltpu.VMEM((lines, SPREAD_LOW, tiles[2] * slots), f32),
                pltpu.VMEM((lines, SPREAD_PLAIN, tiles[2] * slots), f32),
                pltpu.VMEM((count, ROWS, slots), f32),
                pltpu.VMEM((count, ROWS, slots), f32),
                pltpu.VMEM((total_devices, 1, slots), f32),
                pltpu.VMEM((total_devices, 1, 2 * slots), f32),
                pltpu.SemaphoreType.DMA((7,)),
                pltpu.SemaphoreType.DMA((2,)),
                pltpu.SemaphoreType.DMA((2,)),
            ]
            + [pltpu.SemaphoreType.DMA((moves,))] * 6,
            compiler_params=pltpu.CompilerParams(
                collective_id=0, has_side_effects=True, vmem_limit_bytes=67043328
            ),
        )(fractions, polarizability, occupancy, pair_mask, perm_field, history)
        return induced, change[0, 0]

    in_specs = (
        P(None, "gx", "gy", "gz", None),
        P("gx", "gy", "gz", None),
        P("gx", "gy", "gz", None),
        P("gx", "gy", "gz", None),
        P(None, "gx", "gy", "gz", None),
        P(None, None, "gx", "gy", "gz", None),
    )
    out_specs = (P(None, "gx", "gy", "gz", None), P())
    return jax.shard_map(
        on_device, mesh=mesh, in_specs=in_specs, out_specs=out_specs, check_vma=False
    )
```

```python
import functools

import jax
import jax.numpy as jnp
from jax import lax
from jax.experimental import pallas as pl
from jax.experimental.pallas import tpu as pltpu
from jax.sharding import PartitionSpec as P

CELL_EDGE = 10.0
SOFTENING = 0.3
THOLE_DAMP = 0.39
RELAXATION = 0.7
MESH = pl.DeviceIdType.MESH
AXES = ("gx", "gy", "gz")
ROWS = 8
BLOCK = 16
APART = 2.5e25
STREAMS = 4
SPREAD = 128
SPREAD_LOW = 96
SPREAD_PLAIN = 32


def halo_moves(devices, tiles):
    options = []
    for count, n in zip(devices, tiles):
        if count == 2 and n == 2:
            around = [(1, 0, 2, 2)]
        else:
            around = [(1, n - 1, 1, n + 1), (-1, 0, 1, n)]
        options.append([(0, 0, n, 0)] + around)
    return [
        (a, b, c) for a in options[0] for b in options[1] for c in options[2] if (a[0], b[0], c[0]) != (0, 0, 0)
    ]


def solve_fit(total, past, lane, pair_lane):
    def pick(a, b):
        index = pair_lane[(min(a, b), max(a, b))]
        return jnp.sum(jnp.where(lane == index, total, 0.0), axis=1, keepdims=True)

    diagonal = [pick(a, a) for a in range(past)]
    trace = diagonal[0]
    for value in diagonal[1:]:
        trace = trace + value
    ridge = 0.001 * trace / past + 1.0
    lower, inverse = {}, []
    for j in range(past):
        pivot = diagonal[j] + ridge
        for m in range(j):
            pivot = pivot - lower[j, m] * lower[j, m]
        inverse.append(1.0 / jnp.sqrt(pivot))
        for i in range(j + 1, past):
            value = pick(i, j)
            for m in range(j):
                value = value - lower[i, m] * lower[j, m]
            lower[i, j] = value * inverse[j]
    forward = []
    for i in range(past):
        value = pick(i, past)
        for m in range(i):
            value = value - lower[i, m] * forward[m]
        forward.append(value * inverse[i])
    coeffs = [None] * past
    for i in reversed(range(past)):
        value = forward[i]
        for m in range(i + 1, past):
            value = value - lower[m, i] * coeffs[m]
        coeffs[i] = value * inverse[i]
    return coeffs


def kernel(
    devices,
    frac_in, pol_in, occ_in, mask_in, perm_in, hist_in,
    out_hbm, change_ref,
    out_ref,
    frac_ref, pol_ref, occ_ref, mask_ref, perm_ref, hist_ref,
    geom, held_one, held_two, past_sets, spots, split_ref, features, distance, damping, turns, links, weights,
    partial_main, partial_rest, partial_plain, scaled, fixed, slots_a, slots_b,
    load_sem, send_all, recv_all, send_geom, recv_geom, send_one, recv_one, send_two, recv_two,
):
    tiles = tuple(frac_ref.shape[1:4])
    slots = frac_ref.shape[4]
    steps = hist_ref.shape[0]
    rows = hist_ref.shape[1]
    past = steps - 1
    total_devices = devices[0] * devices[1] * devices[2]
    at = [lax.axis_index(axis) for axis in AXES]
    me = (at[0] * devices[1] + at[1]) * devices[2] + at[2]
    moves = sorted(halo_moves(devices, tiles), key=lambda move: (move[1][0] != 0, sum(abs(part[0]) for part in move)))
    lane = lax.broadcasted_iota(jnp.int32, (1, slots), 1)
    loads = [
        pltpu.make_async_copy(source, target, load_sem.at[number])
        for number, (source, target) in enumerate(
            (
                (hist_in, hist_ref), (occ_in, occ_ref), (frac_in, frac_ref),
                (pol_in, pol_ref), (perm_in, perm_ref), (mask_in, mask_ref),
            )
        )
    ]
    for load in loads:
        load.start()

    def each_other(act):
        def pair(step, carry):
            down, across = step // devices[0], step % devices[0]
            x = at[0] + across
            x = jnp.where(x >= devices[0], x - devices[0], x)
            y = jnp.where(2 * at[1] < devices[1], devices[1] - 1 - down, down)
            for shift in range(devices[2] - 1, -1, -1):
                last = at[2] + shift
                last = jnp.where(last >= devices[2], last - devices[2], last)
                if shift == 0:
                    @pl.when(jnp.logical_or(across > 0, y != at[1]))
                    def _():
                        act((x, y, last))
                else:
                    act((x, y, last))
            return carry

        lax.fori_loop(0, devices[0] * devices[1], pair, 0, unroll=4)

    barrier = pltpu.get_barrier_semaphore()

    each_other(
        lambda device: pl.semaphore_signal(barrier, inc=1, device_id=device, device_id_type=MESH)
    )
    for load in loads:
        load.wait()

    def everyone(index, held):
        def start(device):
            pltpu.make_async_remote_copy(
                src_ref=held.at[pl.ds(me, 1)],
                dst_ref=held.at[pl.ds(me, 1)],
                send_sem=send_all.at[index],
                recv_sem=recv_all.at[index],
                device_id=device,
                device_id_type=MESH,
            ).start()

        each_other(start)

    def everyone_wait(index, held):
        whole = pltpu.make_async_remote_copy(
            src_ref=held.at[pl.ds(0, total_devices - 1)],
            dst_ref=held.at[pl.ds(0, total_devices - 1)],
            send_sem=send_all.at[index],
            recv_sem=recv_all.at[index],
            device_id=(at[0], at[1], (at[2] + 1) % devices[2]),
            device_id_type=MESH,
        )
        whole.wait_send()
        whole.wait_recv()

    def halo(held, send, recv, depth):
        copies = []
        for number, move in enumerate(moves):
            source = tuple(pl.ds(part[1], part[2]) for part in move)
            place = tuple(pl.ds(part[3], part[2]) for part in move)
            target = tuple((at[axis] + move[axis][0] + devices[axis]) % devices[axis] for axis in range(3))
            copies.append(
                pltpu.make_async_remote_copy(
                    src_ref=held.at[source + (pl.ds(0, depth),)],
                    dst_ref=held.at[place + (pl.ds(0, depth),)],
                    send_sem=send.at[number],
                    recv_sem=recv.at[number],
                    device_id=target,
                    device_id_type=MESH,
                )
            )
        return copies

    x_moves = {
        move[0][0]: number
        for number, move in enumerate(moves)
        if move[0][0] != 0 and move[1][0] == 0 and move[2][0] == 0
    }
    if len(x_moves) == 2:
        first_x = jnp.where(at[0] % 2 == 0, 1, -1)
        second_x = -first_x
        first_move = jnp.where(at[0] % 2 == 0, x_moves[-1], x_moves[1])
        second_move = x_moves[-1] + x_moves[1] - first_move
    else:
        first_x, second_x = 1, -1
        first_move, second_move = x_moves[1], None

    def arrive_x(held, send, recv, depth, number):
        if number is None:
            return
        move = moves[x_moves[1]]
        pltpu.make_async_remote_copy(
            src_ref=held.at[tuple(pl.ds(part[1], part[2]) for part in move) + (pl.ds(0, depth),)],
            dst_ref=held.at[tuple(pl.ds(part[3], part[2]) for part in move) + (pl.ds(0, depth),)],
            send_sem=send.at[number],
            recv_sem=recv.at[number],
            device_id=tuple((at[axis] + move[axis][0] + devices[axis]) % devices[axis] for axis in range(3)),
            device_id_type=MESH,
        ).wait()

    places = [(x, y, z) for x in range(tiles[0]) for y in range(tiles[1]) for z in range(tiles[2])]
    zero_row = jnp.zeros((1, slots), jnp.float32)
    spare = jnp.zeros((ROWS - rows, slots), jnp.float32)
    for t, (x, y, z) in enumerate(places):
        full = occ_ref[x, y, z, :].reshape(1, slots).astype(jnp.float32)
        pol = pol_ref[x, y, z, :].reshape(1, slots)
        scaled[t] = jnp.broadcast_to(RELAXATION * full * pol, (ROWS, slots))
        tile = jnp.concatenate(
            [frac_ref[c, x, y, z, :].reshape(1, slots) * CELL_EDGE for c in range(3)]
            + [lax.rsqrt(pol)] + [zero_row] * (ROWS - 4),
            axis=0,
        )
        geom[x, y, z] = tile
        for h in range(steps):
            moment = jnp.concatenate(
                [hist_ref[h, c, x, y, z, :].reshape(1, slots) for c in range(rows)], axis=0
            )
            past_sets[h, t] = jnp.concatenate([moment * full, spare], axis=0)
        fixed[t] = jnp.concatenate(
            [perm_ref[c, x, y, z, :].reshape(1, slots) for c in range(rows)] + [spare], axis=0
        )
    pair_lane = {}
    gram = zero_row
    for a in range(steps):
        for b in range(a, steps):
            product = past_sets[a, 0] * past_sets[b, 0]
            for t in range(1, len(places)):
                product = product + past_sets[a, t] * past_sets[b, t]
            value = jnp.sum(jnp.sum(product, axis=0, keepdims=True), axis=1, keepdims=True)
            pair_lane[(a, b)] = len(pair_lane)
            gram = jnp.where(lane == pair_lane[(a, b)], value, gram)
    slots_a[pl.ds(me, 1)] = gram.reshape(1, 1, slots)


    wraps = tuple(n + 2 for n in tiles)
    row_of = lax.broadcasted_iota(jnp.int32, (ROWS, slots), 0)
    count = len(places)
    wide = tiles[2] * slots
    levels = list(range(tiles[2])) + [-1, tiles[2]]

    def wrap(value, size):
        return jnp.where(value < 0, value + size, value)

    def pieces(value):
        high = value.astype(jnp.bfloat16).astype(jnp.float32)
        value = value - high
        middle = value.astype(jnp.bfloat16).astype(jnp.float32)
        return high, middle, value - middle

    def rows_in(*which):
        result = row_of == which[0]
        for row in which[1:]:
            result = jnp.logical_or(result, row_of == row)
        return result

    def mix(base, *choices):
        for where, value in choices:
            base = jnp.where(where, value, base)
        return base

    one_tile = jnp.ones((ROWS, slots), jnp.float32)
    zero_tile = jnp.zeros((ROWS, slots), jnp.float32)

    pair_a, pair_b, pair_c, pair_d = rows_in(1, 6), rows_in(2, 4), rows_in(0, 4), rows_in(2, 5)
    row = [row_of == number for number in range(ROWS)]
    damp_m, damp_l = rows_in(2, 5, 6), rows_in(4, 7)
    damp_m_i, damp_l_i = rows_in(1, 5, 7), rows_in(3, 6)

    def split_rows(slot):
        tile = spots[slot[0], slot[1], slot[2]]
        for number, value in enumerate(pieces(tile) + pieces(tile * tile)):
            split_ref[slot[0], slot[1], slot[2], number] = value

        def take(c, *numbers):
            return [
                jnp.broadcast_to(split_ref[slot[0], slot[1], slot[2], number, pl.ds(c, 1), :], (ROWS, slots))
                for number in numbers
            ]

        return take

    def padded(parts):
        return parts + [zero_tile] * (slots // ROWS - len(parts))

    def source_features(slot):
        take = split_rows(slot)
        parts = []
        for c in range(3):
            high, middle, low, square, square_middle, square_low = take(c, 0, 1, 2, 3, 4, 5)
            parts.append(
                mix(
                    square, (pair_a, one_tile), (pair_b, high), (row[3], square_middle),
                    (row[5], middle), (row[7], square_low),
                )
            )
            parts.append(mix(zero_tile, (pair_c, middle), (row[1], high), (pair_d, low), (row[3], one_tile)))
        high, middle, low = take(3, 0, 1, 2)
        parts.append(mix(high, (damp_m, middle), (damp_l, low)))
        return jnp.concatenate(padded(parts), axis=0).astype(jnp.bfloat16)

    def taker_features(slot):
        take = split_rows(slot)
        parts = []
        for c in range(3):
            high, middle, low, square, square_middle, square_low = take(c, 0, 1, 2, 3, 4, 5)
            high, middle, low = -2.0 * high, -2.0 * middle, -2.0 * low
            parts.append(
                mix(
                    one_tile, (row[1], square), (rows_in(2, 5), high), (row[4], middle),
                    (row[6], square_middle),
                )
            )
            parts.append(
                mix(
                    zero_tile, (rows_in(0, 5), middle), (rows_in(1, 4), low), (row[2], high),
                    (row[3], square_low),
                )
            )
        value = jnp.broadcast_to(spots[slot[0], slot[1], slot[2], pl.ds(3, 1), :], (ROWS, slots))
        high, middle, low = pieces(value * -THOLE_DAMP)
        damp = mix(high, (damp_m_i, middle), (damp_l_i, low))
        far = jnp.concatenate(padded(parts), axis=0).astype(jnp.bfloat16)
        fade = jnp.concatenate(padded([zero_tile] * len(parts) + [damp]), axis=0).astype(jnp.bfloat16)
        return far, fade

    def settle(place, slot):
        tile = geom[slot[0], slot[1], slot[2]]
        shift = jnp.zeros((ROWS, slots), jnp.float32)
        for axis in range(3):
            corner = CELL_EDGE * (jnp.asarray(place[axis], jnp.float32) - 0.5 * tiles[axis])
            shift = jnp.where(row_of == axis, corner, shift)
        tile = tile + shift
        spots[slot[0], slot[1], slot[2]] = tile
        features[slot[0], slot[1], slot[2]] = source_features(slot).T
        one = jnp.ones((2, slots), jnp.float32)
        turns[0, slot[0], slot[1], slot[2]] = jnp.concatenate(
            [tile[0:3], tile[0:3], jnp.zeros((2, slots), jnp.float32)], axis=0
        )
        turns[1, slot[0], slot[1], slot[2]] = jnp.concatenate([one, tile[0:3], tile[0:3]], axis=0)

    def settle_all(xs, ys, zs):
        def one(step, carry):
            x = step + xs[0]
            for y in ys:
                for z in zs:
                    settle((x, y, z), (wrap(x, wraps[0]), y % wraps[1], z % wraps[2]))
            return carry

        lax.fori_loop(0, len(xs), one, 0)

    near_y, far_y = list(range(tiles[1])), [-1, tiles[1]]
    every_x = list(range(-1, tiles[0] + 1))
    own_z, side_z = list(range(tiles[2])), [-1, tiles[2]]

    def geometry(x, y, along_x, along_y, zs):
        nine = (along_x + 1) * 3 + (along_y + 1)
        line = x * tiles[1] + y
        slot_x, slot_y = wrap(x + along_x, wraps[0]), wrap(y + along_y, wraps[1])
        for level in zs:
            spot_at = levels.index(level)
            slot_z = level % wraps[2]
            takers = [z for z in range(tiles[2]) if abs(level - z) <= 1]
            softs = [
                SOFTENING + (1 - mask_ref[x, y, z, nine * 3 + level - z + 1]).astype(jnp.float32) * APART
                for z in takers
            ]
            lanes = slice(takers[0] * slots, (takers[-1] + 1) * slots)
            left = features[slot_x, slot_y, slot_z]
            squares = jnp.dot(left, distance[line, :, lanes], preferred_element_type=jnp.float32)
            damps = jnp.dot(left, damping[line, :, lanes], preferred_element_type=jnp.float32)
            for first in range(0, slots, BLOCK):
                part = pl.ds(first, BLOCK)
                for z, soft in zip(takers, softs):
                    at_lane = (z - takers[0]) * slots
                    square = squares[first : first + BLOCK, at_lane : at_lane + slots] + soft
                    damp = damps[first : first + BLOCK, at_lane : at_lane + slots]
                    root = lax.rsqrt(square)
                    root_two = root * root
                    cube = root_two * root
                    arg = (square * root) * square * damp
                    faded = jnp.exp(arg) * cube
                    direct = cube - faded
                    radial = (direct + arg * faded) * root_two
                    for number, value in ((0, radial), (2, direct)):
                        high = value.astype(jnp.bfloat16)
                        low = (value - high.astype(jnp.float32)).astype(jnp.bfloat16)
                        links[line, nine, number, spot_at, part, z * slots : (z + 1) * slots] = high
                        links[line, nine, number + 1, spot_at, part, z * slots : (z + 1) * slots] = low

    def geometry_near(along_x, zs):
        for to_y in range(tiles[1]):
            for x in range(tiles[0]):
                for y in range(tiles[1]):
                    if abs(to_y - y) <= 1:
                        geometry(x, y, along_x, to_y - y, zs)

    def plane_of(along_x):
        return jnp.where(along_x > 0, tiles[0], -1)

    def settle_plane(along_x, ys, zs):
        plane = plane_of(along_x)
        for y in ys:
            for z in zs:
                settle((plane, y, z), (wrap(plane, wraps[0]), y % wraps[1], z % wraps[2]))

    def arrive(copies, kinds_of):
        for move, copy in zip(moves, copies):
            if move[1][0] != 0:
                kind = "far"
            else:
                kind = ("x" if move[0][0] != 0 else "") + ("z" if move[2][0] != 0 else "")
            if kind in kinds_of:
                copy.wait()

    def geometry_far(first, last):
        def one(step, carry):
            x = step % tiles[0]
            side = step // tiles[0] % 2
            along_x = step // (2 * tiles[0]) - 1
            geometry(x, side * (tiles[1] - 1), along_x, 2 * side - 1, levels)
            return carry

        lax.fori_loop(first * tiles[0], last * tiles[0], one, 0, unroll=True)

    own_x = list(range(tiles[0]))
    settle_all(own_x, near_y, own_z)
    for x, y, z in places:
        lanes = slice(z * slots, (z + 1) * slots)
        far, fade = taker_features((x, y, z))
        distance[x * tiles[1] + y, :, lanes] = far
        damping[x * tiles[1] + y, :, lanes] = fade
    geometry_near(0, own_z)
    off_diagonal = lax.broadcasted_iota(jnp.int32, (slots, slots), 0) != lax.broadcasted_iota(
        jnp.int32, (slots, slots), 1
    )
    for x, y, z in places:
        lanes = slice(z * slots, (z + 1) * slots)
        for number in range(STREAMS):
            link = links[x * tiles[1] + y, 4, number, levels.index(z), :, lanes].astype(jnp.float32)
            links[x * tiles[1] + y, 4, number, levels.index(z), :, lanes] = jnp.where(
                off_diagonal, link, 0.0
            ).astype(jnp.bfloat16)

    pl.semaphore_wait(barrier, total_devices - 1)
    geom_copies = halo(geom, send_geom, recv_geom, 4)
    near_count = sum(1 for move in moves if move[1][0] == 0)
    for copy in geom_copies[:near_count]:
        copy.start()
    everyone(0, slots_a)
    for copy in geom_copies[near_count:]:
        copy.start()
    geom_parts = (geom, send_geom, recv_geom, 4)
    arrive_x(*geom_parts, first_move)
    settle_plane(first_x, near_y, own_z)
    geometry_near(first_x, own_z)
    arrive(geom_copies, ("z",))
    settle_all(own_x, near_y, side_z)
    geometry_near(0, side_z)
    arrive_x(*geom_parts, second_move)
    arrive(geom_copies, ("xz",))
    settle_plane(first_x, near_y, side_z)
    settle_plane(second_x, near_y, levels)
    geometry_near(first_x, side_z)

    everyone_wait(0, slots_a)
    total = jnp.sum(slots_a[...], axis=0)
    coeffs = solve_fit(total, past, lane, pair_lane)
    for t, (x, y, z) in enumerate(places):
        value = coeffs[0] * past_sets[1, t]
        for h in range(1, past):
            value = value + coeffs[h] * past_sets[h + 1, t]
        held_one[x, y, z] = value
    one_copies = halo(held_one, send_one, recv_one, rows)
    for copy in one_copies:
        copy.start()
    geometry_near(second_x, levels)
    arrive(geom_copies, ("far",))
    settle_all(every_x, far_y, levels)

    kinds = 5

    def weigh(held, xs, ys, zs):
        for x in xs:
            for y in ys:
                for z in zs:
                    slot = (wrap(x, wraps[0]), y % wraps[1], z % wraps[2])
                    moment = jnp.where(row_of < rows, held[slot], 0.0)
                    along = moment * turns[(0,) + slot]
                    first = jnp.sum(jnp.where(row_of < 3, along, 0.0), axis=0, keepdims=True)
                    second = jnp.sum(jnp.where(row_of < 3, 0.0, along), axis=0, keepdims=True)
                    which = jnp.logical_or(row_of == 0, jnp.logical_and(row_of >= 2, row_of < 5))
                    both = jnp.where(which, first, second) * turns[(1,) + slot]
                    tiles_of = [moment, both] + [
                        spots[slot + (pl.ds(c, 1), slice(None))] * moment for c in range(3)
                    ]
                    parts = [[], [], []]
                    for value in tiles_of:
                        for level in range(3):
                            piece = value.astype(jnp.bfloat16).astype(jnp.float32)
                            parts[level].append(piece)
                            value = value - piece
                    order = [parts[0][0], parts[1][0], parts[2][0]]
                    for level in range(3):
                        order = order + parts[level][1:]
                    order.append(jnp.zeros((ROWS, slots), jnp.float32))
                    weights[slot] = jnp.concatenate(order, axis=0).astype(jnp.bfloat16)

    def products(line, visits):
        main = jnp.zeros((SPREAD, wide), jnp.float32)
        rest = jnp.zeros((SPREAD_LOW, wide), jnp.float32)
        plain = jnp.zeros((SPREAD_PLAIN, wide), jnp.float32)
        blank = jnp.zeros((slots, slots), jnp.bfloat16)
        for nine, slot_x, slot_y, zs in visits:
            for start in range(0, len(zs), 2):
                chunk = [levels.index(z) for z in zs[start : start + 2]]
                left = jnp.concatenate(
                    [weights[slot_x, slot_y, levels[i] % wraps[2]] for i in chunk], axis=1
                )

                def matrix(number):
                    lines = []
                    for i in chunk:
                        lines.append(
                            jnp.concatenate(
                                [
                                    links[line, nine, number, i, :, z * slots : (z + 1) * slots]
                                    if abs(levels[i] - z) <= 1
                                    else blank
                                    for z in range(tiles[2])
                                ],
                                axis=1,
                            )
                        )
                    return jnp.concatenate(lines, axis=0)

                def times(values, number):
                    return jnp.dot(values, matrix(number), preferred_element_type=jnp.float32)

                main = main + times(left, 0)
                rest = rest + times(left[0:SPREAD_LOW], 1)
                plain = plain + times(left[0:SPREAD_PLAIN], 2)
                plain = plain + times(left[0:SPREAD_PLAIN], 3)
        return main, rest, plain

    def near_products(x, y, parts):
        visits = [
            ((along + 1) * 3 + to_y - y + 1, wrap(x + along, wraps[0]), to_y, zs)
            for along, zs in parts
            for to_y in range(tiles[1])
        ]
        return products(x * tiles[1] + y, visits)

    def far_products(x, y, side):
        visits = [
            ((along + 1) * 3 + 2 * side, wrap(x + along, wraps[0]), wrap((tiles[1] + 1) * side - 1, wraps[1]), levels)
            for along in (-1, 0, 1)
        ]
        return products(x * tiles[1] + y, visits)

    partials = (partial_main, partial_rest, partial_plain)

    def gather(parts, start, which=None):
        def one(step, carry):
            sums = near_products(step // tiles[1], step % tiles[1], parts)
            for partial, value in zip(partials, sums):
                partial[step] = value if start else partial[step] + value
            return carry

        first, last = which or (0, tiles[0] * tiles[1])
        lax.fori_loop(first, last, one, 0, unroll=True)

    def field_of(x, y, main, rest, plain):
        def tile(value, index):
            return value[index * ROWS : (index + 1) * ROWS]

        def both_sum(first):
            total = tile(main, first[0]) + tile(rest, first[0])
            for index in first[1:]:
                total = total + tile(main, index)
                if (index + 1) * ROWS <= SPREAD_LOW:
                    total = total + tile(rest, index)
            return total

        moment = both_sum((0, 1, 2))
        both = both_sum((3, 7, 11))
        lifts = [both_sum((4 + c, 8 + c, 12 + c)) for c in range(3)]
        straight = tile(plain, 0) + tile(plain, 1) + tile(plain, 2)
        result = []
        for z in range(tiles[2]):
            lanes = slice(z * slots, (z + 1) * slots)
            turn = turns[0, x, y, z]
            inner = []
            for c in range(3):
                along = (lifts[c][:, lanes] - spots[x, y, z, pl.ds(c, 1), :] * moment[:, lanes]) * turn
                first = jnp.sum(jnp.where(row_of < 3, along, 0.0), axis=0, keepdims=True)
                second = jnp.sum(jnp.where(row_of < 3, 0.0, along), axis=0, keepdims=True)
                inner.append((first, second))
            inner = jnp.concatenate(
                [inner[c][0] for c in range(3)] + [inner[c][1] for c in range(3)] + [zero_row, zero_row], axis=0
            )
            lifted = jnp.concatenate([both[2:8, lanes], zero_row, zero_row], axis=0)
            dots = jnp.where(row_of < 3, both[0:1, lanes], both[1:2, lanes])
            result.append(3.0 * (lifted - dots * turn - inner) - straight[:, lanes])
        return result

    lines = tiles[0] * tiles[1]

    def field(step, held, act):
        x, y = step // tiles[1], step % tiles[1]
        main, rest, plain = partial_main[step], partial_rest[step], partial_plain[step]
        for side in range(2):
            if tiles[1] == 1:
                more = far_products(x, y, side)
                main, rest, plain = main + more[0], rest + more[1], plain + more[2]
        if tiles[1] > 1:
            side = y // (tiles[1] - 1)
            more = far_products(x, y, side)
            keep = jnp.logical_or(y == 0, y == tiles[1] - 1).astype(jnp.float32)
            if tiles[1] > 2:
                more = tuple(jnp.where(keep > 0.5, value, 0.0) for value in more)
            main, rest, plain = main + more[0], rest + more[1], plain + more[2]
        fields = field_of(x, y, main, rest, plain)
        for z in range(tiles[2]):
            t = step * tiles[2] + z
            act(x, y, z, t, (1.0 - RELAXATION) * held[x, y, z] + scaled[t] * (fixed[t] + fields[z]))

    def arrive_near(parts, copies):
        arrive_x(*parts, first_move)
        arrive_x(*parts, second_move)
        arrive(copies, ("z", "xz"))

    def first_near(held, parts, copies):
        weigh(held, own_x, near_y, own_z)
        lines_half = (tiles[0] * tiles[1] + 1) // 2
        halves = ((0, lines_half), (lines_half, tiles[0] * tiles[1]))
        geometry_far(0, 1)
        gather([(0, own_z)], True, halves[0])
        geometry_far(1, 2)
        gather([(0, own_z)], True, halves[1])
        geometry_far(2, 4)
        arrive_near(parts, copies)
        weigh(held, own_x, near_y, side_z)
        weigh(held, [-1, tiles[0]], near_y, levels)
        near_parts = [(0, side_z), (-1, levels), (1, levels)]
        geometry_far(4, 5)
        gather(near_parts, False, halves[0])
        geometry_far(5, 6)
        gather(near_parts, False, halves[1])

    def second_near(held, parts, copies):
        weigh(held, own_x, near_y, own_z)
        gather([(0, own_z)], True)
        arrive_x(*parts, first_move)
        weigh(held, [plane_of(first_x)], near_y, own_z)
        gather([(first_x, own_z)], False)
        arrive(copies, ("z",))
        weigh(held, own_x, near_y, side_z)
        gather([(0, side_z)], False)
        arrive_x(*parts, second_move)
        arrive(copies, ("xz",))
        weigh(held, [plane_of(first_x)], near_y, side_z)
        weigh(held, [plane_of(second_x)], near_y, levels)
        gather([(first_x, side_z), (second_x, levels)], False)

    def sweep(held, copies, act):
        arrive(copies, ("far",))
        weigh(held, every_x, far_y, levels)

        def one(step, carry):
            field(step, held, act)
            return carry

        lax.fori_loop(0, lines, one, 0, unroll=True)

    def first_act(x, y, z, t, value):
        held_two[x, y, z] = value

    first_near(held_one, (held_one, send_one, recv_one, rows), one_copies)
    sweep(held_one, one_copies, first_act)
    two_copies = halo(held_two, send_two, recv_two, rows)
    for copy in two_copies:
        copy.start()

    def second_act(x, y, z, t, value):
        held_one[x, y, z] = value

    second_near(held_two, (held_two, send_two, recv_two, rows), two_copies)
    sweep(held_two, two_copies, second_act)
    changed = jnp.zeros((ROWS, slots), jnp.float32)
    size = jnp.zeros((ROWS, slots), jnp.float32)
    for t, (x, y, z) in enumerate(places):
        before, after = held_two[x, y, z], held_one[x, y, z]
        for c in range(rows):
            out_ref[c, x, y, z, :] = after[c]
        changed = changed + (after - before) * (after - before)
        size = size + after * after
    put = pltpu.make_async_copy(out_ref, out_hbm, load_sem.at[len(loads)])
    put.start()

    pair = jnp.concatenate(
        [jnp.sum(value, axis=0, keepdims=True) for value in (changed, size)], axis=1
    )
    slots_b[pl.ds(me, 1)] = pair.reshape(1, 1, 2 * slots)
    everyone(1, slots_b)
    everyone_wait(1, slots_b)
    pair = jnp.sum(slots_b[...], axis=0)
    above = jnp.sum(pair[:, 0:slots], axis=1, keepdims=True)
    below = jnp.sum(pair[:, slots : 2 * slots], axis=1, keepdims=True)
    change_ref[...] = jnp.broadcast_to(jnp.sqrt(above / (below + 1.0)), (1, slots))
    put.wait()


def solution(mesh):
    devices = tuple(mesh.shape[axis] for axis in AXES)
    total_devices = devices[0] * devices[1] * devices[2]

    def on_device(fractions, polarizability, occupancy, pair_mask, perm_field, history):
        tiles = fractions.shape[1:4]
        slots = fractions.shape[4]
        count = tiles[0] * tiles[1] * tiles[2]
        lines = tiles[0] * tiles[1]
        wraps = tuple(n + 2 for n in tiles)
        moves = len(halo_moves(devices, tiles))
        rows = history.shape[1]
        vmem = pl.BlockSpec(memory_space=pltpu.VMEM)
        f32 = jnp.float32
        induced, change = pl.pallas_call(
            functools.partial(kernel, devices),
            out_shape=(
                jax.ShapeDtypeStruct(perm_field.shape, f32),
                jax.ShapeDtypeStruct((1, slots), f32),
            ),
            in_specs=[pl.BlockSpec(memory_space=pltpu.HBM)] * 6,
            out_specs=(pl.BlockSpec(memory_space=pltpu.HBM), vmem),
            scratch_shapes=[
                pltpu.VMEM(perm_field.shape, f32),
                pltpu.VMEM(fractions.shape, f32),
                pltpu.VMEM(polarizability.shape, f32),
                pltpu.VMEM(occupancy.shape, jnp.int32),
                pltpu.SMEM(pair_mask.shape, jnp.int32),
                pltpu.VMEM(perm_field.shape, f32),
                pltpu.VMEM(history.shape, f32),
                pltpu.VMEM(wraps + (ROWS, slots), f32),
                pltpu.VMEM(wraps + (ROWS, slots), f32),
                pltpu.VMEM(wraps + (ROWS, slots), f32),
                pltpu.VMEM((history.shape[0], count, ROWS, slots), f32),
                pltpu.VMEM(wraps + (ROWS, slots), f32),
                pltpu.VMEM(wraps + (6, ROWS, slots), f32),
                pltpu.VMEM(wraps + (slots, slots), jnp.bfloat16),
                pltpu.VMEM((lines, slots, tiles[2] * slots), jnp.bfloat16),
                pltpu.VMEM((lines, slots, tiles[2] * slots), jnp.bfloat16),
                pltpu.VMEM((2,) + wraps + (ROWS, slots), f32),
                pltpu.VMEM((lines, 9, STREAMS, wraps[2], slots, tiles[2] * slots), jnp.bfloat16),
                pltpu.VMEM(wraps + (SPREAD, slots), jnp.bfloat16),
                pltpu.VMEM((lines, SPREAD, tiles[2] * slots), f32),
                pltpu.VMEM((lines, SPREAD_LOW, tiles[2] * slots), f32),
                pltpu.VMEM((lines, SPREAD_PLAIN, tiles[2] * slots), f32),
                pltpu.VMEM((count, ROWS, slots), f32),
                pltpu.VMEM((count, ROWS, slots), f32),
                pltpu.VMEM((total_devices, 1, slots), f32),
                pltpu.VMEM((total_devices, 1, 2 * slots), f32),
                pltpu.SemaphoreType.DMA((7,)),
                pltpu.SemaphoreType.DMA((2,)),
                pltpu.SemaphoreType.DMA((2,)),
            ]
            + [pltpu.SemaphoreType.DMA((moves,))] * 6,
            compiler_params=pltpu.CompilerParams(
                collective_id=0, has_side_effects=True, vmem_limit_bytes=67043328
            ),
        )(fractions, polarizability, occupancy, pair_mask, perm_field, history)
        return induced, change[0, 0]

    in_specs = (
        P(None, "gx", "gy", "gz", None),
        P("gx", "gy", "gz", None),
        P("gx", "gy", "gz", None),
        P("gx", "gy", "gz", None),
        P(None, "gx", "gy", "gz", None),
        P(None, None, "gx", "gy", "gz", None),
    )
    out_specs = (P(None, "gx", "gy", "gz", None), P())
    return jax.shard_map(
        on_device, mesh=mesh, in_specs=in_specs, out_specs=out_specs, check_vma=False
    )
```

```python
import functools

import jax
import jax.numpy as jnp
from jax import lax
from jax.experimental import pallas as pl
from jax.experimental.pallas import tpu as pltpu
from jax.sharding import PartitionSpec as P

CELL_EDGE = 10.0
SOFTENING = 0.3
THOLE_DAMP = 0.39
RELAXATION = 0.7
MESH = pl.DeviceIdType.MESH
AXES = ("gx", "gy", "gz")
ROWS = 8
BLOCK = 16
APART = 2.5e25
STREAMS = 4
SPREAD = 128
SPREAD_LOW = 96
SPREAD_PLAIN = 32


def halo_moves(devices, tiles):
    options = []
    for count, n in zip(devices, tiles):
        if count == 2 and n == 2:
            around = [(1, 0, 2, 2)]
        else:
            around = [(1, n - 1, 1, n + 1), (-1, 0, 1, n)]
        options.append([(0, 0, n, 0)] + around)
    return [
        (a, b, c) for a in options[0] for b in options[1] for c in options[2] if (a[0], b[0], c[0]) != (0, 0, 0)
    ]


def solve_fit(total, past, lane, pair_lane):
    def pick(a, b):
        index = pair_lane[(min(a, b), max(a, b))]
        return jnp.sum(jnp.where(lane == index, total, 0.0), axis=1, keepdims=True)

    diagonal = [pick(a, a) for a in range(past)]
    trace = diagonal[0]
    for value in diagonal[1:]:
        trace = trace + value
    ridge = 0.001 * trace / past + 1.0
    lower, inverse = {}, []
    for j in range(past):
        pivot = diagonal[j] + ridge
        for m in range(j):
            pivot = pivot - lower[j, m] * lower[j, m]
        inverse.append(1.0 / jnp.sqrt(pivot))
        for i in range(j + 1, past):
            value = pick(i, j)
            for m in range(j):
                value = value - lower[i, m] * lower[j, m]
            lower[i, j] = value * inverse[j]
    forward = []
    for i in range(past):
        value = pick(i, past)
        for m in range(i):
            value = value - lower[i, m] * forward[m]
        forward.append(value * inverse[i])
    coeffs = [None] * past
    for i in reversed(range(past)):
        value = forward[i]
        for m in range(i + 1, past):
            value = value - lower[m, i] * coeffs[m]
        coeffs[i] = value * inverse[i]
    return coeffs


def kernel(
    devices,
    frac_in, pol_in, occ_in, mask_in, perm_in, hist_in,
    out_hbm, change_ref,
    out_ref,
    frac_ref, pol_ref, occ_ref, mask_ref, perm_ref, hist_ref,
    geom, held_one, held_two, past_sets, spots, split_ref, features, distance, damping, turns, links, weights,
    partial_main, partial_rest, partial_plain, scaled, fixed, slots_a, slots_b,
    load_sem, send_all, recv_all, send_geom, recv_geom, send_one, recv_one, send_two, recv_two,
):
    tiles = tuple(frac_ref.shape[1:4])
    slots = frac_ref.shape[4]
    steps = hist_ref.shape[0]
    rows = hist_ref.shape[1]
    past = steps - 1
    total_devices = devices[0] * devices[1] * devices[2]
    at = [lax.axis_index(axis) for axis in AXES]
    me = (at[0] * devices[1] + at[1]) * devices[2] + at[2]
    moves = sorted(halo_moves(devices, tiles), key=lambda move: (move[1][0] != 0, sum(abs(part[0]) for part in move)))
    lane = lax.broadcasted_iota(jnp.int32, (1, slots), 1)
    loads = [
        pltpu.make_async_copy(source, target, load_sem.at[number])
        for number, (source, target) in enumerate(
            (
                (hist_in, hist_ref), (occ_in, occ_ref), (frac_in, frac_ref),
                (pol_in, pol_ref), (perm_in, perm_ref), (mask_in, mask_ref),
            )
        )
    ]
    for load in loads:
        load.start()

    def each_other(act):
        def pair(step, carry):
            down, across = step // devices[0], step % devices[0]
            x = at[0] + across
            x = jnp.where(x >= devices[0], x - devices[0], x)
            y = jnp.where(2 * at[1] < devices[1], devices[1] - 1 - down, down)
            for shift in range(devices[2] - 1, -1, -1):
                last = at[2] + shift
                last = jnp.where(last >= devices[2], last - devices[2], last)
                if shift == 0:
                    @pl.when(jnp.logical_or(across > 0, y != at[1]))
                    def _():
                        act((x, y, last))
                else:
                    act((x, y, last))
            return carry

        lax.fori_loop(0, devices[0] * devices[1], pair, 0, unroll=8)

    barrier = pltpu.get_barrier_semaphore()

    each_other(
        lambda device: pl.semaphore_signal(barrier, inc=1, device_id=device, device_id_type=MESH)
    )
    for load in loads:
        load.wait()

    def everyone(index, held):
        def start(device):
            pltpu.make_async_remote_copy(
                src_ref=held.at[pl.ds(me, 1)],
                dst_ref=held.at[pl.ds(me, 1)],
                send_sem=send_all.at[index],
                recv_sem=recv_all.at[index],
                device_id=device,
                device_id_type=MESH,
            ).start()

        each_other(start)

    def everyone_wait(index, held):
        whole = pltpu.make_async_remote_copy(
            src_ref=held.at[pl.ds(0, total_devices - 1)],
            dst_ref=held.at[pl.ds(0, total_devices - 1)],
            send_sem=send_all.at[index],
            recv_sem=recv_all.at[index],
            device_id=(at[0], at[1], (at[2] + 1) % devices[2]),
            device_id_type=MESH,
        )
        whole.wait_send()
        whole.wait_recv()

    def halo(held, send, recv, depth):
        copies = []
        for number, move in enumerate(moves):
            source = tuple(pl.ds(part[1], part[2]) for part in move)
            place = tuple(pl.ds(part[3], part[2]) for part in move)
            target = tuple((at[axis] + move[axis][0] + devices[axis]) % devices[axis] for axis in range(3))
            copies.append(
                pltpu.make_async_remote_copy(
                    src_ref=held.at[source + (pl.ds(0, depth),)],
                    dst_ref=held.at[place + (pl.ds(0, depth),)],
                    send_sem=send.at[number],
                    recv_sem=recv.at[number],
                    device_id=target,
                    device_id_type=MESH,
                )
            )
        return copies

    x_moves = {
        move[0][0]: number
        for number, move in enumerate(moves)
        if move[0][0] != 0 and move[1][0] == 0 and move[2][0] == 0
    }
    if len(x_moves) == 2:
        first_x = jnp.where(at[0] % 2 == 0, 1, -1)
        second_x = -first_x
        first_move = jnp.where(at[0] % 2 == 0, x_moves[-1], x_moves[1])
        second_move = x_moves[-1] + x_moves[1] - first_move
    else:
        first_x, second_x = 1, -1
        first_move, second_move = x_moves[1], None

    def arrive_x(held, send, recv, depth, number):
        if number is None:
            return
        move = moves[x_moves[1]]
        pltpu.make_async_remote_copy(
            src_ref=held.at[tuple(pl.ds(part[1], part[2]) for part in move) + (pl.ds(0, depth),)],
            dst_ref=held.at[tuple(pl.ds(part[3], part[2]) for part in move) + (pl.ds(0, depth),)],
            send_sem=send.at[number],
            recv_sem=recv.at[number],
            device_id=tuple((at[axis] + move[axis][0] + devices[axis]) % devices[axis] for axis in range(3)),
            device_id_type=MESH,
        ).wait()

    places = [(x, y, z) for x in range(tiles[0]) for y in range(tiles[1]) for z in range(tiles[2])]
    zero_row = jnp.zeros((1, slots), jnp.float32)
    spare = jnp.zeros((ROWS - rows, slots), jnp.float32)
    for t, (x, y, z) in enumerate(places):
        full = occ_ref[x, y, z, :].reshape(1, slots).astype(jnp.float32)
        pol = pol_ref[x, y, z, :].reshape(1, slots)
        scaled[t] = jnp.broadcast_to(RELAXATION * full * pol, (ROWS, slots))
        tile = jnp.concatenate(
            [frac_ref[c, x, y, z, :].reshape(1, slots) * CELL_EDGE for c in range(3)]
            + [lax.rsqrt(pol)] + [zero_row] * (ROWS - 4),
            axis=0,
        )
        geom[x, y, z] = tile
        for h in range(steps):
            moment = jnp.concatenate(
                [hist_ref[h, c, x, y, z, :].reshape(1, slots) for c in range(rows)], axis=0
            )
            past_sets[h, t] = jnp.concatenate([moment * full, spare], axis=0)
        fixed[t] = jnp.concatenate(
            [perm_ref[c, x, y, z, :].reshape(1, slots) for c in range(rows)] + [spare], axis=0
        )
    pair_lane = {}
    gram = zero_row
    for a in range(steps):
        for b in range(a, steps):
            product = past_sets[a, 0] * past_sets[b, 0]
            for t in range(1, len(places)):
                product = product + past_sets[a, t] * past_sets[b, t]
            value = jnp.sum(jnp.sum(product, axis=0, keepdims=True), axis=1, keepdims=True)
            pair_lane[(a, b)] = len(pair_lane)
            gram = jnp.where(lane == pair_lane[(a, b)], value, gram)
    slots_a[pl.ds(me, 1)] = gram.reshape(1, 1, slots)


    wraps = tuple(n + 2 for n in tiles)
    row_of = lax.broadcasted_iota(jnp.int32, (ROWS, slots), 0)
    count = len(places)
    wide = tiles[2] * slots
    levels = list(range(tiles[2])) + [-1, tiles[2]]

    def wrap(value, size):
        return jnp.where(value < 0, value + size, value)

    def pieces(value):
        high = value.astype(jnp.bfloat16).astype(jnp.float32)
        value = value - high
        middle = value.astype(jnp.bfloat16).astype(jnp.float32)
        return high, middle, value - middle

    def rows_in(*which):
        result = row_of == which[0]
        for row in which[1:]:
            result = jnp.logical_or(result, row_of == row)
        return result

    def mix(base, *choices):
        for where, value in choices:
            base = jnp.where(where, value, base)
        return base

    one_tile = jnp.ones((ROWS, slots), jnp.float32)
    zero_tile = jnp.zeros((ROWS, slots), jnp.float32)

    pair_a, pair_b, pair_c, pair_d = rows_in(1, 6), rows_in(2, 4), rows_in(0, 4), rows_in(2, 5)
    row = [row_of == number for number in range(ROWS)]
    damp_m, damp_l = rows_in(2, 5, 6), rows_in(4, 7)
    damp_m_i, damp_l_i = rows_in(1, 5, 7), rows_in(3, 6)

    def split_rows(slot):
        tile = spots[slot[0], slot[1], slot[2]]
        for number, value in enumerate(pieces(tile) + pieces(tile * tile)):
            split_ref[slot[0], slot[1], slot[2], number] = value

        def take(c, *numbers):
            return [
                jnp.broadcast_to(split_ref[slot[0], slot[1], slot[2], number, pl.ds(c, 1), :], (ROWS, slots))
                for number in numbers
            ]

        return take

    def padded(parts):
        return parts + [zero_tile] * (slots // ROWS - len(parts))

    def source_features(slot):
        take = split_rows(slot)
        parts = []
        for c in range(3):
            high, middle, low, square, square_middle, square_low = take(c, 0, 1, 2, 3, 4, 5)
            parts.append(
                mix(
                    square, (pair_a, one_tile), (pair_b, high), (row[3], square_middle),
                    (row[5], middle), (row[7], square_low),
                )
            )
            parts.append(mix(zero_tile, (pair_c, middle), (row[1], high), (pair_d, low), (row[3], one_tile)))
        high, middle, low = take(3, 0, 1, 2)
        parts.append(mix(high, (damp_m, middle), (damp_l, low)))
        return jnp.concatenate(padded(parts), axis=0).astype(jnp.bfloat16)

    def taker_features(slot):
        take = split_rows(slot)
        parts = []
        for c in range(3):
            high, middle, low, square, square_middle, square_low = take(c, 0, 1, 2, 3, 4, 5)
            high, middle, low = -2.0 * high, -2.0 * middle, -2.0 * low
            parts.append(
                mix(
                    one_tile, (row[1], square), (rows_in(2, 5), high), (row[4], middle),
                    (row[6], square_middle),
                )
            )
            parts.append(
                mix(
                    zero_tile, (rows_in(0, 5), middle), (rows_in(1, 4), low), (row[2], high),
                    (row[3], square_low),
                )
            )
        value = jnp.broadcast_to(spots[slot[0], slot[1], slot[2], pl.ds(3, 1), :], (ROWS, slots))
        high, middle, low = pieces(value * -THOLE_DAMP)
        damp = mix(high, (damp_m_i, middle), (damp_l_i, low))
        far = jnp.concatenate(padded(parts), axis=0).astype(jnp.bfloat16)
        fade = jnp.concatenate(padded([zero_tile] * len(parts) + [damp]), axis=0).astype(jnp.bfloat16)
        return far, fade

    def settle(place, slot):
        tile = geom[slot[0], slot[1], slot[2]]
        shift = jnp.zeros((ROWS, slots), jnp.float32)
        for axis in range(3):
            corner = CELL_EDGE * (jnp.asarray(place[axis], jnp.float32) - 0.5 * tiles[axis])
            shift = jnp.where(row_of == axis, corner, shift)
        tile = tile + shift
        spots[slot[0], slot[1], slot[2]] = tile
        features[slot[0], slot[1], slot[2]] = source_features(slot).T
        one = jnp.ones((2, slots), jnp.float32)
        turns[0, slot[0], slot[1], slot[2]] = jnp.concatenate(
            [tile[0:3], tile[0:3], jnp.zeros((2, slots), jnp.float32)], axis=0
        )
        turns[1, slot[0], slot[1], slot[2]] = jnp.concatenate([one, tile[0:3], tile[0:3]], axis=0)

    def settle_all(xs, ys, zs):
        def one(step, carry):
            x = step + xs[0]
            for y in ys:
                for z in zs:
                    settle((x, y, z), (wrap(x, wraps[0]), y % wraps[1], z % wraps[2]))
            return carry

        lax.fori_loop(0, len(xs), one, 0)

    near_y, far_y = list(range(tiles[1])), [-1, tiles[1]]
    every_x = list(range(-1, tiles[0] + 1))
    own_z, side_z = list(range(tiles[2])), [-1, tiles[2]]

    def geometry(x, y, along_x, along_y, zs):
        nine = (along_x + 1) * 3 + (along_y + 1)
        line = x * tiles[1] + y
        slot_x, slot_y = wrap(x + along_x, wraps[0]), wrap(y + along_y, wraps[1])
        for level in zs:
            spot_at = levels.index(level)
            slot_z = level % wraps[2]
            takers = [z for z in range(tiles[2]) if abs(level - z) <= 1]
            softs = [
                SOFTENING + (1 - mask_ref[x, y, z, nine * 3 + level - z + 1]).astype(jnp.float32) * APART
                for z in takers
            ]
            lanes = slice(takers[0] * slots, (takers[-1] + 1) * slots)
            left = features[slot_x, slot_y, slot_z]
            squares = jnp.dot(left, distance[line, :, lanes], preferred_element_type=jnp.float32)
            damps = jnp.dot(left, damping[line, :, lanes], preferred_element_type=jnp.float32)
            for first in range(0, slots, BLOCK):
                part = pl.ds(first, BLOCK)
                for z, soft in zip(takers, softs):
                    at_lane = (z - takers[0]) * slots
                    square = squares[first : first + BLOCK, at_lane : at_lane + slots] + soft
                    damp = damps[first : first + BLOCK, at_lane : at_lane + slots]
                    root = lax.rsqrt(square)
                    root_two = root * root
                    cube = root_two * root
                    arg = (square * root) * square * damp
                    faded = jnp.exp(arg) * cube
                    direct = cube - faded
                    radial = (direct + arg * faded) * root_two
                    for number, value in ((0, radial), (2, direct)):
                        high = value.astype(jnp.bfloat16)
                        low = (value - high.astype(jnp.float32)).astype(jnp.bfloat16)
                        links[line, nine, number, spot_at, part, z * slots : (z + 1) * slots] = high
                        links[line, nine, number + 1, spot_at, part, z * slots : (z + 1) * slots] = low

    def geometry_near(along_x, zs):
        for to_y in range(tiles[1]):
            for x in range(tiles[0]):
                for y in range(tiles[1]):
                    if abs(to_y - y) <= 1:
                        geometry(x, y, along_x, to_y - y, zs)

    def plane_of(along_x):
        return jnp.where(along_x > 0, tiles[0], -1)

    def settle_plane(along_x, ys, zs):
        plane = plane_of(along_x)
        for y in ys:
            for z in zs:
                settle((plane, y, z), (wrap(plane, wraps[0]), y % wraps[1], z % wraps[2]))

    def arrive(copies, kinds_of):
        for move, copy in zip(moves, copies):
            if move[1][0] != 0:
                kind = "far"
            else:
                kind = ("x" if move[0][0] != 0 else "") + ("z" if move[2][0] != 0 else "")
            if kind in kinds_of:
                copy.wait()

    def geometry_far(first, last):
        def one(step, carry):
            x = step % tiles[0]
            side = step // tiles[0] % 2
            along_x = step // (2 * tiles[0]) - 1
            geometry(x, side * (tiles[1] - 1), along_x, 2 * side - 1, levels)
            return carry

        lax.fori_loop(first * tiles[0], last * tiles[0], one, 0, unroll=True)

    own_x = list(range(tiles[0]))
    settle_all(own_x, near_y, own_z)
    for x, y, z in places:
        lanes = slice(z * slots, (z + 1) * slots)
        far, fade = taker_features((x, y, z))
        distance[x * tiles[1] + y, :, lanes] = far
        damping[x * tiles[1] + y, :, lanes] = fade
    geometry_near(0, own_z)
    off_diagonal = lax.broadcasted_iota(jnp.int32, (slots, slots), 0) != lax.broadcasted_iota(
        jnp.int32, (slots, slots), 1
    )
    for x, y, z in places:
        lanes = slice(z * slots, (z + 1) * slots)
        for number in range(STREAMS):
            link = links[x * tiles[1] + y, 4, number, levels.index(z), :, lanes].astype(jnp.float32)
            links[x * tiles[1] + y, 4, number, levels.index(z), :, lanes] = jnp.where(
                off_diagonal, link, 0.0
            ).astype(jnp.bfloat16)

    pl.semaphore_wait(barrier, total_devices - 1)
    geom_copies = halo(geom, send_geom, recv_geom, 4)
    near_count = sum(1 for move in moves if move[1][0] == 0)
    for copy in geom_copies[:near_count]:
        copy.start()
    everyone(0, slots_a)
    for copy in geom_copies[near_count:]:
        copy.start()
    geom_parts = (geom, send_geom, recv_geom, 4)
    arrive_x(*geom_parts, first_move)
    settle_plane(first_x, near_y, own_z)
    geometry_near(first_x, own_z)
    arrive(geom_copies, ("z",))
    settle_all(own_x, near_y, side_z)
    geometry_near(0, side_z)
    arrive_x(*geom_parts, second_move)
    arrive(geom_copies, ("xz",))
    settle_plane(first_x, near_y, side_z)
    settle_plane(second_x, near_y, levels)
    geometry_near(first_x, side_z)

    everyone_wait(0, slots_a)
    total = jnp.sum(slots_a[...], axis=0)
    coeffs = solve_fit(total, past, lane, pair_lane)
    for t, (x, y, z) in enumerate(places):
        value = coeffs[0] * past_sets[1, t]
        for h in range(1, past):
            value = value + coeffs[h] * past_sets[h + 1, t]
        held_one[x, y, z] = value
    one_copies = halo(held_one, send_one, recv_one, rows)
    for copy in one_copies:
        copy.start()
    geometry_near(second_x, levels)
    arrive(geom_copies, ("far",))
    settle_all(every_x, far_y, levels)

    kinds = 5

    def weigh(held, xs, ys, zs):
        for x in xs:
            for y in ys:
                for z in zs:
                    slot = (wrap(x, wraps[0]), y % wraps[1], z % wraps[2])
                    moment = jnp.where(row_of < rows, held[slot], 0.0)
                    along = moment * turns[(0,) + slot]
                    first = jnp.sum(jnp.where(row_of < 3, along, 0.0), axis=0, keepdims=True)
                    second = jnp.sum(jnp.where(row_of < 3, 0.0, along), axis=0, keepdims=True)
                    which = jnp.logical_or(row_of == 0, jnp.logical_and(row_of >= 2, row_of < 5))
                    both = jnp.where(which, first, second) * turns[(1,) + slot]
                    tiles_of = [moment, both] + [
                        spots[slot + (pl.ds(c, 1), slice(None))] * moment for c in range(3)
                    ]
                    parts = [[], [], []]
                    for value in tiles_of:
                        for level in range(3):
                            piece = value.astype(jnp.bfloat16).astype(jnp.float32)
                            parts[level].append(piece)
                            value = value - piece
                    order = [parts[0][0], parts[1][0], parts[2][0]]
                    for level in range(3):
                        order = order + parts[level][1:]
                    order.append(jnp.zeros((ROWS, slots), jnp.float32))
                    weights[slot] = jnp.concatenate(order, axis=0).astype(jnp.bfloat16)

    def products(line, visits):
        main = jnp.zeros((SPREAD, wide), jnp.float32)
        rest = jnp.zeros((SPREAD_LOW, wide), jnp.float32)
        plain = jnp.zeros((SPREAD_PLAIN, wide), jnp.float32)
        blank = jnp.zeros((slots, slots), jnp.bfloat16)
        for nine, slot_x, slot_y, zs in visits:
            for start in range(0, len(zs), 2):
                chunk = [levels.index(z) for z in zs[start : start + 2]]
                left = jnp.concatenate(
                    [weights[slot_x, slot_y, levels[i] % wraps[2]] for i in chunk], axis=1
                )

                def matrix(number):
                    lines = []
                    for i in chunk:
                        lines.append(
                            jnp.concatenate(
                                [
                                    links[line, nine, number, i, :, z * slots : (z + 1) * slots]
                                    if abs(levels[i] - z) <= 1
                                    else blank
                                    for z in range(tiles[2])
                                ],
                                axis=1,
                            )
                        )
                    return jnp.concatenate(lines, axis=0)

                def times(values, number):
                    return jnp.dot(values, matrix(number), preferred_element_type=jnp.float32)

                main = main + times(left, 0)
                rest = rest + times(left[0:SPREAD_LOW], 1)
                plain = plain + times(left[0:SPREAD_PLAIN], 2)
                plain = plain + times(left[0:SPREAD_PLAIN], 3)
        return main, rest, plain

    def near_products(x, y, parts):
        visits = [
            ((along + 1) * 3 + to_y - y + 1, wrap(x + along, wraps[0]), to_y, zs)
            for along, zs in parts
            for to_y in range(tiles[1])
        ]
        return products(x * tiles[1] + y, visits)

    def far_products(x, y, side):
        visits = [
            ((along + 1) * 3 + 2 * side, wrap(x + along, wraps[0]), wrap((tiles[1] + 1) * side - 1, wraps[1]), levels)
            for along in (-1, 0, 1)
        ]
        return products(x * tiles[1] + y, visits)

    partials = (partial_main, partial_rest, partial_plain)

    def gather(parts, start):
        def one(step, carry):
            sums = near_products(step // tiles[1], step % tiles[1], parts)
            for partial, value in zip(partials, sums):
                partial[step] = value if start else partial[step] + value
            return carry

        lax.fori_loop(0, tiles[0] * tiles[1], one, 0, unroll=True)

    def field_of(x, y, main, rest, plain):
        def tile(value, index):
            return value[index * ROWS : (index + 1) * ROWS]

        def both_sum(first):
            total = tile(main, first[0]) + tile(rest, first[0])
            for index in first[1:]:
                total = total + tile(main, index)
                if (index + 1) * ROWS <= SPREAD_LOW:
                    total = total + tile(rest, index)
            return total

        moment = both_sum((0, 1, 2))
        both = both_sum((3, 7, 11))
        lifts = [both_sum((4 + c, 8 + c, 12 + c)) for c in range(3)]
        straight = tile(plain, 0) + tile(plain, 1) + tile(plain, 2)
        result = []
        for z in range(tiles[2]):
            lanes = slice(z * slots, (z + 1) * slots)
            turn = turns[0, x, y, z]
            inner = []
            for c in range(3):
                along = (lifts[c][:, lanes] - spots[x, y, z, pl.ds(c, 1), :] * moment[:, lanes]) * turn
                first = jnp.sum(jnp.where(row_of < 3, along, 0.0), axis=0, keepdims=True)
                second = jnp.sum(jnp.where(row_of < 3, 0.0, along), axis=0, keepdims=True)
                inner.append((first, second))
            inner = jnp.concatenate(
                [inner[c][0] for c in range(3)] + [inner[c][1] for c in range(3)] + [zero_row, zero_row], axis=0
            )
            lifted = jnp.concatenate([both[2:8, lanes], zero_row, zero_row], axis=0)
            dots = jnp.where(row_of < 3, both[0:1, lanes], both[1:2, lanes])
            result.append(3.0 * (lifted - dots * turn - inner) - straight[:, lanes])
        return result

    lines = tiles[0] * tiles[1]

    def field(step, held, act):
        x, y = step // tiles[1], step % tiles[1]
        main, rest, plain = partial_main[step], partial_rest[step], partial_plain[step]
        for side in range(2):
            if tiles[1] == 1:
                more = far_products(x, y, side)
                main, rest, plain = main + more[0], rest + more[1], plain + more[2]
        if tiles[1] > 1:
            side = y // (tiles[1] - 1)
            more = far_products(x, y, side)
            keep = jnp.logical_or(y == 0, y == tiles[1] - 1).astype(jnp.float32)
            if tiles[1] > 2:
                more = tuple(jnp.where(keep > 0.5, value, 0.0) for value in more)
            main, rest, plain = main + more[0], rest + more[1], plain + more[2]
        fields = field_of(x, y, main, rest, plain)
        for z in range(tiles[2]):
            t = step * tiles[2] + z
            act(x, y, z, t, (1.0 - RELAXATION) * held[x, y, z] + scaled[t] * (fixed[t] + fields[z]))

    def arrive_near(parts, copies):
        arrive_x(*parts, first_move)
        arrive_x(*parts, second_move)
        arrive(copies, ("z", "xz"))

    def first_near(held, parts, copies):
        weigh(held, own_x, near_y, own_z)
        gather([(0, own_z)], True)
        geometry_far(0, 4)
        arrive_near(parts, copies)
        weigh(held, own_x, near_y, side_z)
        weigh(held, [-1, tiles[0]], near_y, levels)
        geometry_far(4, 6)
        gather([(0, side_z), (-1, levels), (1, levels)], False)

    def second_near(held, parts, copies):
        weigh(held, own_x, near_y, own_z)
        gather([(0, own_z)], True)
        arrive_x(*parts, first_move)
        weigh(held, [plane_of(first_x)], near_y, own_z)
        gather([(first_x, own_z)], False)
        arrive(copies, ("z",))
        weigh(held, own_x, near_y, side_z)
        gather([(0, side_z)], False)
        arrive_x(*parts, second_move)
        arrive(copies, ("xz",))
        weigh(held, [plane_of(first_x)], near_y, side_z)
        weigh(held, [plane_of(second_x)], near_y, levels)
        gather([(first_x, side_z), (second_x, levels)], False)

    def sweep(held, copies, act):
        arrive(copies, ("far",))
        weigh(held, every_x, far_y, levels)

        def one(step, carry):
            field(step, held, act)
            return carry

        lax.fori_loop(0, lines, one, 0, unroll=True)

    def first_act(x, y, z, t, value):
        held_two[x, y, z] = value

    first_near(held_one, (held_one, send_one, recv_one, rows), one_copies)
    sweep(held_one, one_copies, first_act)
    two_copies = halo(held_two, send_two, recv_two, rows)
    for copy in two_copies:
        copy.start()

    def second_act(x, y, z, t, value):
        held_one[x, y, z] = value

    second_near(held_two, (held_two, send_two, recv_two, rows), two_copies)
    sweep(held_two, two_copies, second_act)
    changed = jnp.zeros((ROWS, slots), jnp.float32)
    size = jnp.zeros((ROWS, slots), jnp.float32)
    for t, (x, y, z) in enumerate(places):
        before, after = held_two[x, y, z], held_one[x, y, z]
        changed = changed + (after - before) * (after - before)
        size = size + after * after

    pair = jnp.concatenate(
        [jnp.sum(value, axis=0, keepdims=True) for value in (changed, size)], axis=1
    )
    slots_b[pl.ds(me, 1)] = pair.reshape(1, 1, 2 * slots)
    everyone(1, slots_b)
    for x, y, z in places:
        after = held_one[x, y, z]
        for c in range(rows):
            out_ref[c, x, y, z, :] = after[c]
    put = pltpu.make_async_copy(out_ref, out_hbm, load_sem.at[len(loads)])
    put.start()
    everyone_wait(1, slots_b)
    pair = jnp.sum(slots_b[...], axis=0)
    above = jnp.sum(pair[:, 0:slots], axis=1, keepdims=True)
    below = jnp.sum(pair[:, slots : 2 * slots], axis=1, keepdims=True)
    change_ref[...] = jnp.broadcast_to(jnp.sqrt(above / (below + 1.0)), (1, slots))
    put.wait()


def solution(mesh):
    devices = tuple(mesh.shape[axis] for axis in AXES)
    total_devices = devices[0] * devices[1] * devices[2]

    def on_device(fractions, polarizability, occupancy, pair_mask, perm_field, history):
        tiles = fractions.shape[1:4]
        slots = fractions.shape[4]
        count = tiles[0] * tiles[1] * tiles[2]
        lines = tiles[0] * tiles[1]
        wraps = tuple(n + 2 for n in tiles)
        moves = len(halo_moves(devices, tiles))
        rows = history.shape[1]
        vmem = pl.BlockSpec(memory_space=pltpu.VMEM)
        f32 = jnp.float32
        induced, change = pl.pallas_call(
            functools.partial(kernel, devices),
            out_shape=(
                jax.ShapeDtypeStruct(perm_field.shape, f32),
                jax.ShapeDtypeStruct((1, slots), f32),
            ),
            in_specs=[pl.BlockSpec(memory_space=pltpu.HBM)] * 6,
            out_specs=(pl.BlockSpec(memory_space=pltpu.HBM), vmem),
            scratch_shapes=[
                pltpu.VMEM(perm_field.shape, f32),
                pltpu.VMEM(fractions.shape, f32),
                pltpu.VMEM(polarizability.shape, f32),
                pltpu.VMEM(occupancy.shape, jnp.int32),
                pltpu.SMEM(pair_mask.shape, jnp.int32),
                pltpu.VMEM(perm_field.shape, f32),
                pltpu.VMEM(history.shape, f32),
                pltpu.VMEM(wraps + (ROWS, slots), f32),
                pltpu.VMEM(wraps + (ROWS, slots), f32),
                pltpu.VMEM(wraps + (ROWS, slots), f32),
                pltpu.VMEM((history.shape[0], count, ROWS, slots), f32),
                pltpu.VMEM(wraps + (ROWS, slots), f32),
                pltpu.VMEM(wraps + (6, ROWS, slots), f32),
                pltpu.VMEM(wraps + (slots, slots), jnp.bfloat16),
                pltpu.VMEM((lines, slots, tiles[2] * slots), jnp.bfloat16),
                pltpu.VMEM((lines, slots, tiles[2] * slots), jnp.bfloat16),
                pltpu.VMEM((2,) + wraps + (ROWS, slots), f32),
                pltpu.VMEM((lines, 9, STREAMS, wraps[2], slots, tiles[2] * slots), jnp.bfloat16),
                pltpu.VMEM(wraps + (SPREAD, slots), jnp.bfloat16),
                pltpu.VMEM((lines, SPREAD, tiles[2] * slots), f32),
                pltpu.VMEM((lines, SPREAD_LOW, tiles[2] * slots), f32),
                pltpu.VMEM((lines, SPREAD_PLAIN, tiles[2] * slots), f32),
                pltpu.VMEM((count, ROWS, slots), f32),
                pltpu.VMEM((count, ROWS, slots), f32),
                pltpu.VMEM((total_devices, 1, slots), f32),
                pltpu.VMEM((total_devices, 1, 2 * slots), f32),
                pltpu.SemaphoreType.DMA((7,)),
                pltpu.SemaphoreType.DMA((2,)),
                pltpu.SemaphoreType.DMA((2,)),
            ]
            + [pltpu.SemaphoreType.DMA((moves,))] * 6,
            compiler_params=pltpu.CompilerParams(
                collective_id=0, has_side_effects=True, vmem_limit_bytes=67043328
            ),
        )(fractions, polarizability, occupancy, pair_mask, perm_field, history)
        return induced, change[0, 0]

    in_specs = (
        P(None, "gx", "gy", "gz", None),
        P("gx", "gy", "gz", None),
        P("gx", "gy", "gz", None),
        P("gx", "gy", "gz", None),
        P(None, "gx", "gy", "gz", None),
        P(None, None, "gx", "gy", "gz", None),
    )
    out_specs = (P(None, "gx", "gy", "gz", None), P())
    return jax.shard_map(
        on_device, mesh=mesh, in_specs=in_specs, out_specs=out_specs, check_vma=False
    )
```
